128 devices in a mesh: model: 64 (over z, y, x), fsdp: 2 (over core).
Axes of the slice: x: 4, y: 4, z: 4, core: 2. Of those that a mesh axis runs over, the one named last changes fastest.
Arguments:
- tok_ids: int32 [2, 1024], P('fsdp')
- tok_labels: int32 [2, 1024], P('fsdp')
- emb_table: bfloat16 [50304, 1024], P(('model', 'fsdp'))
- w_gate: bfloat16 [1024, 4096], P('fsdp')
- w_up: bfloat16 [1024, 4096], P('fsdp')
- w_down: bfloat16 [4096, 1024], P('fsdp')
- gain_in: float32 [1024], replicated
- gain_out: float32 [1024], replicated
Outputs:
- output 1: float32 [], replicated
- output 2: float32 [50304, 1024], P(('model', 'fsdp'))
- output 3: float32 [1024, 4096], P('fsdp')
- output 4: float32 [1024, 4096], P('fsdp')
- output 5: float32 [4096, 1024], P('fsdp')
All inputs are finite; a program needn't handle non-finite values.
Results may differ from the reference program's by a relative error of at most 0.0118123.
Values are sent between devices in bfloat16 or wider.
A program may use at most 1 GiB of HBM per device.

```python
import jax
import jax.numpy as jnp
from jax import lax

V = 50304
D = 1024
F = 4096
BATCH = 2
SEQ = 1024
HEAD_BLOCK = 64
EPS = 1e-6


def draw_tokens(base_key):
    id_key, label_key = jax.random.split(base_key)
    tok_ids = jax.random.randint(id_key, (BATCH, SEQ), 0, V, dtype=jnp.int32)
    tok_ids = tok_ids.at[0, 0].set(0).at[BATCH - 1, SEQ - 1].set(V - 1)
    tok_labels = jax.random.randint(label_key, (BATCH, SEQ), 0, V, dtype=jnp.int32)
    tok_labels = tok_labels.at[0, 0].set(V - 1).at[BATCH - 1, SEQ - 1].set(0)
    return tok_ids, tok_labels


def setup_inputs(seed: int = 0) -> dict:
    rng_keys = jax.random.split(jax.random.key(seed), 7)
    tok_ids, tok_labels = draw_tokens(rng_keys[0])
    emb_table = (jax.random.normal(rng_keys[1], (V, D), jnp.float32) * D ** -0.5).astype(jnp.bfloat16)
    w_gate = (jax.random.normal(rng_keys[2], (D, F), jnp.float32) * D ** -0.5).astype(jnp.bfloat16)
    w_up = (jax.random.normal(rng_keys[3], (D, F), jnp.float32) * D ** -0.5).astype(jnp.bfloat16)
    w_down = (jax.random.normal(rng_keys[4], (F, D), jnp.float32) * (2.0 * (F * D) ** -0.5)).astype(jnp.bfloat16)
    gain_in = jax.random.uniform(rng_keys[5], (D,), jnp.float32, 0.5, 1.5)
    gain_out = jax.random.uniform(rng_keys[6], (D,), jnp.float32, 0.5, 1.5)
    return {"tok_ids": tok_ids, "tok_labels": tok_labels, "emb_table": emb_table, "w_gate": w_gate, "w_up": w_up, "w_down": w_down, "gain_in": gain_in, "gain_out": gain_out}


def rms_scale(values, gain_vec):
    mean_sq = jnp.mean(values * values, axis=-1, keepdims=True)
    return values * lax.rsqrt(mean_sq + EPS) * gain_vec


def reference(tok_ids, tok_labels, emb_table, w_gate, w_up, w_down, gain_in, gain_out):
    num_tokens = BATCH * SEQ
    flat_ids = tok_ids.reshape(num_tokens)
    flat_labels = tok_labels.reshape(num_tokens)
    x_emb = emb_table[flat_ids].astype(jnp.float32)
    normed_in, norm_in_back = jax.vjp(lambda values: rms_scale(values, gain_in), x_emb)
    normed_bf = normed_in.astype(jnp.bfloat16)
    gate_f = jnp.dot(normed_bf, w_gate, preferred_element_type=jnp.float32).astype(jnp.bfloat16).astype(jnp.float32)
    up_f = jnp.dot(normed_bf, w_up, preferred_element_type=jnp.float32).astype(jnp.bfloat16).astype(jnp.float32)
    gate_sig = jax.nn.sigmoid(gate_f)
    silu_gate = gate_f * gate_sig
    act_bf = (silu_gate * up_f).astype(jnp.bfloat16)
    mlp_out = jnp.dot(act_bf, w_down, preferred_element_type=jnp.float32).astype(jnp.bfloat16)
    h_res = x_emb + mlp_out.astype(jnp.float32)
    hn_f, norm_out_back = jax.vjp(lambda values: rms_scale(values, gain_out), h_res)
    hn_bf = hn_f.astype(jnp.bfloat16)
    num_blocks = num_tokens // HEAD_BLOCK
    hn_blocks = hn_bf.reshape(num_blocks, HEAD_BLOCK, D)
    label_blocks = flat_labels.reshape(num_blocks, HEAD_BLOCK)

    def head_step(d_head, block_in):
        hn_blk, label_blk = block_in
        logits = jnp.dot(hn_blk, emb_table.T, preferred_element_type=jnp.float32)
        row_max = jnp.max(logits, axis=-1, keepdims=True)
        exp_shift = jnp.exp(logits - row_max)
        sum_exp = jnp.sum(exp_shift, axis=-1, keepdims=True)
        onehot = lax.broadcasted_iota(jnp.int32, logits.shape, 1) == label_blk[:, None]
        label_logit = jnp.sum(jnp.where(onehot, logits, 0.0), axis=-1)
        tok_loss = row_max[:, 0] + jnp.log(sum_exp[:, 0]) - label_logit
        soft_probs = exp_shift / sum_exp
        d_logits = (jnp.where(onehot, soft_probs - 1.0, soft_probs) / num_tokens).astype(jnp.bfloat16)
        d_head = d_head + jnp.dot(d_logits.T, hn_blk, preferred_element_type=jnp.float32)
        d_hn = jnp.dot(d_logits, emb_table, preferred_element_type=jnp.float32)
        return d_head, (tok_loss, d_hn)

    d_head, (tok_losses, d_hn_blocks) = lax.scan(head_step, jnp.zeros((V, D), jnp.float32), (hn_blocks, label_blocks))
    loss = jnp.sum(tok_losses) / num_tokens
    d_hn = d_hn_blocks.reshape(num_tokens, D)
    d_hidden = norm_out_back(d_hn)[0]
    d_mlp = d_hidden.astype(jnp.bfloat16)
    d_act = jnp.dot(d_mlp, w_down.T, preferred_element_type=jnp.float32)
    grad_down = jnp.dot(act_bf.T, d_mlp, preferred_element_type=jnp.float32)
    d_gate = (d_act * up_f * (gate_sig * (1.0 + gate_f * (1.0 - gate_sig)))).astype(jnp.bfloat16)
    d_up = (d_act * silu_gate).astype(jnp.bfloat16)
    grad_gate = jnp.dot(normed_bf.T, d_gate, preferred_element_type=jnp.float32)
    grad_up = jnp.dot(normed_bf.T, d_up, preferred_element_type=jnp.float32)
    d_normed = jnp.dot(d_gate, w_gate.T, preferred_element_type=jnp.float32) + jnp.dot(d_up, w_up.T, preferred_element_type=jnp.float32)
    d_x = d_hidden + norm_in_back(d_normed)[0]
    d_in = jax.ops.segment_sum(d_x, flat_ids, num_segments=V)
    grad_table = d_head + d_in
    return (loss, grad_table, grad_gate, grad_up, grad_down)
```

```python
import functools

import jax
import jax.numpy as jnp
from jax import lax
from jax.experimental import pallas as pl
from jax.experimental.pallas import tpu as pltpu
from jax.sharding import PartitionSpec as P

EPS = 1e-6
MESH = pl.DeviceIdType.MESH
VMEM_LIMIT = 64 * 1024 * 1024 - 64 * 1024
F32 = jnp.float32
BF16 = jnp.bfloat16
COLORS = 3


def dot(a, b, ca, cb):
    return lax.dot_general(a, b, (((ca,), (cb,)), ((), ())), preferred_element_type=F32)


def rms_scale(values, gain):
    mean_sq = jnp.mean(values * values, axis=-1, keepdims=True)
    return values * lax.rsqrt(mean_sq + EPS) * gain


def rms_back(values, gain, grad):
    r = lax.rsqrt(jnp.mean(values * values, axis=-1, keepdims=True) + EPS)
    gg = grad * gain
    return r * gg - values * (r * r * r) * jnp.mean(values * gg, axis=-1, keepdims=True)


class Cube:
    def __init__(self, model, rows, width):
        axes = {4: 1, 16: 2, 64: 3}[model]
        self.axes, self.nb, self.rows = axes, 2 * axes, rows
        self.last = rows >> self.nb
        unit = width // 8 if width % 1024 == 0 else width // 3
        sizes = [3 * unit, 3 * unit, 2 * unit] if width % 1024 == 0 else [unit] * 3
        self.widths = sizes
        self.starts = [0, sizes[0], sizes[0] + sizes[1]]

    def bind(self):
        self.m = lax.axis_index("model")
        self.c = lax.axis_index("fsdp")
        self.digits = [(self.m // 4**a) % 4 for a in range(self.axes)]
        self.partner, self.bit, self.base = [], [], []
        for k in range(COLORS):
            partners, bits, bases = [], [], [0]
            for s in range(self.nb):
                d = (k + s) % self.nb
                a = d % self.axes
                t = (d // self.axes + self.c) % 2
                b = self.digits[a]
                b1, b0 = b // 2, b % 2
                v0, v1 = (b0 + b1) % 2, b1
                bit = v0 + t * (v1 - v0)
                d0, d1 = 1 - 2 * b0, 3 - 2 * b
                partners.append(self.m + 4**a * (d0 + t * (d1 - d0)))
                bits.append(bit)
                bases.append(bases[-1] + bit * (self.rows >> (s + 1)))
            self.partner.append(partners)
            self.bit.append(bits)
            self.base.append(bases)

    def neighbours(self, far):
        out = []
        for a in range(self.axes):
            b = self.digits[a]
            b0 = b % 2
            out.append(self.m + 4**a * (1 - 2 * b0))
            out.append(self.m + 4**a * (3 - 2 * b))
            if far:
                out.append(self.m + 4**a * ((b + 2) % 4 - b))
        return out

    def barrier(self, far=False):
        sem = pltpu.get_barrier_semaphore()
        peers = self.neighbours(far)
        for p in peers:
            pl.semaphore_signal(sem, inc=1, device_id=(p, self.c), device_id_type=MESH)
        pl.semaphore_signal(sem, inc=1, device_id=(self.m, 1 - self.c), device_id_type=MESH)
        pl.semaphore_wait(sem, len(peers) + 1)

    def place(self, k, j):
        pos = []
        for c in range(2):
            p = 0
            for s in range(self.nb):
                d = (k + s) % self.nb
                a = d % self.axes
                t = (d // self.axes + c) % 2
                p |= ((j >> (a + self.axes * t)) & 1) << (self.nb - 1 - s)
            pos.append(p * self.last)
        return pl.multiple_of(pos[0] + self.c * (pos[1] - pos[0]), self.last)

    def rows_at(self, start, size):
        return pl.ds(pl.multiple_of(start, self.last), size)

    def cols(self, k):
        return pl.ds(self.starts[k], self.widths[k])

    def spread(self, nat, bufs):
        for j in range(1 << self.nb):
            for k in range(COLORS):
                bufs[k][pl.ds(self.place(k, j), self.last), :] = nat[pl.ds(j * self.last, self.last), self.cols(k)]

    def collect(self, bufs, nat, offset=0):
        for j in range(1 << self.nb):
            for k in range(COLORS):
                at = pl.ds(j * self.last, self.last) if isinstance(offset, int) and offset == 0 else self.rows_at(offset + j * self.last, self.last)
                nat[at, self.cols(k)] = bufs[k][pl.ds(self.place(k, j), self.last), :]

    def own(self, k):
        return self.rows_at(self.base[k][self.nb], self.last)

    def rs_copy(self, bufs, recvs, send, recv, k, s):
        ln = self.rows >> (s + 1)
        start = self.base[k][s] + (1 - self.bit[k][s]) * ln
        off = self.rows - (self.rows >> s)
        return pltpu.make_async_remote_copy(
            src_ref=bufs[k].at[self.rows_at(start, ln)],
            dst_ref=recvs[k].at[pl.ds(off, ln)],
            send_sem=send.at[k, s],
            recv_sem=recv.at[k, s],
            device_id=(self.partner[k][s], self.c),
            device_id_type=MESH,
        )

    def rs_add(self, bufs, recvs, k, s):
        ln = self.rows >> (s + 1)
        off = self.rows - (self.rows >> s)
        at = self.rows_at(self.base[k][s + 1], ln)
        got = recvs[k][pl.ds(off, ln), :].astype(F32)
        bufs[k][at, :] = (bufs[k][at, :].astype(F32) + got).astype(bufs[k].dtype)

    def reduce_scatter(self, bufs, recvs, send, recv, fill=None):
        for k in range(COLORS):
            self.rs_copy(bufs, recvs, send, recv, k, 0).start()
        for s in range(self.nb):
            if fill is not None:
                fill(s)
            for k in range(COLORS):
                self.rs_copy(bufs, recvs, send, recv, k, s).wait()
                self.rs_add(bufs, recvs, k, s)
                if s + 1 < self.nb:
                    self.rs_copy(bufs, recvs, send, recv, k, s + 1).start()

    def ag_copy(self, bufs, send, recv, k, s):
        ln = self.rows >> (s + 1)
        at = self.rows_at(self.base[k][s + 1], ln)
        return pltpu.make_async_remote_copy(
            src_ref=bufs[k].at[at],
            dst_ref=bufs[k].at[at],
            send_sem=send.at[k, s],
            recv_sem=recv.at[k, s],
            device_id=(self.partner[k][s], self.c),
            device_id_type=MESH,
        )

    def ag_start(self, bufs, send, recv, s):
        for k in range(COLORS):
            self.ag_copy(bufs, send, recv, k, s).start()

    def ag_next(self, bufs, send, recv, s):
        for k in range(COLORS):
            self.ag_copy(bufs, send, recv, k, s).wait()
            if s > 0:
                self.ag_copy(bufs, send, recv, k, s - 1).start()

    def all_gather(self, bufs, send, recv, fill=None):
        self.ag_start(bufs, send, recv, self.nb - 1)
        for s in range(self.nb - 1, -1, -1):
            if fill is not None:
                fill(s)
            self.ag_next(bufs, send, recv, s)

    def pair_copy(self, src, dst, send, recv):
        return pltpu.make_async_remote_copy(
            src_ref=src, dst_ref=dst, send_sem=send, recv_sem=recv, device_id=(self.m, 1 - self.c), device_id_type=MESH
        )

    def group_scratch(self, dtype):
        return [pltpu.VMEM((self.rows, w), dtype) for w in self.widths]

    def sems(self):
        return [pltpu.SemaphoreType.DMA((COLORS, self.nb))] * 2


def embed_kernel(cube, vb, idx, e_ref, wg, wu, wd, g1, g2, hn, ep, xf, wgh, wuh, h_own, gt_own, u_own, x_own, *scratch):
    it = iter(scratch)
    wd_s = next(it)
    xb = [next(it) for _ in range(COLORS)]
    xr = [next(it) for _ in range(COLORS)]
    gb = [next(it) for _ in range(COLORS)]
    hb = [next(it) for _ in range(COLORS)]
    xnat, x32, mp, mr = next(it), next(it), next(it), next(it)
    rs_s, rs_r, xg_s, xg_r, hg_s, hg_r, psend, precv, lsem = [next(it) for _ in range(9)]
    cube.bind()
    c = cube.c
    d = hn.shape[1]
    half_d, half_f = d // 2, wgh.shape[1]
    nb, last = cube.nb, cube.last
    mine_f = pl.ds(pl.multiple_of(c * half_f, half_f), half_f)
    other_f = pl.ds(pl.multiple_of((1 - c) * half_f, half_f), half_f)
    mine_d = pl.ds(pl.multiple_of(c * half_d, half_d), half_d)
    e_local = pltpu.make_async_copy(e_ref, ep.at[pl.ds(0, vb)], lsem.at[0])
    e_local.start()
    wd_local = pltpu.make_async_copy(wd, wd_s, lsem.at[1])
    wg_local = pltpu.make_async_copy(wg.at[:, mine_f], wgh.at[mine_d], lsem.at[2])
    wu_local = pltpu.make_async_copy(wu.at[:, mine_f], wuh.at[mine_d], lsem.at[3])
    cube.barrier()
    e_pair = cube.pair_copy(e_ref, ep.at[pl.ds(vb, vb)], psend.at[0], precv.at[0])
    e_pair.start()
    wg_pair = cube.pair_copy(wg.at[:, other_f], wgh.at[mine_d], psend.at[1], precv.at[1])
    wu_pair = cube.pair_copy(wu.at[:, other_f], wuh.at[mine_d], psend.at[2], precv.at[2])
    wg_pair.start()
    wu_pair.start()
    wd_local.start()
    wg_local.start()
    wu_local.start()
    e_local.wait()
    e_pair.wait()

    chunk = min(256, cube.rows)

    def lookup(i, carry):
        at = pl.ds(pl.multiple_of(i * chunk, chunk), chunk)
        hot = (lax.broadcasted_iota(jnp.int32, (2 * vb, chunk), 0) == idx[:, at]).astype(F32).astype(BF16)
        xnat[at, :] = dot(hot, ep[...], 0, 0).astype(BF16)
        return carry

    lax.fori_loop(0, cube.rows // chunk, lookup, 0)
    cube.spread(xnat, xb)
    cube.reduce_scatter(xb, xr, rs_s, rs_r)
    for k in range(COLORS):
        part = xb[k][cube.own(k), :]
        gb[k][cube.own(k), :] = part
        x32[0, :, cube.cols(k)] = part
    x_pair = cube.pair_copy(x32.at[0], x32.at[1], psend.at[3], precv.at[3])
    x_pair.start()
    cube.ag_start(gb, xg_s, xg_r, nb - 1)
    x_pair.wait()
    wd_local.wait()
    wg_local.wait()
    wu_local.wait()
    wg_pair.wait()
    wu_pair.wait()
    x_rows = x32[...].reshape(2 * last, d).astype(F32)
    a_rows = rms_scale(x_rows, g1[...]).astype(BF16)
    parts = 4
    fc = half_f // parts
    total = jnp.zeros((2 * last, d), F32)
    step = nb - 1
    for p in range(parts):
        at = pl.ds(p * fc, fc)
        gate = dot(a_rows, wgh[:, at], 1, 0).astype(BF16)
        up = dot(a_rows, wuh[:, at], 1, 0).astype(BF16)
        gt_own[:, at] = gate
        u_own[:, at] = up
        gate_f = gate.astype(F32)
        act = (gate_f * jax.nn.sigmoid(gate_f) * up.astype(F32)).astype(BF16)
        total = total + dot(act, wd_s[at, :], 1, 0)
        if step > 1:
            cube.ag_next(gb, xg_s, xg_r, step)
            step -= 1
    mp[...] = total.reshape(2, last, d)
    m_pair = cube.pair_copy(mp.at[1], mr, psend.at[4], precv.at[4])
    m_pair.start()
    m_pair.wait()
    m_rows = (mp[0] + mr[...]).astype(BF16)
    x_first = x32[0].astype(F32)
    h_rows = x_first + m_rows.astype(F32)
    x_own[...] = x_first
    h_own[...] = h_rows
    hn_rows = rms_scale(h_rows, g2[...]).astype(BF16)
    for k in range(COLORS):
        hb[k][cube.own(k), :] = hn_rows[:, cube.starts[k] : cube.starts[k] + cube.widths[k]]
    cube.ag_start(hb, hg_s, hg_r, nb - 1)
    hstep = nb - 1
    while step >= 0:
        cube.ag_next(gb, xg_s, xg_r, step)
        step -= 1
        if hstep > 0:
            cube.ag_next(hb, hg_s, hg_r, hstep)
            hstep -= 1
    cube.collect(gb, xf, c * cube.rows)
    mine_t = pl.ds(pl.multiple_of(c * cube.rows, cube.rows), cube.rows)
    xf_pair = cube.pair_copy(xf.at[mine_t], xf.at[mine_t], psend.at[5], precv.at[5])
    xf_pair.start()
    while hstep >= 0:
        cube.ag_next(hb, hg_s, hg_r, hstep)
        hstep -= 1
    cube.collect(hb, hn)
    xf_pair.wait()


def head_kernel(cube, vb, real, num_tokens, hn, ep, lab, h_own, g2, dmf, loss, deh, dh_own, *scratch):
    it = iter(scratch)
    z, dz, nat = next(it), next(it), next(it)
    rb = [next(it) for _ in range(COLORS)]
    rr = [next(it) for _ in range(COLORS)]
    gb = [next(it) for _ in range(COLORS)]
    stats, lbuf = next(it), next(it)
    rs_s, rs_r, ag_s, ag_r, st_s, st_r, psend, precv = [next(it) for _ in range(8)]
    cube.bind()
    c = cube.c
    t, d = hn.shape
    cube.barrier(far=True)
    chunk = min(256, t)

    def logits(i, carry):
        at = pl.ds(pl.multiple_of(i * chunk, chunk), chunk)
        row = lax.broadcasted_iota(jnp.int32, (2 * vb, chunk), 0)
        valid = (row < real) | ((row >= vb) & (row < vb + real))
        zz = dot(ep[...], hn[at, :], 1, 1)
        zz = jnp.where(valid, zz, -1e38)
        z[:, at] = zz
        top = jnp.max(zz, axis=0, keepdims=True)
        mine = cube.digits[0]
        stats[0, mine, 0:1, at] = top
        stats[0, mine, 1:2, at] = jnp.sum(jnp.exp(zz - top), axis=0, keepdims=True)
        stats[0, mine, 2:3, at] = jnp.sum(jnp.where(row == lab[:, at], zz, 0.0), axis=0, keepdims=True)
        return carry

    lax.fori_loop(0, t // chunk, logits, 0)
    top = total = label = None
    for a in range(cube.axes):
        b = cube.digits[a]
        copies = []
        for step in range(1, 4):
            peer = cube.m + 4**a * ((b + step) % 4 - b)
            copies.append(
                pltpu.make_async_remote_copy(
                    src_ref=stats.at[a, b],
                    dst_ref=stats.at[a, b],
                    send_sem=st_s.at[a, step - 1],
                    recv_sem=st_r.at[a, step - 1],
                    device_id=(peer, c),
                    device_id_type=MESH,
                )
            )
        for copy in copies:
            copy.start()
        for copy in copies:
            copy.wait()
        top = jnp.maximum(jnp.maximum(stats[a, 0, 0:1, :], stats[a, 1, 0:1, :]), jnp.maximum(stats[a, 2, 0:1, :], stats[a, 3, 0:1, :]))
        total = sum(stats[a, i, 1:2, :] * jnp.exp(stats[a, i, 0:1, :] - top) for i in range(4))
        label = sum(stats[a, i, 2:3, :] for i in range(4))
        nxt = (a + 1, cube.digits[a + 1]) if a + 1 < cube.axes else (a + 1, 0)
        stats[nxt[0], nxt[1], 0:1, :] = top
        stats[nxt[0], nxt[1], 1:2, :] = total
        stats[nxt[0], nxt[1], 2:3, :] = label
    fin = cube.axes
    tok_loss = jnp.sum(top + jnp.log(total) - label, axis=1, keepdims=True)
    lbuf[c] = jnp.broadcast_to(tok_loss, (8, 128))
    l_pair = cube.pair_copy(lbuf.at[c], lbuf.at[c], psend.at[0], precv.at[0])
    l_pair.start()

    def backward(i, carry):
        at = pl.ds(pl.multiple_of(i * chunk, chunk), chunk)
        row = lax.broadcasted_iota(jnp.int32, (2 * vb, chunk), 0)
        soft = jnp.exp(z[:, at] - stats[fin, 0, 0:1, at]) / stats[fin, 0, 1:2, at]
        dzz = (jnp.where(row == lab[:, at], soft - 1.0, soft) / num_tokens).astype(BF16)
        dz[:, at] = dzz
        nat[at, :] = dot(dzz, ep[...], 0, 0)
        return carry

    lax.fori_loop(0, t // chunk, backward, 0)
    cube.spread(nat, rb)

    def fill(s):
        if s == 0:
            rows = 2 * vb // 2

            def head_grad(i, carry):
                at = pl.ds(pl.multiple_of(i * rows, rows), rows)
                deh[at, :] = dot(dz[at, :], hn[...], 1, 0)
                return carry

            lax.fori_loop(0, 2, head_grad, 0)

    cube.reduce_scatter(rb, rr, rs_s, rs_r, fill)
    dhn = jnp.concatenate([rb[k][cube.own(k), :] for k in range(COLORS)], axis=1)
    dh = rms_back(h_own[...], g2[...], dhn)
    dh_own[...] = dh
    dm = dh.astype(BF16)
    for k in range(COLORS):
        gb[k][cube.own(k), :] = dm[:, cube.starts[k] : cube.starts[k] + cube.widths[k]]
    cube.all_gather(gb, ag_s, ag_r)
    cube.collect(gb, dmf, c * cube.rows)
    mine_t = pl.ds(pl.multiple_of(c * cube.rows, cube.rows), cube.rows)
    dm_pair = cube.pair_copy(dmf.at[mine_t], dmf.at[mine_t], psend.at[1], precv.at[1])
    dm_pair.start()
    l_pair.wait()
    loss[...] = (lbuf[0] + lbuf[1]) / num_tokens
    dm_pair.wait()


def table_kernel(cube, vb, idx, dh_own, x_own, gt_own, u_own, wgh, wuh, wd, g1, deh, de, *scratch):
    it = iter(scratch)
    dm32, mp, mr, nat, mix, de_r = [next(it) for _ in range(6)]
    gb = [next(it) for _ in range(COLORS)]
    ag_s, ag_r, psend, precv = [next(it) for _ in range(4)]
    cube.bind()
    last, d = dh_own.shape
    dh = dh_own[...]
    dm32[0] = dh.astype(BF16)
    cube.barrier()
    dm_pair = cube.pair_copy(dm32.at[0], dm32.at[1], psend.at[0], precv.at[0])
    dm_pair.start()
    dm_pair.wait()
    dm_rows = dm32[...].reshape(2 * last, d)
    half_f = wgh.shape[1]
    parts = 4
    fc = half_f // parts
    total = jnp.zeros((2 * last, d), F32)
    for p in range(parts):
        at = pl.ds(p * fc, fc)
        d_act = dot(dm_rows, wd[at, :], 1, 1)
        gate = gt_own[:, at].astype(F32)
        sig = jax.nn.sigmoid(gate)
        d_gate = (d_act * u_own[:, at].astype(F32) * (sig * (1.0 + gate * (1.0 - sig)))).astype(BF16)
        d_up = (d_act * (gate * sig)).astype(BF16)
        total = total + (dot(d_gate, wgh[:, at], 1, 1) + dot(d_up, wuh[:, at], 1, 1))
    mp[...] = total.reshape(2, last, d)
    m_pair = cube.pair_copy(mp.at[1], mr, psend.at[1], precv.at[1])
    m_pair.start()
    m_pair.wait()
    dx = dh + rms_back(x_own[...], g1[...], mp[0] + mr[...])
    for k in range(COLORS):
        gb[k][cube.own(k), :] = dx[:, cube.starts[k] : cube.starts[k] + cube.widths[k]]
    cube.all_gather(gb, ag_s, ag_r)
    cube.collect(gb, nat)
    t = cube.rows
    chunk = min(256, t)
    mix[...] = deh[...]

    def scatter(i, carry):
        at = pl.ds(pl.multiple_of(i * chunk, chunk), chunk)
        hot = (lax.broadcasted_iota(jnp.int32, (2 * vb, chunk), 0) == idx[:, at]).astype(F32).astype(BF16)
        val = nat[at, :]
        hi = val.astype(BF16)
        rest = val - hi.astype(F32)
        mid = rest.astype(BF16)
        low = (rest - mid.astype(F32)).astype(BF16)
        mix[...] = mix[...] + ((dot(hot, low, 1, 0) + dot(hot, mid, 1, 0)) + dot(hot, hi, 1, 0))
        return carry

    lax.fori_loop(0, t // chunk, scatter, 0)
    e_pair = cube.pair_copy(mix.at[pl.ds(vb, vb)], de_r, psend.at[2], precv.at[2])
    e_pair.start()
    e_pair.wait()
    de[...] = mix[pl.ds(0, vb), :] + de_r[...]


def solution(mesh):
    model, fsdp_size = mesh.shape["model"], mesh.shape["fsdp"]
    tok_spec = P("fsdp", None)
    row_spec = P(("model", "fsdp"), None)
    weight_spec = P("fsdp", None)
    vmem = pl.BlockSpec(memory_space=pltpu.VMEM)
    hbm = pl.BlockSpec(memory_space=pl.ANY)

    def params(cid):
        return pltpu.CompilerParams(collective_id=cid, has_side_effects=True, vmem_limit_bytes=VMEM_LIMIT)

    def device_step(tok_ids, tok_labels, table_shard, gate_shard, up_shard, down_shard, gain_in, gain_out):
        t = tok_ids.shape[0] * tok_ids.shape[1]
        num_tokens = t * fsdp_size
        real, d = table_shard.shape
        vb = -(-real // 16) * 16
        f = gate_shard.shape[1]
        half_f = f // 2
        cube = Cube(model, t, d)
        last, nb = cube.last, cube.nb
        me, core = lax.axis_index("model"), lax.axis_index("fsdp")
        first = (2 * me + core) * real
        other = (2 * me + 1 - core) * real

        def local_rows(ids):
            flat = ids.reshape(1, t)
            here, there = flat - first, flat - other
            return jnp.where((here >= 0) & (here < real), here, jnp.where((there >= 0) & (there < real), vb + there, -1))

        idx = local_rows(tok_ids)
        lab = local_rows(tok_labels)
        table = jnp.pad(table_shard, ((0, vb - real), (0, 0)))
        g1, g2 = gain_in.reshape(1, d), gain_out.reshape(1, d)
        sds = jax.ShapeDtypeStruct
        dma = pltpu.SemaphoreType.DMA
        hn, ep, xf, wgh, wuh, h_own, gt_own, u_own, x_own = pl.pallas_call(
            functools.partial(embed_kernel, cube, vb),
            out_shape=(
                sds((t, d), BF16),
                sds((2 * vb, d), BF16),
                sds((2 * t, d), BF16),
                sds((d, half_f), BF16),
                sds((d, half_f), BF16),
                sds((last, d), F32),
                sds((2 * last, half_f), BF16),
                sds((2 * last, half_f), BF16),
                sds((last, d), F32),
            ),
            in_specs=[vmem, hbm, hbm, hbm, hbm, vmem, vmem],
            out_specs=(vmem,) * 9,
            scratch_shapes=[pltpu.VMEM((half_f, d), BF16)]
            + cube.group_scratch(BF16) * 4
            + [pltpu.VMEM((t, d), BF16), pltpu.VMEM((2, last, d), BF16), pltpu.VMEM((2, last, d), F32), pltpu.VMEM((last, d), F32)]
            + cube.sems() * 3
            + [dma((6,)), dma((6,)), dma((4,))],
            compiler_params=params(0),
            name="embed",
        )(idx, table, gate_shard, up_shard, down_shard, g1, g2)
        dmf, loss, deh, dh_own = pl.pallas_call(
            functools.partial(head_kernel, cube, vb, real, num_tokens),
            out_shape=(sds((2 * t, d), BF16), sds((8, 128), F32), sds((2 * vb, d), F32), sds((last, d), F32)),
            in_specs=[vmem] * 5,
            out_specs=(vmem,) * 4,
            scratch_shapes=[pltpu.VMEM((2 * vb, t), F32), pltpu.VMEM((2 * vb, t), BF16), pltpu.VMEM((t, d), F32)]
            + cube.group_scratch(F32) * 2
            + cube.group_scratch(BF16)
            + [pltpu.VMEM((cube.axes + 1, 4, 8, t), F32), pltpu.VMEM((2, 8, 128), F32)]
            + cube.sems() * 2
            + [dma((cube.axes, 3)), dma((cube.axes, 3)), dma((2,)), dma((2,))],
            compiler_params=params(1),
            name="head",
        )(hn, ep, lab, h_own, g2)
        de = pl.pallas_call(
            functools.partial(table_kernel, cube, vb),
            out_shape=sds((vb, d), F32),
            in_specs=[vmem] * 10,
            out_specs=vmem,
            scratch_shapes=[
                pltpu.VMEM((2, last, d), BF16),
                pltpu.VMEM((2, last, d), F32),
                pltpu.VMEM((last, d), F32),
                pltpu.VMEM((t, d), F32),
                pltpu.VMEM((2 * vb, d), F32),
                pltpu.VMEM((vb, d), F32),
            ]
            + cube.group_scratch(F32)
            + cube.sems()
            + [dma((3,)), dma((3,))],
            compiler_params=params(2),
            name="table",
        )(idx, dh_own, x_own, gt_own, u_own, wgh, wuh, down_shard, g1, deh)
        normed = rms_scale(xf.astype(F32), gain_in).astype(BF16)
        gate_f = jnp.dot(normed, wgh, preferred_element_type=F32).astype(BF16).astype(F32)
        up_f = jnp.dot(normed, wuh, preferred_element_type=F32).astype(BF16).astype(F32)
        sig = jax.nn.sigmoid(gate_f)
        silu = gate_f * sig
        act = (silu * up_f).astype(BF16)
        d_act = dot(dmf, down_shard, 1, 1)
        grad_down = dot(act, dmf, 0, 0)
        d_gate = (d_act * up_f * (sig * (1.0 + gate_f * (1.0 - sig)))).astype(BF16)
        d_up = (d_act * silu).astype(BF16)
        half_d = d // 2
        a_own = lax.dynamic_slice(normed, (0, core * half_d), (2 * t, half_d))
        a_oth = lax.dynamic_slice(normed, (0, (1 - core) * half_d), (2 * t, half_d))

        def weight_grad(grad):
            got = lax.ppermute(dot(a_oth, grad, 0, 0), "fsdp", [(0, 1), (1, 0)])
            own = dot(a_own, grad, 0, 0)
            out = jnp.zeros((half_d, f), F32)
            out = lax.dynamic_update_slice(out, own, (0, core * half_f))
            return lax.dynamic_update_slice(out, got, (0, (1 - core) * half_f))

        return loss[0, 0], de[:real], weight_grad(d_gate), weight_grad(d_up), grad_down

    return jax.shard_map(device_step, mesh=mesh, in_specs=(tok_spec, tok_spec, row_spec, weight_spec, weight_spec, weight_spec, P(), P()), out_specs=(P(), row_spec, weight_spec, weight_spec, weight_spec), check_vma=False)
```

```python
import functools

import jax
import jax.numpy as jnp
from jax import lax
from jax.experimental import pallas as pl
from jax.experimental.pallas import tpu as pltpu
from jax.sharding import PartitionSpec as P

EPS = 1e-6
MESH = pl.DeviceIdType.MESH
VMEM_LIMIT = 64 * 1024 * 1024 - 64 * 1024
F32 = jnp.float32
BF16 = jnp.bfloat16
COLORS = 3


def dot(a, b, ca, cb):
    return lax.dot_general(a, b, (((ca,), (cb,)), ((), ())), preferred_element_type=F32)


def rms_scale(values, gain):
    mean_sq = jnp.mean(values * values, axis=-1, keepdims=True)
    return values * lax.rsqrt(mean_sq + EPS) * gain


def rms_back(values, gain, grad):
    r = lax.rsqrt(jnp.mean(values * values, axis=-1, keepdims=True) + EPS)
    gg = grad * gain
    return r * gg - values * (r * r * r) * jnp.mean(values * gg, axis=-1, keepdims=True)


class Cube:
    def __init__(self, model, rows, width):
        axes = {4: 1, 16: 2, 64: 3}[model]
        self.axes, self.nb, self.rows = axes, 2 * axes, rows
        self.last = rows >> self.nb
        unit = width // 8 if width % 1024 == 0 else width // 3
        sizes = [3 * unit, 3 * unit, 2 * unit] if width % 1024 == 0 else [unit] * 3
        self.widths = sizes
        self.starts = [0, sizes[0], sizes[0] + sizes[1]]

    def bind(self):
        self.m = lax.axis_index("model")
        self.c = lax.axis_index("fsdp")
        self.digits = [(self.m // 4**a) % 4 for a in range(self.axes)]
        self.partner, self.bit, self.base = [], [], []
        for k in range(COLORS):
            partners, bits, bases = [], [], [0]
            for s in range(self.nb):
                d = (k + s) % self.nb
                a = d % self.axes
                t = (d // self.axes + self.c) % 2
                b = self.digits[a]
                b1, b0 = b // 2, b % 2
                v0, v1 = (b0 + b1) % 2, b1
                bit = v0 + t * (v1 - v0)
                d0, d1 = 1 - 2 * b0, 3 - 2 * b
                partners.append(self.m + 4**a * (d0 + t * (d1 - d0)))
                bits.append(bit)
                bases.append(bases[-1] + bit * (self.rows >> (s + 1)))
            self.partner.append(partners)
            self.bit.append(bits)
            self.base.append(bases)

    def neighbours(self, far):
        out = []
        for a in range(self.axes):
            b = self.digits[a]
            b0 = b % 2
            out.append(self.m + 4**a * (1 - 2 * b0))
            out.append(self.m + 4**a * (3 - 2 * b))
            if far:
                out.append(self.m + 4**a * ((b + 2) % 4 - b))
        return out

    def barrier(self, far=False):
        sem = pltpu.get_barrier_semaphore()
        peers = self.neighbours(far)
        for p in peers:
            pl.semaphore_signal(sem, inc=1, device_id=(p, self.c), device_id_type=MESH)
        pl.semaphore_signal(sem, inc=1, device_id=(self.m, 1 - self.c), device_id_type=MESH)
        pl.semaphore_wait(sem, len(peers) + 1)

    def place(self, k, j):
        pos = []
        for c in range(2):
            p = 0
            for s in range(self.nb):
                d = (k + s) % self.nb
                a = d % self.axes
                t = (d // self.axes + c) % 2
                p |= ((j >> (a + self.axes * t)) & 1) << (self.nb - 1 - s)
            pos.append(p * self.last)
        return pl.multiple_of(pos[0] + self.c * (pos[1] - pos[0]), self.last)

    def rows_at(self, start, size):
        return pl.ds(pl.multiple_of(start, self.last), size)

    def cols(self, k):
        return pl.ds(self.starts[k], self.widths[k])

    def spread(self, nat, bufs):
        for j in range(1 << self.nb):
            for k in range(COLORS):
                bufs[k][pl.ds(self.place(k, j), self.last), :] = nat[pl.ds(j * self.last, self.last), self.cols(k)]

    def collect(self, bufs, nat, offset=0):
        for j in range(1 << self.nb):
            for k in range(COLORS):
                at = pl.ds(j * self.last, self.last) if isinstance(offset, int) and offset == 0 else self.rows_at(offset + j * self.last, self.last)
                nat[at, self.cols(k)] = bufs[k][pl.ds(self.place(k, j), self.last), :]

    def own(self, k):
        return self.rows_at(self.base[k][self.nb], self.last)

    def rs_copy(self, bufs, recvs, send, recv, k, s):
        ln = self.rows >> (s + 1)
        start = self.base[k][s] + (1 - self.bit[k][s]) * ln
        off = self.rows - (self.rows >> s)
        return pltpu.make_async_remote_copy(
            src_ref=bufs[k].at[self.rows_at(start, ln)],
            dst_ref=recvs[k].at[pl.ds(off, ln)],
            send_sem=send.at[k, s],
            recv_sem=recv.at[k, s],
            device_id=(self.partner[k][s], self.c),
            device_id_type=MESH,
        )

    def rs_add(self, bufs, recvs, k, s):
        ln = self.rows >> (s + 1)
        off = self.rows - (self.rows >> s)
        at = self.rows_at(self.base[k][s + 1], ln)
        got = recvs[k][pl.ds(off, ln), :].astype(F32)
        bufs[k][at, :] = (bufs[k][at, :].astype(F32) + got).astype(bufs[k].dtype)

    def reduce_scatter(self, bufs, recvs, send, recv, fill=None):
        for k in range(COLORS):
            self.rs_copy(bufs, recvs, send, recv, k, 0).start()
        for s in range(self.nb):
            if fill is not None:
                fill(s)
            for k in range(COLORS):
                self.rs_copy(bufs, recvs, send, recv, k, s).wait()
                self.rs_add(bufs, recvs, k, s)
                if s + 1 < self.nb:
                    self.rs_copy(bufs, recvs, send, recv, k, s + 1).start()

    def ag_copy(self, bufs, send, recv, k, s):
        ln = self.rows >> (s + 1)
        at = self.rows_at(self.base[k][s + 1], ln)
        return pltpu.make_async_remote_copy(
            src_ref=bufs[k].at[at],
            dst_ref=bufs[k].at[at],
            send_sem=send.at[k, s],
            recv_sem=recv.at[k, s],
            device_id=(self.partner[k][s], self.c),
            device_id_type=MESH,
        )

    def ag_start(self, bufs, send, recv, s):
        for k in range(COLORS):
            self.ag_copy(bufs, send, recv, k, s).start()

    def ag_next(self, bufs, send, recv, s):
        for k in range(COLORS):
            self.ag_copy(bufs, send, recv, k, s).wait()
            if s > 0:
                self.ag_copy(bufs, send, recv, k, s - 1).start()

    def all_gather(self, bufs, send, recv, fill=None):
        self.ag_start(bufs, send, recv, self.nb - 1)
        for s in range(self.nb - 1, -1, -1):
            if fill is not None:
                fill(s)
            self.ag_next(bufs, send, recv, s)

    def pair_copy(self, src, dst, send, recv):
        return pltpu.make_async_remote_copy(
            src_ref=src, dst_ref=dst, send_sem=send, recv_sem=recv, device_id=(self.m, 1 - self.c), device_id_type=MESH
        )

    def group_scratch(self, dtype):
        return [pltpu.VMEM((self.rows, w), dtype) for w in self.widths]

    def sems(self):
        return [pltpu.SemaphoreType.DMA((COLORS, self.nb))] * 2


def embed_kernel(cube, vb, idx, e_ref, wg, wu, wd, g1, g2, hn, ep_o, wgh_o, wuh_o, h_own, gt_own, u_own, x_own, *scratch):
    it = iter(scratch)
    wd_s, ep, wgh, wuh = [next(it) for _ in range(4)]
    xb = [next(it) for _ in range(COLORS)]
    xr = [next(it) for _ in range(COLORS)]
    hb = [next(it) for _ in range(COLORS)]
    xnat, x32, mp, mr = next(it), next(it), next(it), next(it)
    rs_s, rs_r, hg_s, hg_r, psend, precv, lsem = [next(it) for _ in range(7)]
    cube.bind()
    c = cube.c
    d = hn.shape[1]
    half_d, half_f = d // 2, wgh.shape[1]
    last = cube.last
    mine_f = pl.ds(pl.multiple_of(c * half_f, half_f), half_f)
    other_f = pl.ds(pl.multiple_of((1 - c) * half_f, half_f), half_f)
    mine_d = pl.ds(pl.multiple_of(c * half_d, half_d), half_d)
    e_local = pltpu.make_async_copy(e_ref, ep.at[pl.ds(0, vb)], lsem.at[0])
    e_local.start()
    wd_local = pltpu.make_async_copy(wd, wd_s, lsem.at[1])
    wg_local = pltpu.make_async_copy(wg.at[:, mine_f], wgh.at[mine_d], lsem.at[2])
    wu_local = pltpu.make_async_copy(wu.at[:, mine_f], wuh.at[mine_d], lsem.at[3])
    cube.barrier()
    e_pair = cube.pair_copy(e_ref, ep.at[pl.ds(vb, vb)], psend.at[0], precv.at[0])
    e_pair.start()
    wg_pair = cube.pair_copy(wg.at[:, other_f], wgh.at[mine_d], psend.at[1], precv.at[1])
    wu_pair = cube.pair_copy(wu.at[:, other_f], wuh.at[mine_d], psend.at[2], precv.at[2])
    wg_pair.start()
    wu_pair.start()
    wd_local.start()
    wg_local.start()
    wu_local.start()
    e_local.wait()
    e_pair.wait()
    ep_out = pltpu.make_async_copy(ep, ep_o, lsem.at[4])
    ep_out.start()

    chunk = min(256, cube.rows)

    def lookup(i, carry):
        at = pl.ds(pl.multiple_of(i * chunk, chunk), chunk)
        hot = (lax.broadcasted_iota(jnp.int32, (2 * vb, chunk), 0) == idx[:, at]).astype(F32).astype(BF16)
        xnat[at, :] = dot(hot, ep[...], 0, 0).astype(BF16)
        return carry

    lax.fori_loop(0, cube.rows // chunk, lookup, 0)
    cube.spread(xnat, xb)
    cube.reduce_scatter(xb, xr, rs_s, rs_r)
    for k in range(COLORS):
        x32[0, :, cube.cols(k)] = xb[k][cube.own(k), :]
    x_pair = cube.pair_copy(x32.at[0], x32.at[1], psend.at[3], precv.at[3])
    x_pair.start()
    wd_local.wait()
    wg_local.wait()
    wu_local.wait()
    wg_pair.wait()
    wu_pair.wait()
    wg_out = pltpu.make_async_copy(wgh, wgh_o, lsem.at[5])
    wu_out = pltpu.make_async_copy(wuh, wuh_o, lsem.at[6])
    wg_out.start()
    wu_out.start()
    x_pair.wait()
    x_rows = x32[...].reshape(2 * last, d).astype(F32)
    a_rows = rms_scale(x_rows, g1[...]).astype(BF16)
    parts = 4
    fc = half_f // parts
    total = jnp.zeros((2 * last, d), F32)
    for p in range(parts):
        at = pl.ds(p * fc, fc)
        gate = dot(a_rows, wgh[:, at], 1, 0).astype(BF16)
        up = dot(a_rows, wuh[:, at], 1, 0).astype(BF16)
        gt_own[:, at] = gate
        u_own[:, at] = up
        gate_f = gate.astype(F32)
        act = (gate_f * jax.nn.sigmoid(gate_f) * up.astype(F32)).astype(BF16)
        total = total + dot(act, wd_s[at, :], 1, 0)
    mp[...] = total.reshape(2, last, d)
    m_pair = cube.pair_copy(mp.at[1], mr, psend.at[4], precv.at[4])
    m_pair.start()
    m_pair.wait()
    m_rows = (mp[0] + mr[...]).astype(BF16)
    x_own[...] = x32[0]
    h_rows = x32[0].astype(F32) + m_rows.astype(F32)
    h_own[...] = h_rows
    hn_rows = rms_scale(h_rows, g2[...]).astype(BF16)
    for k in range(COLORS):
        hb[k][cube.own(k), :] = hn_rows[:, cube.starts[k] : cube.starts[k] + cube.widths[k]]
    cube.all_gather(hb, hg_s, hg_r)
    cube.collect(hb, hn)
    ep_out.wait()
    wg_out.wait()
    wu_out.wait()


def head_kernel(
    cube, vb, real, num_tokens, parts, hn, ep, lab, h_own, g2, x_own, g1, gt_own, u_own, wgh_i, wuh_i, wd_i,
    dmf, loss, deh, dx_own, at_o, gt_o, u_o, *scratch
):
    it = iter(scratch)
    z, dz, nat = next(it), next(it), next(it)
    rb = [next(it) for _ in range(COLORS)]
    rr = [next(it) for _ in range(COLORS)]
    gb = [next(it) for _ in range(COLORS)]
    xg = [next(it) for _ in range(COLORS)]
    stats, lbuf, dm32, mp, mr = [next(it) for _ in range(5)]
    wgh, wuh, wd, xf, tstage, stage = [next(it) for _ in range(6)]
    rs_s, rs_r, ag_s, ag_r, xg_s, xg_r, st_s, st_r, psend, precv, lsem, tsem, osem = [next(it) for _ in range(13)]
    cube.bind()
    c = cube.c
    t, d = hn.shape
    nb, last = cube.nb, cube.last
    w_copies = [pltpu.make_async_copy(src, dst, lsem.at[i]) for i, (src, dst) in enumerate(((wgh_i, wgh), (wuh_i, wuh), (wd_i, wd)))]
    for copy in w_copies:
        copy.start()
    for k in range(COLORS):
        xg[k][cube.own(k), :] = x_own[:, cube.starts[k] : cube.starts[k] + cube.widths[k]]
    cube.barrier(far=True)
    cube.ag_start(xg, xg_s, xg_r, nb - 1)
    xstep = nb - 1
    chunk = min(256, t)
    chunks = t // chunk

    def logits(i, carry):
        at = pl.ds(pl.multiple_of(i * chunk, chunk), chunk)
        row = lax.broadcasted_iota(jnp.int32, (2 * vb, chunk), 0)
        valid = (row < real) | ((row >= vb) & (row < vb + real))
        zz = dot(ep[...], hn[at, :], 1, 1)
        zz = jnp.where(valid, zz, -1e38)
        z[:, at] = zz
        top = jnp.max(zz, axis=0, keepdims=True)
        mine = cube.digits[0]
        stats[0, mine, 0:1, at] = top
        stats[0, mine, 1:2, at] = jnp.sum(jnp.exp(zz - top), axis=0, keepdims=True)
        stats[0, mine, 2:3, at] = jnp.sum(jnp.where(row == lab[:, at], zz, 0.0), axis=0, keepdims=True)
        return carry

    for i in range(chunks):
        lax.fori_loop(i, i + 1, logits, 0)
        if xstep > 1:
            cube.ag_next(xg, xg_s, xg_r, xstep)
            xstep -= 1
    top = total = label = None
    for a in range(cube.axes):
        b = cube.digits[a]
        copies = []
        for step in range(1, 4):
            peer = cube.m + 4**a * ((b + step) % 4 - b)
            copies.append(
                pltpu.make_async_remote_copy(
                    src_ref=stats.at[a, b],
                    dst_ref=stats.at[a, b],
                    send_sem=st_s.at[a, step - 1],
                    recv_sem=st_r.at[a, step - 1],
                    device_id=(peer, c),
                    device_id_type=MESH,
                )
            )
        for copy in copies:
            copy.start()
        for copy in copies:
            copy.wait()
        top = jnp.maximum(jnp.maximum(stats[a, 0, 0:1, :], stats[a, 1, 0:1, :]), jnp.maximum(stats[a, 2, 0:1, :], stats[a, 3, 0:1, :]))
        total = sum(stats[a, i, 1:2, :] * jnp.exp(stats[a, i, 0:1, :] - top) for i in range(4))
        label = sum(stats[a, i, 2:3, :] for i in range(4))
        nxt = (a + 1, cube.digits[a + 1]) if a + 1 < cube.axes else (a + 1, 0)
        stats[nxt[0], nxt[1], 0:1, :] = top
        stats[nxt[0], nxt[1], 1:2, :] = total
        stats[nxt[0], nxt[1], 2:3, :] = label
    fin = cube.axes
    while xstep > 0:
        cube.ag_next(xg, xg_s, xg_r, xstep)
        xstep -= 1
    tok_loss = jnp.sum(top + jnp.log(total) - label, axis=1, keepdims=True)
    lbuf[c] = jnp.broadcast_to(tok_loss, (8, 128))
    l_pair = cube.pair_copy(lbuf.at[c], lbuf.at[c], psend.at[0], precv.at[0])
    l_pair.start()

    def backward(i, carry):
        at = pl.ds(pl.multiple_of(i * chunk, chunk), chunk)
        row = lax.broadcasted_iota(jnp.int32, (2 * vb, chunk), 0)
        soft = jnp.exp(z[:, at] - stats[fin, 0, 0:1, at]) / stats[fin, 0, 1:2, at]
        dzz = (jnp.where(row == lab[:, at], soft - 1.0, soft) / num_tokens).astype(BF16)
        dz[:, at] = dzz
        nat[at, :] = dot(dzz, ep[...], 0, 0)
        return carry

    lax.fori_loop(0, chunks, backward, 0)
    cube.spread(nat, rb)
    cube.ag_next(xg, xg_s, xg_r, 0)
    mine_t = pl.ds(pl.multiple_of(c * t, t), t)
    xf_pair = cube.pair_copy(xf.at[mine_t], xf.at[mine_t], psend.at[2], precv.at[2])
    fc = wgh.shape[1] // parts
    tile = min(512, 2 * t)

    def out_copy(p, which):
        dst = (gt_o, u_o)[which]
        return pltpu.make_async_copy(stage.at[p % 2, which], dst.at[p], osem.at[which, p])

    def gate_up(p):
        if p >= 2:
            out_copy(p - 2, 0).wait()
            out_copy(p - 2, 1).wait()
        cols = pl.ds(p * fc, fc)

        def body(i, carry):
            at = pl.ds(pl.multiple_of(i * tile, tile), tile)
            stage[p % 2, 0, at, :] = dot(xf[at, :], wgh[:, cols], 1, 0).astype(BF16)
            stage[p % 2, 1, at, :] = dot(xf[at, :], wuh[:, cols], 1, 0).astype(BF16)
            return carry

        lax.fori_loop(0, 2 * t // tile, body, 0)
        out_copy(p, 0).start()
        out_copy(p, 1).start()

    def normalise():
        def body(i, carry):
            at = pl.ds(pl.multiple_of(i * chunk, chunk), chunk)
            val = rms_scale(xf[at, :].astype(F32), g1[...])
            xf[at, :] = val.astype(BF16)
            tstage[:, at] = val.T.astype(BF16)
            return carry

        lax.fori_loop(0, 2 * t // chunk, body, 0)

    t_out = pltpu.make_async_copy(tstage, at_o, tsem)
    todo = list(range(parts))

    def run(n):
        for _ in range(min(n, len(todo))):
            gate_up(todo.pop(0))

    def rs_fill(s):
        if s == 0:
            cube.collect(xg, xf, c * t)
            xf_pair.start()
            rows = vb

            def head_grad(i, carry):
                at = pl.ds(pl.multiple_of(i * rows, rows), rows)
                deh[at, :] = dot(dz[at, :], hn[...], 1, 0)
                return carry

            lax.fori_loop(0, 2, head_grad, 0)
            xf_pair.wait()
            normalise()
            t_out.start()
            for copy in w_copies:
                copy.wait()
        elif s == 1:
            run(2)
        elif s <= 4:
            run(1)

    cube.reduce_scatter(rb, rr, rs_s, rs_r, rs_fill)
    dhn = jnp.concatenate([rb[k][cube.own(k), :] for k in range(COLORS)], axis=1)
    dh = rms_back(h_own[...], g2[...], dhn)
    dm = dh.astype(BF16)
    for k in range(COLORS):
        gb[k][cube.own(k), :] = dm[:, cube.starts[k] : cube.starts[k] + cube.widths[k]]
    dm32[0] = dm
    d_pair = cube.pair_copy(dm32.at[0], dm32.at[1], psend.at[3], precv.at[3])
    m_pair = cube.pair_copy(mp.at[1], mr, psend.at[4], precv.at[4])

    def token_part(p, n):
        w = wgh.shape[1] // n
        at = pl.ds(p * w, w)
        d_act = dot(dm32[...].reshape(2 * last, d), wd[at, :], 1, 1)
        gate = gt_own[:, at].astype(F32)
        sig = jax.nn.sigmoid(gate)
        d_gate = (d_act * u_own[:, at].astype(F32) * (sig * (1.0 + gate * (1.0 - sig)))).astype(BF16)
        d_up = (d_act * (gate * sig)).astype(BF16)
        part = (dot(d_gate, wgh[:, at], 1, 1) + dot(d_up, wuh[:, at], 1, 1)).reshape(2, last, d)
        if p == 0:
            mp[...] = part
        else:
            mp[...] = mp[...] + part

    def ag_fill(s):
        done = nb - 1 - s
        if done == 0:
            d_pair.wait()
            token_part(0, 4)
        elif done == 1:
            token_part(1, 4)
        elif done == 2:
            token_part(2, 4)
        elif done == 3:
            token_part(3, 4)
            m_pair.start()
        elif done == 4:
            run(1)
        else:
            run(2)

    d_pair.start()
    cube.all_gather(gb, ag_s, ag_r, ag_fill)
    if nb < 6:
        for p in range(nb, 4):
            token_part(p, 4)
        if nb < 4:
            m_pair.start()
    cube.collect(gb, dmf, c * cube.rows)
    dm_pair = cube.pair_copy(dmf.at[mine_t], dmf.at[mine_t], psend.at[1], precv.at[1])
    dm_pair.start()
    run(parts)
    m_pair.wait()
    dx_own[...] = dh + rms_back(x_own[...].astype(F32), g1[...], mp[0] + mr[...])
    l_pair.wait()
    loss[...] = (lbuf[0] + lbuf[1]) / num_tokens
    t_out.wait()
    for p in range(parts - 2, parts):
        out_copy(p, 0).wait()
        out_copy(p, 1).wait()
    dm_pair.wait()


def table_kernel(
    cube, vb, parts, idx, dx_own, dmf, wd, deh, at_i, gt_i, u_i,
    de, act_o, dg_o, du_o, got_g, got_u, *scratch
):
    it = iter(scratch)
    nat, mix, de_r, aoth, fin, fout, part = [next(it) for _ in range(7)]
    gb = [next(it) for _ in range(COLORS)]
    ag_s, ag_r, psend, precv, lsem, isem, osem, gsend, grecv = [next(it) for _ in range(9)]
    cube.bind()
    c = cube.c
    t = cube.rows
    nb = cube.nb
    d = dx_own.shape[1]
    half_d = d // 2
    fc = wd.shape[0] // parts
    a_copy = pltpu.make_async_copy(at_i.at[pl.ds(pl.multiple_of((1 - c) * half_d, half_d), half_d)], aoth, lsem)
    a_copy.start()

    def in_copy(p, which):
        return pltpu.make_async_copy((gt_i, u_i)[which].at[p], fin.at[p % 2, which], isem.at[which, p])

    def out_copy(p, which):
        return pltpu.make_async_copy(fout.at[p % 2, which], (act_o, dg_o, du_o)[which].at[p], osem.at[which, p])

    def send_copy(p, which):
        return cube.pair_copy(part.at[p % 2, which], (got_g, got_u)[which].at[p], gsend.at[which, p], grecv.at[which, p])

    in_copy(0, 0).start()
    in_copy(0, 1).start()
    for k in range(COLORS):
        gb[k][cube.own(k), :] = dx_own[:, cube.starts[k] : cube.starts[k] + cube.widths[k]]
    cube.barrier()
    cube.ag_start(gb, ag_s, ag_r, nb - 1)
    step = nb - 1
    mix[...] = deh[...]
    a_copy.wait()
    tile = min(512, 2 * t)
    for p in range(parts):
        if p + 1 < parts:
            in_copy(p + 1, 0).start()
            in_copy(p + 1, 1).start()
        in_copy(p, 0).wait()
        in_copy(p, 1).wait()
        slot = p % 2
        if p >= 2:
            for which in range(3):
                out_copy(p - 2, which).wait()
            for which in range(2):
                send_copy(p - 2, which).wait_send()

        def body(i, carry):
            at = pl.ds(pl.multiple_of(i * tile, tile), tile)
            d_act = dot(dmf[at, :], wd[pl.ds(p * fc, fc), :], 1, 1)
            gate = fin[slot, 0, at, :].astype(F32)
            up = fin[slot, 1, at, :].astype(F32)
            sig = jax.nn.sigmoid(gate)
            silu = gate * sig
            fout[slot, 0, at, :] = (silu * up).astype(BF16)
            fout[slot, 1, at, :] = (d_act * up * (sig * (1.0 + gate * (1.0 - sig)))).astype(BF16)
            fout[slot, 2, at, :] = (d_act * silu).astype(BF16)
            return carry

        lax.fori_loop(0, 2 * t // tile, body, 0)
        part[slot, 0] = dot(aoth[...], fout[slot, 1], 1, 0)
        part[slot, 1] = dot(aoth[...], fout[slot, 2], 1, 0)
        for which in range(3):
            out_copy(p, which).start()
        for which in range(2):
            send_copy(p, which).start()
        if step > 0 and (p < 4 or p == 5 or nb < 6):
            cube.ag_next(gb, ag_s, ag_r, step)
            step -= 1
    while step >= 0:
        cube.ag_next(gb, ag_s, ag_r, step)
        step -= 1
    cube.collect(gb, nat)
    chunk = min(256, t)

    def scatter(i, carry):
        at = pl.ds(pl.multiple_of(i * chunk, chunk), chunk)
        hot = (lax.broadcasted_iota(jnp.int32, (2 * vb, chunk), 0) == idx[:, at]).astype(F32).astype(BF16)
        val = nat[at, :]
        hi = val.astype(BF16)
        rest = val - hi.astype(F32)
        mid = rest.astype(BF16)
        low = (rest - mid.astype(F32)).astype(BF16)
        mix[...] = mix[...] + ((dot(hot, low, 1, 0) + dot(hot, mid, 1, 0)) + dot(hot, hi, 1, 0))
        return carry

    lax.fori_loop(0, t // chunk, scatter, 0)
    e_pair = cube.pair_copy(mix.at[pl.ds(vb, vb)], de_r, psend.at[0], precv.at[0])
    e_pair.start()
    for p in range(parts - 2, parts):
        for which in range(3):
            out_copy(p, which).wait()
        for which in range(2):
            send_copy(p, which).wait_send()
    for p in range(parts):
        for which in range(2):
            send_copy(p, which).wait_recv()
    e_pair.wait()
    de[...] = mix[pl.ds(0, vb), :] + de_r[...]


def weight_kernel(core, aown, dg, du, act, dmf, got_g, got_u, og, ou, od):
    even = pl.program_id(0) % 2 == 0

    @pl.when(even)
    def _():
        og[...] = dot(aown[...], dg[0], 1, 0)
        ou[...] = dot(aown[...], du[0], 1, 0)

    @pl.when(jnp.logical_not(even))
    def _():
        og[...] = got_g[0]
        ou[...] = got_u[0]
        od[...] = dot(act[0], dmf[...], 0, 0)


def solution(mesh):
    model, fsdp_size = mesh.shape["model"], mesh.shape["fsdp"]
    tok_spec = P("fsdp", None)
    row_spec = P(("model", "fsdp"), None)
    weight_spec = P("fsdp", None)
    vmem = pl.BlockSpec(memory_space=pltpu.VMEM)
    hbm = pl.BlockSpec(memory_space=pl.ANY)
    parts = 8

    def params(cid):
        return pltpu.CompilerParams(collective_id=cid, has_side_effects=True, vmem_limit_bytes=VMEM_LIMIT)

    def device_step(tok_ids, tok_labels, table_shard, gate_shard, up_shard, down_shard, gain_in, gain_out):
        t = tok_ids.shape[0] * tok_ids.shape[1]
        num_tokens = t * fsdp_size
        real, d = table_shard.shape
        vb = -(-real // 16) * 16
        f = gate_shard.shape[1]
        half_f, half_d = f // 2, d // 2
        fc = half_f // parts
        cube = Cube(model, t, d)
        last = cube.last
        me, core = lax.axis_index("model"), lax.axis_index("fsdp")
        first = (2 * me + core) * real
        other = (2 * me + 1 - core) * real

        def local_rows(ids):
            flat = ids.reshape(1, t)
            here, there = flat - first, flat - other
            return jnp.where((here >= 0) & (here < real), here, jnp.where((there >= 0) & (there < real), vb + there, -1))

        idx = local_rows(tok_ids)
        lab = local_rows(tok_labels)
        table = jnp.pad(table_shard, ((0, vb - real), (0, 0)))
        g1, g2 = gain_in.reshape(1, d), gain_out.reshape(1, d)
        sds = jax.ShapeDtypeStruct
        dma = pltpu.SemaphoreType.DMA
        hn, ep, wgh, wuh, h_own, gt_own, u_own, x_own = pl.pallas_call(
            functools.partial(embed_kernel, cube, vb),
            out_shape=(
                sds((t, d), BF16),
                sds((2 * vb, d), BF16),
                sds((d, half_f), BF16),
                sds((d, half_f), BF16),
                sds((last, d), F32),
                sds((2 * last, half_f), BF16),
                sds((2 * last, half_f), BF16),
                sds((last, d), BF16),
            ),
            in_specs=[vmem, hbm, hbm, hbm, hbm, vmem, vmem],
            out_specs=(vmem, hbm, hbm, hbm, vmem, vmem, vmem, vmem),
            scratch_shapes=[pltpu.VMEM((half_f, d), BF16), pltpu.VMEM((2 * vb, d), BF16), pltpu.VMEM((d, half_f), BF16), pltpu.VMEM((d, half_f), BF16)]
            + cube.group_scratch(BF16) * 3
            + [pltpu.VMEM((t, d), BF16), pltpu.VMEM((2, last, d), BF16), pltpu.VMEM((2, last, d), F32), pltpu.VMEM((last, d), F32)]
            + cube.sems() * 2
            + [dma((5,)), dma((5,)), dma((7,))],
            compiler_params=params(0),
            name="embed",
        )(idx, table, gate_shard, up_shard, down_shard, g1, g2)
        dmf, loss, deh, dx_own, a_t, gt, u = pl.pallas_call(
            functools.partial(head_kernel, cube, vb, real, num_tokens, parts),
            out_shape=(
                sds((2 * t, d), BF16),
                sds((8, 128), F32),
                sds((2 * vb, d), F32),
                sds((last, d), F32),
                sds((d, 2 * t), BF16),
                sds((parts, 2 * t, fc), BF16),
                sds((parts, 2 * t, fc), BF16),
            ),
            in_specs=[vmem] * 9 + [hbm] * 3,
            out_specs=(vmem,) * 4 + (hbm,) * 3,
            scratch_shapes=[pltpu.VMEM((2 * vb, t), F32), pltpu.VMEM((2 * vb, t), BF16), pltpu.VMEM((t, d), F32)]
            + cube.group_scratch(F32) * 2
            + cube.group_scratch(BF16) * 2
            + [pltpu.VMEM((cube.axes + 1, 4, 8, t), F32), pltpu.VMEM((2, 8, 128), F32)]
            + [pltpu.VMEM((2, last, d), BF16), pltpu.VMEM((2, last, d), F32), pltpu.VMEM((last, d), F32)]
            + [pltpu.VMEM((d, half_f), BF16), pltpu.VMEM((d, half_f), BF16), pltpu.VMEM((half_f, d), BF16)]
            + [pltpu.VMEM((2 * t, d), BF16), pltpu.VMEM((d, 2 * t), BF16), pltpu.VMEM((2, 2, 2 * t, fc), BF16)]
            + cube.sems() * 3
            + [dma((cube.axes, 3)), dma((cube.axes, 3)), dma((5,)), dma((5,)), dma((3,)), dma, dma((2, parts))],
            compiler_params=params(1),
            name="head",
        )(hn, ep, lab, h_own, g2, x_own, g1, gt_own, u_own, wgh, wuh, down_shard)
        chunked = sds((parts, 2 * t, fc), BF16)
        got = sds((parts, half_d, fc), F32)
        de, act, d_gate, d_up, got_g, got_u = pl.pallas_call(
            functools.partial(table_kernel, cube, vb, parts),
            out_shape=(sds((vb, d), F32), chunked, chunked, chunked, got, got),
            in_specs=[vmem] * 5 + [hbm] * 3,
            out_specs=(vmem,) + (hbm,) * 5,
            scratch_shapes=[
                pltpu.VMEM((t, d), F32),
                pltpu.VMEM((2 * vb, d), F32),
                pltpu.VMEM((vb, d), F32),
                pltpu.VMEM((half_d, 2 * t), BF16),
                pltpu.VMEM((2, 2, 2 * t, fc), BF16),
                pltpu.VMEM((2, 3, 2 * t, fc), BF16),
                pltpu.VMEM((2, 2, half_d, fc), F32),
            ]
            + cube.group_scratch(F32)
            + cube.sems()
            + [dma((1,)), dma((1,)), dma, dma((2, parts)), dma((3, parts)), dma((2, parts)), dma((2, parts))],
            compiler_params=params(2),
            name="table",
        )(idx, dx_own, dmf, down_shard, deh, a_t, gt, u)
        chunk_spec = pl.BlockSpec((1, 2 * t, fc), lambda i, s: (i // 2, 0, 0))
        got_spec = pl.BlockSpec((1, half_d, fc), lambda i, s: (i // 2, 0, 0))
        grad_spec = pl.BlockSpec((half_d, fc), lambda i, s: (0, (s[0] + i % 2) % 2 * parts + i // 2))
        grad_gate, grad_up, grad_down = pl.pallas_call(
            weight_kernel,
            out_shape=(sds((half_d, f), F32), sds((half_d, f), F32), sds((half_f, d), F32)),
            grid_spec=pltpu.PrefetchScalarGridSpec(
                num_scalar_prefetch=1,
                grid=(2 * parts,),
                in_specs=[
                    pl.BlockSpec((half_d, 2 * t), lambda i, s: (s[0], 0)),
                    chunk_spec,
                    chunk_spec,
                    chunk_spec,
                    pl.BlockSpec((2 * t, d), lambda i, s: (0, 0)),
                    got_spec,
                    got_spec,
                ],
                out_specs=(grad_spec, grad_spec, pl.BlockSpec((fc, d), lambda i, s: (i // 2, 0))),
            ),
            compiler_params=pltpu.CompilerParams(vmem_limit_bytes=VMEM_LIMIT),
            name="weights",
        )(core.reshape(1).astype(jnp.int32), a_t, d_gate, d_up, act, dmf, got_g, got_u)
        return loss[0, 0], de[:real], grad_gate, grad_up, grad_down

    return jax.shard_map(device_step, mesh=mesh, in_specs=(tok_spec, tok_spec, row_spec, weight_spec, weight_spec, weight_spec, P(), P()), out_specs=(P(), row_spec, weight_spec, weight_spec, weight_spec), check_vma=False)
```

```python
import functools
import itertools

import jax
import jax.numpy as jnp
from jax import lax
from jax.experimental import pallas as pl
from jax.experimental.pallas import tpu as pltpu
from jax.sharding import PartitionSpec as P

EPS = 1e-6
MESH = pl.DeviceIdType.MESH
VMEM_LIMIT = 67043328
F32 = jnp.float32
BF16 = jnp.bfloat16
COLORS = 3
DIRECT = 3
PARTS = 8
RING = 4
TOP, SUM, LABEL = range(3)


def contract(a, b, dims):
    return lax.dot_general(a, b, (dims, ((), ())), preferred_element_type=F32)


def nn(a, b):
    return contract(a, b, ((1,), (0,)))


def nt(a, b):
    return contract(a, b, ((1,), (1,)))


def tn(a, b):
    return contract(a, b, ((0,), (0,)))


def span(i, n):
    return pl.ds(pl.multiple_of(i * n, n), n)


def loop(lo, hi, body):
    def step(i, carry):
        body(i)
        return carry

    lax.fori_loop(lo, hi, step, 0)


def mean(v):
    return jnp.mean(v, axis=-1, keepdims=True)


def rms_scale(values, gain):
    return values * lax.rsqrt(mean(values * values) + EPS) * gain


def rms_back(values, gain, grad):
    r = lax.rsqrt(mean(values * values) + EPS)
    gg = grad * gain
    return r * gg - values * (r * r * r) * mean(values * gg)


def one_hot(rows, ids):
    return (lax.broadcasted_iota(jnp.int32, (rows, ids.shape[-1]), 0) == ids).astype(F32).astype(BF16)


class Local:
    def __init__(self, sems):
        self.sems, self.free = sems, itertools.count()

    def __call__(self, src, dst):
        return pltpu.make_async_copy(src, dst, self.sems.at[next(self.free)])


class Cube:
    def __init__(self, model, rows, width):
        axes = 1
        while RING**axes < model:
            axes += 1
        self.axes, self.nb, self.rows = axes, 2 * axes, rows
        self.direct = min(DIRECT, self.nb - 1)
        self.walk = self.nb - self.direct
        self.peers = 2**self.direct - 1
        self.last = rows >> self.nb
        tiles = width // 128
        big = -(-tiles // COLORS) * 128
        self.widths = [big, big, width - 2 * big]
        self.starts = [0, big, 2 * big]

    def dim(self, k, s):
        d = (k + s) % self.nb
        return d % self.axes, d // self.axes

    def bind(self, psend=None, precv=None):
        self.m = lax.axis_index("model")
        self.c = lax.axis_index("fsdp")
        self.psend, self.precv, self.free = psend, precv, itertools.count()
        self.digits = [(self.m // RING**a) % RING for a in range(self.axes)]
        self.bit, self.base = [], []
        for k in range(COLORS):
            bits, bases = [], [0]
            for s in range(self.nb):
                a, kind = self.dim(k, s)
                b = self.digits[a]
                v0, v1 = (b % 2 + b // 2) % 2, b // 2
                bits.append(v0 + ((kind + self.c) % 2) * (v1 - v0))
                bases.append(bases[-1] + bits[-1] * (self.rows >> len(bits)))
            self.bit.append(bits)
            self.base.append(bases)

    def toggled(self, k, steps):
        digits = list(self.digits)
        for s in steps:
            a, kind = self.dim(k, s)
            near = 1 - 2 * (digits[a] % 2)
            digits[a] = digits[a] + near + ((kind + self.c) % 2) * (RING - 1 - 2 * digits[a] - near)
        return sum(v * RING**a for a, v in enumerate(digits))

    def group(self, q):
        return [self.walk + i for i in range(self.direct) if (q >> i) % 2]

    def ring_peer(self, a, step):
        b = self.digits[a]
        return self.m + RING**a * ((b + step) % RING - b)

    def barrier(self, rings=False):
        sem = pltpu.get_barrier_semaphore()
        peers = [(self.m, 1 - self.c)]
        for k in range(COLORS):
            steps = [[s] for s in range(self.walk)] + [self.group(q + 1) for q in range(self.peers)]
            peers += [(self.toggled(k, st), self.c) for st in steps]
        if rings:
            peers += [(self.ring_peer(a, step), self.c) for a in range(self.axes) for step in range(1, RING)]
        for peer in peers:
            pl.semaphore_signal(sem, inc=1, device_id=peer, device_id_type=MESH)
        pl.semaphore_wait(sem, len(peers))

    def place(self, k, j):
        pos = []
        for c in range(2):
            p = 0
            for s in range(self.nb):
                a, kind = self.dim(k, s)
                p = 2 * p + (j >> (a + self.axes * ((kind + c) % 2))) % 2
            pos.append(p * self.last)
        return self.rows_at(pos[0] + self.c * (pos[1] - pos[0]), self.last)

    def rows_at(self, start, size):
        return pl.ds(pl.multiple_of(start, self.last), size)

    def cols(self, k):
        return pl.ds(self.starts[k], self.widths[k])

    def pieces(self):
        return itertools.product(range(2**self.nb), range(COLORS))

    def spread(self, nat, bufs):
        for j, k in self.pieces():
            bufs[k][self.place(k, j), :] = nat[span(j, self.last), self.cols(k)]

    def collect(self, bufs, nat, half=None):
        start = 0 if half is None else half * self.rows
        for j, k in self.pieces():
            nat[self.rows_at(start + j * self.last, self.last), self.cols(k)] = bufs[k][self.place(k, j), :]

    def own(self, k):
        return self.rows_at(self.base[k][-1], self.last)

    def put_own(self, bufs, value):
        for k in range(COLORS):
            bufs[k][self.own(k), :] = value[:, self.starts[k] : self.starts[k] + self.widths[k]]

    def get_own(self, bufs):
        return jnp.concatenate([bufs[k][self.own(k), :] for k in range(COLORS)], axis=1)

    def send(self, src, dst, sems, index, peer):
        return pltpu.make_async_remote_copy(
            src_ref=src, dst_ref=dst, send_sem=sems[0].at[index], recv_sem=sems[1].at[index], device_id=(peer, self.c), device_id_type=MESH
        )

    def rs_copies(self, bufs, recvs, sems, k, s):
        if s < self.walk:
            ln = self.rows >> (s + 1)
            start = self.base[k][s] + (1 - self.bit[k][s]) * ln
            off = self.rows - (self.rows >> s)
            peer = self.toggled(k, [s])
            return [self.send(bufs[k].at[self.rows_at(start, ln)], recvs[k].at[pl.ds(off, ln)], sems, (k, s), peer)]
        out = []
        for q in range(self.peers):
            steps = self.group(q + 1)
            start = self.base[k][-1] + sum((1 - 2 * self.bit[k][st]) * (self.rows >> (st + 1)) for st in steps)
            src = bufs[k].at[self.rows_at(start, self.last)]
            out.append(self.send(src, recvs[k].at[self.slot(q)], sems, (k, s + q), self.toggled(k, steps)))
        return out

    def slot(self, q):
        return pl.ds(self.rows - (self.rows >> self.walk) + q * self.last, self.last)

    def rs_add(self, bufs, recvs, k, s):
        if s < self.walk:
            ln = self.rows >> (s + 1)
            at = self.rows_at(self.base[k][s + 1], ln)
            got = recvs[k][pl.ds(self.rows - (self.rows >> s), ln), :].astype(F32)
        else:
            at = self.own(k)
            got = sum(recvs[k][self.slot(q), :].astype(F32) for q in range(self.peers))
        bufs[k][at, :] = (bufs[k][at, :].astype(F32) + got).astype(bufs[k].dtype)

    def reduce_scatter(self, bufs, recvs, sems, fill=None):
        for k in range(COLORS):
            self.start(self.rs_copies(bufs, recvs, sems, k, 0))
        for s in range(self.walk + 1):
            if fill is not None:
                fill(s)
            for k in range(COLORS):
                self.finish(self.rs_copies(bufs, recvs, sems, k, s))
                self.rs_add(bufs, recvs, k, s)
                if s < self.walk:
                    self.start(self.rs_copies(bufs, recvs, sems, k, s + 1))

    def start(self, copies):
        for copy in copies:
            copy.start()

    def finish(self, copies):
        for copy in copies:
            copy.wait()

    def ag_copies(self, bufs, sems, k, s):
        if s == self.walk:
            ref = bufs[k].at[self.own(k)]
            return [self.send(ref, ref, sems, (k, s + q), self.toggled(k, self.group(q + 1))) for q in range(self.peers)]
        ref = bufs[k].at[self.rows_at(self.base[k][s + 1], self.rows >> (s + 1))]
        return [self.send(ref, ref, sems, (k, s), self.toggled(k, [s]))]

    def ag_start(self, bufs, sems):
        for k in range(COLORS):
            self.start(self.ag_copies(bufs, sems, k, self.walk))
        return self.walk

    def ag_next(self, bufs, sems, s):
        for k in range(COLORS):
            self.finish(self.ag_copies(bufs, sems, k, s))
            if s > 0:
                self.start(self.ag_copies(bufs, sems, k, s - 1))
        return s - 1

    def all_gather(self, bufs, sems, fill=None):
        s = self.ag_start(bufs, sems)
        while s >= 0:
            if fill is not None:
                fill(s)
            s = self.ag_next(bufs, sems, s)

    def pair(self, src, dst):
        i = next(self.free)
        return pltpu.make_async_remote_copy(
            src_ref=src, dst_ref=dst, send_sem=self.psend.at[i], recv_sem=self.precv.at[i], device_id=(self.m, 1 - self.c), device_id_type=MESH
        )

    def groups(self, *dtypes):
        return [pltpu.VMEM((self.rows, w), dtype) for dtype in dtypes for w in self.widths]

    def sems(self, n):
        return [pltpu.SemaphoreType.DMA((COLORS, self.walk + self.peers))] * (2 * n)


def by(n, items):
    return [items[i : i + n] for i in range(0, len(items), n)]


def embed_kernel(cube, vb, idx, e_ref, wg, wu, wd, g1, g2, hn, ep_o, wgh_o, wuh_o, h_own, gt_own, u_own, x_own, *scratch):
    wd_s, ep, wgh, wuh, xnat, x32, mp, mr, psend, precv, lsem, *rest = scratch
    xb, xr, hb = by(COLORS, rest[: 3 * COLORS])
    rs_sems, hg_sems = by(2, rest[3 * COLORS :])
    cube.bind(psend, precv)
    local = Local(lsem)
    c = cube.c
    d = hn.shape[1]
    half_d, half_f = d // 2, wgh.shape[1]
    last = cube.last
    mine_d = span(c, half_d)
    e_local = local(e_ref, ep.at[pl.ds(0, vb)])
    e_local.start()
    w_local = [local(wd, wd_s), local(wg.at[:, span(c, half_f)], wgh.at[mine_d]), local(wu.at[:, span(c, half_f)], wuh.at[mine_d])]
    cube.barrier()
    e_pair = cube.pair(e_ref, ep.at[pl.ds(vb, vb)])
    e_pair.start()
    w_pair = [cube.pair(src.at[:, span(1 - c, half_f)], dst.at[mine_d]) for src, dst in ((wg, wgh), (wu, wuh))]
    cube.start(w_pair + w_local)
    cube.finish([e_local, e_pair])
    outs = [local(ep, ep_o), local(wgh, wgh_o), local(wuh, wuh_o)]
    outs[0].start()
    chunk = min(256, cube.rows)

    def lookup(i):
        at = span(i, chunk)
        xnat[at, :] = tn(one_hot(2 * vb, idx[:, at]), ep[...]).astype(BF16)

    loop(0, cube.rows // chunk, lookup)
    cube.spread(xnat, xb)
    cube.reduce_scatter(xb, xr, rs_sems)
    x_own[...] = cube.get_own(xb)
    x32[0] = x_own[...]
    x_pair = cube.pair(x32.at[0], x32.at[1])
    x_pair.start()
    cube.finish(w_local + w_pair)
    cube.start(outs[1:])
    x_pair.wait()
    a_rows = rms_scale(x32[...].reshape(2 * last, d).astype(F32), g1[...]).astype(BF16)
    parts = 4
    fc = half_f // parts
    total = jnp.zeros((2 * last, d), F32)
    for p in range(parts):
        at = pl.ds(p * fc, fc)
        gate = nn(a_rows, wgh[:, at]).astype(BF16)
        up = nn(a_rows, wuh[:, at]).astype(BF16)
        gt_own[:, at] = gate
        u_own[:, at] = up
        gate_f = gate.astype(F32)
        act = (gate_f * jax.nn.sigmoid(gate_f) * up.astype(F32)).astype(BF16)
        total = total + nn(act, wd_s[at, :])
    mp[...] = total.reshape(2, last, d)
    m_pair = cube.pair(mp.at[1], mr)
    m_pair.start()
    m_pair.wait()
    h_rows = x_own[...].astype(F32) + (mp[0] + mr[...]).astype(BF16).astype(F32)
    h_own[...] = h_rows
    cube.put_own(hb, rms_scale(h_rows, g2[...]).astype(BF16))
    cube.all_gather(hb, hg_sems)
    cube.collect(hb, hn)
    cube.finish(outs)


def head_kernel(
    cube, vb, real, num_tokens, hn, ep, lab, h_own, g2, x_own, g1, gt_own, u_own, wgh_i, wuh_i, wd_i,
    dmf, loss, deh, dx_own, at_o, gt_o, u_o, *scratch
):
    z, dz, nat, stats, lbuf, dm32, mp, mr, wgh, wuh, wd, xf, tstage, stage, psend, precv, lsem, osem, st_s, st_r, *rest = scratch
    rb, rr, gb, xg = by(COLORS, rest[: 4 * COLORS])
    rs_sems, ag_sems, xg_sems = by(2, rest[4 * COLORS :])
    cube.bind(psend, precv)
    local = Local(lsem)
    c = cube.c
    t, d = hn.shape
    walk, last = cube.walk, cube.last
    w_copies = [local(wgh_i, wgh), local(wuh_i, wuh), local(wd_i, wd)]
    cube.start(w_copies)
    cube.put_own(xg, x_own[...])
    cube.barrier(rings=True)
    xstep = cube.ag_start(xg, xg_sems)
    chunk = min(256, t)
    chunks = t // chunk
    mine = cube.digits[0]

    def logits(i):
        at = span(i, chunk)
        row = lax.broadcasted_iota(jnp.int32, (2 * vb, chunk), 0)
        valid = (row < real) | ((row >= vb) & (row < vb + real))
        zz = jnp.where(valid, nt(ep[...], hn[at, :]), -1e38)
        z[:, at] = zz
        top = jnp.max(zz, axis=0, keepdims=True)
        parts = {TOP: top, SUM: jnp.exp(zz - top), LABEL: jnp.where(row == lab[:, at], zz, 0.0)}
        for r, v in parts.items():
            stats[0, mine, pl.ds(r, 1), at] = v if r == TOP else jnp.sum(v, axis=0, keepdims=True)

    loop(0, chunks, logits)
    xstep = cube.ag_next(xg, xg_sems, xstep)
    for a in range(cube.axes):
        here = stats.at[a, cube.digits[a]]
        copies = [cube.send(here, here, (st_s, st_r), (a, step - 1), cube.ring_peer(a, step)) for step in range(1, RING)]
        cube.start(copies)
        cube.finish(copies)
        if xstep > 1:
            xstep = cube.ag_next(xg, xg_sems, xstep)
        tops, sums, labels = [[stats[a, i, pl.ds(r, 1), :] for i in range(RING)] for r in range(LABEL + 1)]
        top = functools.reduce(jnp.maximum, tops)
        total = sum(v * jnp.exp(m - top) for m, v in zip(tops, sums))
        label = sum(labels)
        slot = cube.digits[a + 1] if a + 1 < cube.axes else 0
        for r, v in enumerate((top, total, label)):
            stats[a + 1, slot, pl.ds(r, 1), :] = v
    while xstep > 0:
        xstep = cube.ag_next(xg, xg_sems, xstep)
    tok_loss = jnp.sum(top + jnp.log(total) - label, axis=1, keepdims=True)
    lbuf[c] = jnp.broadcast_to(tok_loss, lbuf.shape[1:])
    l_pair = cube.pair(lbuf.at[c], lbuf.at[c])
    l_pair.start()
    final = stats.at[cube.axes, 0]

    def backward(i):
        at = span(i, chunk)
        row = lax.broadcasted_iota(jnp.int32, (2 * vb, chunk), 0)
        soft = jnp.exp(z[:, at] - final[pl.ds(TOP, 1), at]) / final[pl.ds(SUM, 1), at]
        dzz = (jnp.where(row == lab[:, at], soft - 1.0, soft) / num_tokens).astype(BF16)
        dz[:, at] = dzz
        nat[at, :] = tn(dzz, ep[...])

    loop(0, chunks, backward)
    cube.spread(nat, rb)
    mine_t = span(c, t)
    xf_pair = cube.pair(xf.at[mine_t], xf.at[mine_t])
    dm_pair = cube.pair(dmf.at[mine_t], dmf.at[mine_t])
    d_pair = cube.pair(dm32.at[0], dm32.at[1])
    m_pair = cube.pair(mp.at[1], mr)
    t_out = local(tstage, at_o)
    fc = wgh.shape[1] // PARTS
    tile = min(512, 2 * t)

    def out_copies(p):
        return [pltpu.make_async_copy(stage.at[p % 2, i], dst.at[p], osem.at[i, p]) for i, dst in enumerate((gt_o, u_o))]

    def gate_up(p):
        if p >= 2:
            cube.finish(out_copies(p - 2))
        cols = pl.ds(p * fc, fc)
        slot = stage.at[p % 2]

        def body(i):
            at = span(i, tile)
            for which, w in enumerate((wgh, wuh)):
                slot[which, at, :] = nn(xf[at, :], w[:, cols]).astype(BF16)

        loop(0, 2 * t // tile, body)
        cube.start(out_copies(p))

    def normalise():
        def body(i):
            at = span(i, chunk)
            val = rms_scale(xf[at, :].astype(F32), g1[...])
            xf[at, :] = val.astype(BF16)
            tstage[:, at] = val.T.astype(BF16)

        loop(0, 2 * chunks, body)

    def head_grad(i):
        deh[span(i, vb), :] = nn(dz[span(i, vb), :], hn[...])

    todo = list(range(PARTS))

    def run(n):
        while n > 0 and todo:
            gate_up(todo.pop(0))
            n -= 1

    def rs_fill(s):
        if s == 0:
            loop(0, 2, head_grad)
            cube.ag_next(xg, xg_sems, xstep)
            cube.collect(xg, xf, c)
            xf_pair.start()
            cube.finish(w_copies + [xf_pair])
            normalise()
            t_out.start()
            run(1)
        else:
            run(walk + 1 - s)

    cube.reduce_scatter(rb, rr, rs_sems, rs_fill)
    dh = rms_back(h_own[...], g2[...], cube.get_own(rb))
    dm = dh.astype(BF16)
    cube.put_own(gb, dm)
    dm32[0] = dm

    def token_back():
        d_pair.wait()
        w = wgh.shape[1] // RING
        part = jnp.zeros((2 * last, d), F32)
        for p in range(RING):
            at = pl.ds(p * w, w)
            d_act = nt(dm32[...].reshape(2 * last, d), wd[at, :])
            gate = gt_own[:, at].astype(F32)
            sig = jax.nn.sigmoid(gate)
            d_gate = (d_act * u_own[:, at].astype(F32) * (sig * (1.0 + gate * (1.0 - sig)))).astype(BF16)
            d_up = (d_act * (gate * sig)).astype(BF16)
            part = part + (nt(d_gate, wgh[:, at]) + nt(d_up, wuh[:, at]))
        mp[...] = part.reshape(mp.shape)
        m_pair.start()

    def ag_fill(s):
        if s == walk:
            token_back()
        else:
            run(1)

    d_pair.start()
    cube.all_gather(gb, ag_sems, ag_fill)
    cube.collect(gb, dmf, c)
    dm_pair.start()
    run(PARTS)
    m_pair.wait()
    dx_own[...] = dh + rms_back(x_own[...].astype(F32), g1[...], mp[0] + mr[...])
    l_pair.wait()
    loss[...] = (lbuf[0] + lbuf[1]) / num_tokens
    t_out.wait()
    cube.finish(out_copies(PARTS - 2) + out_copies(PARTS - 1) + [dm_pair])


def table_kernel(cube, vb, idx, dx_own, dmf, wd, deh, at_i, gt_i, u_i, de, act_o, dg_o, du_o, got_g, got_u, *scratch):
    nat, mix, de_r, aoth, fin, fout, part, psend, precv, lsem, isem, osem, gsend, grecv, *rest = scratch
    gb, ag_sems = rest[:COLORS], rest[COLORS:]
    cube.bind(psend, precv)
    c = cube.c
    t = cube.rows
    fc = wd.shape[0] // PARTS
    half_d = aoth.shape[0]
    a_copy = pltpu.make_async_copy(at_i.at[span(1 - c, half_d)], aoth, lsem)

    def in_copies(p):
        return [pltpu.make_async_copy(src.at[p], fin.at[p % 2, i], isem.at[i, p]) for i, src in enumerate((gt_i, u_i))]

    def out_copies(p):
        return [pltpu.make_async_copy(fout.at[p % 2, i], dst.at[p], osem.at[i, p]) for i, dst in enumerate((act_o, dg_o, du_o))]

    def send_copies(p):
        dev = (cube.m, 1 - c)
        return [
            pltpu.make_async_remote_copy(
                src_ref=part.at[p % 2, i], dst_ref=dst.at[p], send_sem=gsend.at[i, p], recv_sem=grecv.at[i, p], device_id=dev, device_id_type=MESH
            )
            for i, dst in enumerate((got_g, got_u))
        ]

    def drain(p):
        cube.finish(out_copies(p))
        for copy in send_copies(p):
            copy.wait_send()

    cube.start([a_copy] + in_copies(0))
    cube.put_own(gb, dx_own[...])
    cube.barrier()
    step = cube.ag_start(gb, ag_sems)
    mix[...] = deh[...]
    a_copy.wait()
    tile = min(512, 2 * t)
    for p in range(PARTS):
        if p + 1 < PARTS:
            cube.start(in_copies(p + 1))
        cube.finish(in_copies(p))
        if p >= 2:
            drain(p - 2)
        src, dst, res = fin.at[p % 2], fout.at[p % 2], part.at[p % 2]

        def body(i):
            at = span(i, tile)
            d_act = nt(dmf[at, :], wd[pl.ds(p * fc, fc), :])
            gate = src[0, at, :].astype(F32)
            up = src[1, at, :].astype(F32)
            sig = jax.nn.sigmoid(gate)
            silu = gate * sig
            outs = (silu * up, d_act * up * (sig * (1.0 + gate * (1.0 - sig))), d_act * silu)
            for which, v in enumerate(outs):
                dst[which, at, :] = v.astype(BF16)

        loop(0, 2 * t // tile, body)
        for which in range(2):
            res[which] = nn(aoth[...], dst[which + 1])
        cube.start(out_copies(p) + send_copies(p))
        if step > 0 and p % 2 < 1:
            step = cube.ag_next(gb, ag_sems, step)
    while step >= 0:
        step = cube.ag_next(gb, ag_sems, step)
    cube.collect(gb, nat)
    chunk = min(256, t)

    def scatter(i):
        at = span(i, chunk)
        hot = one_hot(2 * vb, idx[:, at])
        val = nat[at, :]
        hi = val.astype(BF16)
        rest = val - hi.astype(F32)
        mid = rest.astype(BF16)
        low = (rest - mid.astype(F32)).astype(BF16)
        mix[...] = mix[...] + ((nn(hot, low) + nn(hot, mid)) + nn(hot, hi))

    loop(0, t // chunk, scatter)
    e_pair = cube.pair(mix.at[pl.ds(vb, vb)], de_r)
    e_pair.start()
    drain(PARTS - 2)
    drain(PARTS - 1)
    for p in range(PARTS):
        for copy in send_copies(p):
            copy.wait_recv()
    e_pair.wait()
    de[...] = mix[pl.ds(0, vb), :] + de_r[...]


def weight_kernel(core, aown, dg, du, act, dmf, got_g, got_u, og, ou, od):
    even = pl.program_id(0) % 2 == 0
    n, _, fc = dg.shape

    @pl.when(even)
    def _():
        for i in range(n):
            og[:, pl.ds(i * fc, fc)] = nn(aown[...], dg[i])
            ou[:, pl.ds(i * fc, fc)] = nn(aown[...], du[i])

    @pl.when(jnp.logical_not(even))
    def _():
        for i in range(n):
            og[:, pl.ds(i * fc, fc)] = got_g[i]
            ou[:, pl.ds(i * fc, fc)] = got_u[i]
            od[pl.ds(i * fc, fc), :] = tn(act[i], dmf[...])


def solution(mesh):
    model, fsdp_size = mesh.shape["model"], mesh.shape["fsdp"]
    tok_spec = P("fsdp", None)
    row_spec = P(("model", "fsdp"), None)
    weight_spec = P("fsdp", None)
    vmem = pl.BlockSpec(memory_space=pltpu.VMEM)
    hbm = pl.BlockSpec(memory_space=pl.ANY)
    sds = jax.ShapeDtypeStruct
    dma = pltpu.SemaphoreType.DMA

    def params(cid):
        return pltpu.CompilerParams(collective_id=cid, has_side_effects=True, vmem_limit_bytes=VMEM_LIMIT)

    def device_step(tok_ids, tok_labels, table_shard, gate_shard, up_shard, down_shard, gain_in, gain_out):
        t = tok_ids.size
        num_tokens = t * fsdp_size
        real, d = table_shard.shape
        vb = -(-real // 16) * 16
        f = gate_shard.shape[1]
        half_f, half_d = f // 2, d // 2
        fc = half_f // PARTS
        cube = Cube(model, t, d)
        last = cube.last
        me, core = lax.axis_index("model"), lax.axis_index("fsdp")
        first = (2 * me + core) * real
        other = (2 * me + 1 - core) * real

        def local_rows(ids):
            flat = ids.reshape(1, t)
            here, there = flat - first, flat - other
            return jnp.where((here >= 0) & (here < real), here, jnp.where((there >= 0) & (there < real), vb + there, -1))

        idx = local_rows(tok_ids)
        lab = local_rows(tok_labels)
        table = jnp.pad(table_shard, ((0, vb - real), (0, 0)))
        g1, g2 = gain_in.reshape(1, d), gain_out.reshape(1, d)
        act_own = sds((2 * last, half_f), BF16)
        w_half = sds((d, half_f), BF16)
        hn, ep, wgh, wuh, h_own, gt_own, u_own, x_own = pl.pallas_call(
            functools.partial(embed_kernel, cube, vb),
            out_shape=(sds((t, d), BF16), sds((2 * vb, d), BF16), w_half, w_half, sds((last, d), F32), act_own, act_own, sds((last, d), BF16)),
            in_specs=[vmem, hbm, hbm, hbm, hbm, vmem, vmem],
            out_specs=(vmem, hbm, hbm, hbm, vmem, vmem, vmem, vmem),
            scratch_shapes=[
                pltpu.VMEM((half_f, d), BF16),
                pltpu.VMEM((2 * vb, d), BF16),
                pltpu.VMEM((d, half_f), BF16),
                pltpu.VMEM((d, half_f), BF16),
                pltpu.VMEM((t, d), BF16),
                pltpu.VMEM((2, last, d), BF16),
                pltpu.VMEM((2, last, d), F32),
                pltpu.VMEM((last, d), F32),
                dma((8,)),
                dma((8,)),
                dma((8,)),
            ]
            + cube.groups(BF16, BF16, BF16)
            + cube.sems(2),
            compiler_params=params(0),
            name="embed",
        )(idx, table, gate_shard, up_shard, down_shard, g1, g2)
        chunked = sds((PARTS, 2 * t, fc), BF16)
        dmf, loss, deh, dx_own, a_t, gt, u = pl.pallas_call(
            functools.partial(head_kernel, cube, vb, real, num_tokens),
            out_shape=(sds((2 * t, d), BF16), sds((8, 128), F32), sds((2 * vb, d), F32), sds((last, d), F32), sds((d, 2 * t), BF16), chunked, chunked),
            in_specs=[vmem] * 9 + [hbm] * 3,
            out_specs=(vmem,) * 4 + (hbm,) * 3,
            scratch_shapes=[
                pltpu.VMEM((2 * vb, t), F32),
                pltpu.VMEM((2 * vb, t), BF16),
                pltpu.VMEM((t, d), F32),
                pltpu.VMEM((cube.axes + 1, RING, RING, t), F32),
                pltpu.VMEM((2, 8, 128), F32),
                pltpu.VMEM((2, last, d), BF16),
                pltpu.VMEM((2, last, d), F32),
                pltpu.VMEM((last, d), F32),
                pltpu.VMEM((d, half_f), BF16),
                pltpu.VMEM((d, half_f), BF16),
                pltpu.VMEM((half_f, d), BF16),
                pltpu.VMEM((2 * t, d), BF16),
                pltpu.VMEM((d, 2 * t), BF16),
                pltpu.VMEM((2, 2, 2 * t, fc), BF16),
                dma((8,)),
                dma((8,)),
                dma((8,)),
                dma((2, PARTS)),
                dma((cube.axes, RING)),
                dma((cube.axes, RING)),
            ]
            + cube.groups(F32, F32, BF16, BF16)
            + cube.sems(3),
            compiler_params=params(1),
            name="head",
        )(hn, ep, lab, h_own, g2, x_own, g1, gt_own, u_own, wgh, wuh, down_shard)
        got = sds((PARTS, half_d, fc), F32)
        de, act, d_gate, d_up, got_g, got_u = pl.pallas_call(
            functools.partial(table_kernel, cube, vb),
            out_shape=(sds((vb, d), F32), chunked, chunked, chunked, got, got),
            in_specs=[vmem] * 5 + [hbm] * 3,
            out_specs=(vmem,) + (hbm,) * 5,
            scratch_shapes=[
                pltpu.VMEM((t, d), F32),
                pltpu.VMEM((2 * vb, d), F32),
                pltpu.VMEM((vb, d), F32),
                pltpu.VMEM((half_d, 2 * t), BF16),
                pltpu.VMEM((2, 2, 2 * t, fc), BF16),
                pltpu.VMEM((2, 3, 2 * t, fc), BF16),
                pltpu.VMEM((2, 2, half_d, fc), F32),
                dma((1,)),
                dma((1,)),
                dma,
                dma((2, PARTS)),
                dma((3, PARTS)),
                dma((2, PARTS)),
                dma((2, PARTS)),
            ]
            + cube.groups(F32)
            + cube.sems(1),
            compiler_params=params(2),
            name="table",
        )(idx, dx_own, dmf, down_shard, deh, a_t, gt, u)
        wide = 2
        chunk_spec = pl.BlockSpec((wide, 2 * t, fc), lambda i, s: (i // 2, 0, 0))
        got_spec = pl.BlockSpec((wide, half_d, fc), lambda i, s: (i // 2, 0, 0))
        grad_spec = pl.BlockSpec((half_d, wide * fc), lambda i, s: (0, (s[0] + i % 2) % 2 * (PARTS // wide) + i // 2))
        grad_gate, grad_up, grad_down = pl.pallas_call(
            weight_kernel,
            out_shape=(sds((half_d, f), F32), sds((half_d, f), F32), sds((half_f, d), F32)),
            grid_spec=pltpu.PrefetchScalarGridSpec(
                num_scalar_prefetch=1,
                grid=(2 * PARTS // wide,),
                in_specs=[
                    pl.BlockSpec((half_d, 2 * t), lambda i, s: (s[0], 0)),
                    chunk_spec,
                    chunk_spec,
                    chunk_spec,
                    pl.BlockSpec((2 * t, d), lambda i, s: (0, 0)),
                    got_spec,
                    got_spec,
                ],
                out_specs=(grad_spec, grad_spec, pl.BlockSpec((wide * fc, d), lambda i, s: (i // 2, 0))),
            ),
            compiler_params=pltpu.CompilerParams(vmem_limit_bytes=VMEM_LIMIT),
            name="weights",
        )(core.reshape(1).astype(jnp.int32), a_t, d_gate, d_up, act, dmf, got_g, got_u)
        return loss[0, 0], de[:real], grad_gate, grad_up, grad_down

    return jax.shard_map(device_step, mesh=mesh, in_specs=(tok_spec, tok_spec, row_spec, weight_spec, weight_spec, weight_spec, P(), P()), out_specs=(P(), row_spec, weight_spec, weight_spec, weight_spec), check_vma=False)
```

```python
import functools
import itertools

import jax
import jax.numpy as jnp
from jax import lax
from jax.experimental import pallas as pl
from jax.experimental.pallas import tpu as pltpu
from jax.sharding import PartitionSpec as P

EPS = 1e-6
MESH = pl.DeviceIdType.MESH
VMEM_LIMIT = 67043328
F32 = jnp.float32
BF16 = jnp.bfloat16
COLORS = 3
DIRECT = 3
PARTS = 8
RING = 4
TOP, SUM, LABEL = range(3)


def contract(a, b, dims):
    return lax.dot_general(a, b, (dims, ((), ())), preferred_element_type=F32)


def nn(a, b):
    return contract(a, b, ((1,), (0,)))


def nt(a, b):
    return contract(a, b, ((1,), (1,)))


def tn(a, b):
    return contract(a, b, ((0,), (0,)))


def span(i, n):
    return pl.ds(pl.multiple_of(i * n, n), n)


def loop(lo, hi, body):
    def step(i, carry):
        body(i)
        return carry

    lax.fori_loop(lo, hi, step, 0)


def mean(v):
    return jnp.mean(v, axis=-1, keepdims=True)


def rms_scale(values, gain):
    return values * lax.rsqrt(mean(values * values) + EPS) * gain


def rms_back(values, gain, grad):
    r = lax.rsqrt(mean(values * values) + EPS)
    gg = grad * gain
    return r * gg - values * (r * r * r) * mean(values * gg)


def one_hot(rows, ids):
    return (lax.broadcasted_iota(jnp.int32, (rows, ids.shape[-1]), 0) == ids).astype(F32).astype(BF16)


def table_rows(cube, real, vb, ids):
    here = ids - (2 * cube.m + cube.c) * real
    there = ids - (2 * cube.m + 1 - cube.c) * real
    return jnp.where((here >= 0) & (here < real), here, jnp.where((there >= 0) & (there < real), vb + there, -1))


class Local:
    def __init__(self, sems):
        self.sems, self.free = sems, itertools.count()

    def __call__(self, src, dst):
        return pltpu.make_async_copy(src, dst, self.sems.at[next(self.free)])


class Cube:
    def __init__(self, model, rows, width):
        axes = 1
        while RING**axes < model:
            axes += 1
        self.axes, self.nb, self.rows = axes, 2 * axes, rows
        self.direct = min(DIRECT, self.nb - 1)
        self.walk = self.nb - self.direct
        self.peers = 2**self.direct - 1
        self.last = rows >> self.nb
        tiles = width // 128
        big = -(-tiles // COLORS) * 128
        self.widths = [big, big, width - 2 * big]
        self.starts = [0, big, 2 * big]

    def dim(self, k, s):
        d = (k + s) % self.nb
        return d % self.axes, d // self.axes

    def bind(self, psend=None, precv=None):
        self.m = lax.axis_index("model")
        self.c = lax.axis_index("fsdp")
        self.psend, self.precv, self.free = psend, precv, itertools.count()
        self.digits = [(self.m // RING**a) % RING for a in range(self.axes)]
        self.bit, self.base = [], []
        for k in range(COLORS):
            bits, bases = [], [0]
            for s in range(self.nb):
                a, kind = self.dim(k, s)
                b = self.digits[a]
                v0, v1 = (b % 2 + b // 2) % 2, b // 2
                bits.append(v0 + ((kind + self.c) % 2) * (v1 - v0))
                bases.append(bases[-1] + bits[-1] * (self.rows >> len(bits)))
            self.bit.append(bits)
            self.base.append(bases)

    def toggled(self, k, steps):
        digits = list(self.digits)
        for s in steps:
            a, kind = self.dim(k, s)
            near = 1 - 2 * (digits[a] % 2)
            digits[a] = digits[a] + near + ((kind + self.c) % 2) * (RING - 1 - 2 * digits[a] - near)
        return sum(v * RING**a for a, v in enumerate(digits))

    def group(self, q):
        return [self.walk + i for i in range(self.direct) if (q >> i) % 2]

    def ring_peer(self, a, step):
        b = self.digits[a]
        return self.m + RING**a * ((b + step) % RING - b)

    def barrier(self, rings=False):
        sem = pltpu.get_barrier_semaphore()
        peers = [(self.m, 1 - self.c)]
        for k in range(COLORS):
            steps = [[s] for s in range(self.walk)] + [self.group(q + 1) for q in range(self.peers)]
            peers += [(self.toggled(k, st), self.c) for st in steps]
        if rings:
            peers += [(self.ring_peer(a, step), self.c) for a in range(self.axes) for step in range(1, RING)]
        for peer in peers:
            pl.semaphore_signal(sem, inc=1, device_id=peer, device_id_type=MESH)
        pl.semaphore_wait(sem, len(peers))

    def place(self, k, j):
        pos = []
        for c in range(2):
            p = 0
            for s in range(self.nb):
                a, kind = self.dim(k, s)
                p = 2 * p + (j >> (a + self.axes * ((kind + c) % 2))) % 2
            pos.append(p * self.last)
        return self.rows_at(pos[0] + self.c * (pos[1] - pos[0]), self.last)

    def rows_at(self, start, size):
        return pl.ds(pl.multiple_of(start, self.last), size)

    def cols(self, k):
        return pl.ds(self.starts[k], self.widths[k])

    def pieces(self):
        return itertools.product(range(2**self.nb), range(COLORS))

    def spread(self, nat, bufs):
        for j, k in self.pieces():
            bufs[k][self.place(k, j), :] = nat[span(j, self.last), self.cols(k)]

    def collect(self, bufs, nat, half=None):
        start = 0 if half is None else half * self.rows
        for j, k in self.pieces():
            nat[self.rows_at(start + j * self.last, self.last), self.cols(k)] = bufs[k][self.place(k, j), :]

    def own(self, k):
        return self.rows_at(self.base[k][-1], self.last)

    def put_own(self, bufs, value):
        for k in range(COLORS):
            bufs[k][self.own(k), :] = value[:, self.starts[k] : self.starts[k] + self.widths[k]]

    def get_own(self, bufs):
        return jnp.concatenate([bufs[k][self.own(k), :] for k in range(COLORS)], axis=1)

    def send(self, src, dst, sems, index, peer):
        return pltpu.make_async_remote_copy(
            src_ref=src, dst_ref=dst, send_sem=sems[0].at[index], recv_sem=sems[1].at[index], device_id=(peer, self.c), device_id_type=MESH
        )

    def flip(self, k, steps):
        return sum((1 - 2 * self.bit[k][s]) * (self.rows >> (s + 1)) for s in steps)

    def start(self, copies):
        for copy in copies:
            copy.start()

    def finish(self, copies):
        for copy in copies:
            copy.wait()

    def rs_parts(self, k, s):
        base, off, ln = self.base[k], self.rows - (self.rows >> s), self.rows >> (s + 1)
        if s == self.walk:
            first = self.rows - (self.rows >> s)
            return [(base[-1] + self.flip(k, self.group(q + 1)), base[-1], first + q * self.last, self.last) for q in range(self.peers)]
        away = base[s + 1] + self.flip(k, [s])
        if s == self.walk - 1:
            return [(away, base[s + 1], off, ln)]
        half = ln // 2
        b = self.bit[k][s + 1]
        return [(away + x * half, base[s + 1] + x * half, off + i * half, half) for i, x in enumerate((1 - b, b))]

    def rs_copies(self, bufs, recvs, sems, k, s, which=slice(None)):
        out = []
        for i, (src, _, dst, ln) in list(enumerate(self.rs_parts(k, s)))[which]:
            peer = self.toggled(k, self.group(i + 1) if s == self.walk else [s])
            at = 2 * s + i
            out.append(self.send(bufs[k].at[self.rows_at(src, ln)], recvs[k].at[pl.ds(dst, ln)], sems, (k, at), peer))
        return out

    def rs_take(self, bufs, recvs, sems, k, s, which):
        parts = self.rs_parts(k, s)[which]
        self.finish(self.rs_copies(bufs, recvs, sems, k, s, which))
        at = self.rows_at(parts[0][1], parts[0][3])
        got = sum(recvs[k][pl.ds(dst, ln), :].astype(F32) for _, _, dst, ln in parts)
        bufs[k][at, :] = (bufs[k][at, :].astype(F32) + got).astype(bufs[k].dtype)

    def reduce_scatter(self, bufs, recvs, sems, fill=None):
        for k in range(COLORS):
            self.start(self.rs_copies(bufs, recvs, sems, k, 0))
        for s in range(self.walk + 1):
            if fill is not None:
                fill(s)
            for k in range(COLORS):
                if 0 < s < self.walk:
                    self.rs_take(bufs, recvs, sems, k, s - 1, slice(1, 2))
                if s < self.walk:
                    self.rs_take(bufs, recvs, sems, k, s, slice(0, 1))
                    self.start(self.rs_copies(bufs, recvs, sems, k, s + 1))
                else:
                    self.rs_take(bufs, recvs, sems, k, s, slice(None))

    def blocks(self, s):
        later = range(s + 1, self.walk)
        return [st for n in range(len(later) + 1) for st in itertools.combinations(later, n)]

    def ag_block(self, bufs, sems, k, s, block):
        at = self.base[k][self.walk] + self.flip(k, block)
        ref = bufs[k].at[self.rows_at(at, self.rows >> self.walk)]
        index = 2 ** (self.walk - 1 - s) - 1 + self.blocks(s).index(block)
        return self.send(ref, ref, sems, (k, self.peers + index), self.toggled(k, [s]))

    def ag_direct(self, bufs, sems, k):
        ref = bufs[k].at[self.own(k)]
        return [self.send(ref, ref, sems, (k, q), self.toggled(k, self.group(q + 1))) for q in range(self.peers)]

    def ag_start(self, bufs, sems):
        for k in range(COLORS):
            self.start(self.ag_direct(bufs, sems, k))
        return self.walk

    def ag_next(self, bufs, sems, s):
        if s == self.walk:
            for k in range(COLORS):
                self.finish(self.ag_direct(bufs, sems, k))
                for to in range(s - 1, -1, -1):
                    self.ag_block(bufs, sems, k, to, ()).start()
            return s - 1
        for block in self.blocks(s):
            for k in range(COLORS):
                self.ag_block(bufs, sems, k, s, block).wait()
                for to in range(s - 1, -1, -1):
                    self.ag_block(bufs, sems, k, to, tuple(sorted(block + (s,)))).start()
        return s - 1

    def all_gather(self, bufs, sems, fill=None):
        s = self.ag_start(bufs, sems)
        while s >= 0:
            if fill is not None:
                fill(s)
            s = self.ag_next(bufs, sems, s)

    def pair(self, src, dst):
        i = next(self.free)
        return pltpu.make_async_remote_copy(
            src_ref=src, dst_ref=dst, send_sem=self.psend.at[i], recv_sem=self.precv.at[i], device_id=(self.m, 1 - self.c), device_id_type=MESH
        )

    def groups(self, *dtypes):
        return [pltpu.VMEM((self.rows, w), dtype) for dtype in dtypes for w in self.widths]

    def sems(self, n):
        return [pltpu.SemaphoreType.DMA((COLORS, self.peers + max(2 * self.walk, 2**self.walk)))] * (2 * n)


def by(n, items):
    return [items[i : i + n] for i in range(0, len(items), n)]


def embed_kernel(cube, vb, ids, e_ref, wg, wu, wd, g1, g2, hn, ep_o, wgh_o, wuh_o, h_own, gt_own, u_own, x_own, *scratch):
    e_s, wd_s, ep, wgh, wuh, xnat, x32, mp, mr, psend, precv, lsem, *rest = scratch
    xb, xr, hb = by(COLORS, rest[: 3 * COLORS])
    rs_sems, hg_sems = by(2, rest[3 * COLORS :])
    cube.bind(psend, precv)
    local = Local(lsem)
    c = cube.c
    d = hn.shape[1]
    half_d, half_f = d // 2, wgh.shape[1]
    last = cube.last
    mine_d = span(c, half_d)
    e_local = local(e_ref, e_s)
    e_local.start()
    w_local = [local(wd, wd_s), local(wg.at[:, span(c, half_f)], wgh.at[mine_d]), local(wu.at[:, span(c, half_f)], wuh.at[mine_d])]
    cube.barrier()
    e_local.wait()
    real = e_s.shape[0]
    body = real - real % 16
    if body > 0:
        ep[pl.ds(0, body), :] = e_s[pl.ds(0, body), :]
    if vb > body:
        ep[pl.ds(body, vb - body), :] = jnp.zeros((vb - body, d), BF16)
        ep[pl.ds(body, real - body), :] = e_s[pl.ds(body, real - body), :]
    e_pair = cube.pair(ep.at[pl.ds(0, vb)], ep.at[pl.ds(vb, vb)])
    e_pair.start()
    w_pair = [cube.pair(src.at[:, span(1 - c, half_f)], dst.at[mine_d]) for src, dst in ((wg, wgh), (wu, wuh))]
    cube.start(w_pair + w_local)
    e_pair.wait()
    outs = [local(ep, ep_o), local(wgh, wgh_o), local(wuh, wuh_o)]
    outs[0].start()
    chunk = min(256, cube.rows)

    def lookup(i):
        at = span(i, chunk)
        xnat[at, :] = tn(one_hot(2 * vb, table_rows(cube, real, vb, ids[:, at])), ep[...]).astype(BF16)

    loop(0, cube.rows // chunk, lookup)
    cube.spread(xnat, xb)
    cube.reduce_scatter(xb, xr, rs_sems)
    x_own[...] = cube.get_own(xb)
    x32[0] = x_own[...]
    x_pair = cube.pair(x32.at[0], x32.at[1])
    x_pair.start()
    cube.finish(w_local + w_pair)
    cube.start(outs[1:])
    x_pair.wait()
    a_rows = rms_scale(x32[...].reshape(2 * last, d).astype(F32), g1[...]).astype(BF16)
    parts = 4
    fc = half_f // parts
    total = jnp.zeros((2 * last, d), F32)
    for p in range(parts):
        at = pl.ds(p * fc, fc)
        gate = nn(a_rows, wgh[:, at]).astype(BF16)
        up = nn(a_rows, wuh[:, at]).astype(BF16)
        gt_own[:, at] = gate
        u_own[:, at] = up
        gate_f = gate.astype(F32)
        act = (gate_f * jax.nn.sigmoid(gate_f) * up.astype(F32)).astype(BF16)
        total = total + nn(act, wd_s[at, :])
    mp[...] = total.reshape(2, last, d)
    m_pair = cube.pair(mp.at[1], mr)
    m_pair.start()
    m_pair.wait()
    h_rows = x_own[...].astype(F32) + (mp[0] + mr[...]).astype(BF16).astype(F32)
    h_own[...] = h_rows
    cube.put_own(hb, rms_scale(h_rows, g2[...]).astype(BF16))
    cube.all_gather(hb, hg_sems)
    cube.collect(hb, hn)
    cube.finish(outs)


def head_kernel(
    cube, vb, real, num_tokens, hn, ep, labels, h_own, g2, x_own, g1, gt_own, u_own, wgh_i, wuh_i, wd_i,
    dm_nat, loss, deh, dx_own, at_o, gt_o, u_o, *scratch
):
    z, dz, nat, stats, lbuf, dm32, mp, mr, wgh, wuh, wd, xf, tstage, stage, psend, precv, lsem, osem, st_s, st_r, *rest = scratch
    rb, rr, gb, xg = by(COLORS, rest[: 4 * COLORS])
    rs_sems, ag_sems, xg_sems = by(2, rest[4 * COLORS :])
    cube.bind(psend, precv)
    local = Local(lsem)
    c = cube.c
    t, d = hn.shape
    walk, last = cube.walk, cube.last
    w_copies = [local(wgh_i, wgh), local(wuh_i, wuh), local(wd_i, wd)]
    cube.start(w_copies)
    cube.put_own(xg, x_own[...])
    cube.barrier(rings=True)
    xstep = cube.ag_start(xg, xg_sems)
    chunk = min(256, t)
    chunks = t // chunk
    mine = cube.digits[0]

    def logits(i):
        at = span(i, chunk)
        row = lax.broadcasted_iota(jnp.int32, (2 * vb, chunk), 0)
        valid = (row < real) | ((row >= vb) & (row < vb + real))
        zz = jnp.where(valid, nt(ep[...], hn[at, :]), -1e38)
        z[:, at] = zz
        top = jnp.max(zz, axis=0, keepdims=True)
        parts = {TOP: top, SUM: jnp.exp(zz - top), LABEL: jnp.where(row == table_rows(cube, real, vb, labels[:, at]), zz, 0.0)}
        for r, v in parts.items():
            stats[0, mine, pl.ds(r, 1), at] = v if r == TOP else jnp.sum(v, axis=0, keepdims=True)

    loop(0, chunks, logits)
    xstep = cube.ag_next(xg, xg_sems, xstep)
    for a in range(cube.axes):
        here = stats.at[a, cube.digits[a]]
        copies = [cube.send(here, here, (st_s, st_r), (a, step - 1), cube.ring_peer(a, step)) for step in range(1, RING)]
        cube.start(copies)
        cube.finish(copies)
        if xstep > 1:
            xstep = cube.ag_next(xg, xg_sems, xstep)
        tops, sums, marks = [[stats[a, i, pl.ds(r, 1), :] for i in range(RING)] for r in range(LABEL + 1)]
        top = functools.reduce(jnp.maximum, tops)
        total = sum(v * jnp.exp(m - top) for m, v in zip(tops, sums))
        label = sum(marks)
        slot = cube.digits[a + 1] if a + 1 < cube.axes else 0
        for r, v in enumerate((top, total, label)):
            stats[a + 1, slot, pl.ds(r, 1), :] = v
    while xstep > 0:
        xstep = cube.ag_next(xg, xg_sems, xstep)
    tok_loss = jnp.sum(top + jnp.log(total) - label, axis=1, keepdims=True)
    lbuf[c] = jnp.broadcast_to(tok_loss, lbuf.shape[1:])
    l_pair = cube.pair(lbuf.at[c], lbuf.at[c])
    l_pair.start()
    final = stats.at[cube.axes, 0]

    def backward(i):
        at = span(i, chunk)
        row = lax.broadcasted_iota(jnp.int32, (2 * vb, chunk), 0)
        soft = jnp.exp(z[:, at] - final[pl.ds(TOP, 1), at]) / final[pl.ds(SUM, 1), at]
        dzz = (jnp.where(row == table_rows(cube, real, vb, labels[:, at]), soft - 1.0, soft) / num_tokens).astype(BF16)
        dz[:, at] = dzz
        nat[at, :] = tn(dzz, ep[...])

    loop(0, chunks, backward)
    cube.spread(nat, rb)
    mine_t = span(c, t)
    xf_pair = cube.pair(xf.at[mine_t], xf.at[mine_t])
    d_pair = cube.pair(dm32.at[0], dm32.at[1])
    m_pair = cube.pair(mp.at[1], mr)
    t_out = local(tstage, at_o)
    fc = wgh.shape[1] // PARTS
    tile = min(512, 2 * t)

    def out_copies(p):
        return [pltpu.make_async_copy(stage.at[p % 2, i], dst.at[p], osem.at[i, p]) for i, dst in enumerate((gt_o, u_o))]

    def gate_up(p):
        if p >= 2:
            cube.finish(out_copies(p - 2))
        cols = pl.ds(p * fc, fc)
        slot = stage.at[p % 2]

        def body(i):
            at = span(i, tile)
            for which, w in enumerate((wgh, wuh)):
                slot[which, at, :] = nn(xf[at, :], w[:, cols]).astype(BF16)

        loop(0, 2 * t // tile, body)
        cube.start(out_copies(p))

    def normalise(i):
        at = span(c * chunks + i, chunk)
        xf[at, :] = rms_scale(xf[at, :].astype(F32), g1[...]).astype(BF16)

    def transpose(half, i):
        at = span(half * chunks + i, chunk)
        tstage[:, at] = xf[at, :].astype(F32).T.astype(BF16)

    def head_grad(i):
        deh[span(i, vb), :] = nn(dz[span(i, vb), :], hn[...])

    todo = list(range(PARTS))

    def run(n):
        while n > 0 and todo:
            gate_up(todo.pop(0))
            n -= 1

    def rs_fill(s):
        if s == 0:
            cube.ag_next(xg, xg_sems, xstep)
            cube.collect(xg, xf, c)
            loop(0, chunks, normalise)
            xf_pair.start()
            loop(0, 2, head_grad)
            loop(0, chunks, functools.partial(transpose, c))
        elif s == 1:
            cube.finish(w_copies + [xf_pair])
            loop(0, chunks, functools.partial(transpose, 1 - c))
            t_out.start()
            run(2)
        else:
            run(2)

    cube.reduce_scatter(rb, rr, rs_sems, rs_fill)
    dh = rms_back(h_own[...], g2[...], cube.get_own(rb))
    dm = dh.astype(BF16)
    cube.put_own(gb, dm)
    dm32[0] = dm

    def token_back():
        d_pair.wait()
        w = wgh.shape[1] // RING
        part = jnp.zeros((2 * last, d), F32)
        for p in range(RING):
            at = pl.ds(p * w, w)
            d_act = nt(dm32[...].reshape(2 * last, d), wd[at, :])
            gate = gt_own[:, at].astype(F32)
            sig = jax.nn.sigmoid(gate)
            d_gate = (d_act * u_own[:, at].astype(F32) * (sig * (1.0 + gate * (1.0 - sig)))).astype(BF16)
            d_up = (d_act * (gate * sig)).astype(BF16)
            part = part + (nt(d_gate, wgh[:, at]) + nt(d_up, wuh[:, at]))
        mp[...] = part.reshape(mp.shape)
        m_pair.start()

    def ag_fill(s):
        if s == walk:
            token_back()
        else:
            run(1)

    d_pair.start()
    cube.all_gather(gb, ag_sems, ag_fill)
    cube.collect(gb, dm_nat)
    run(PARTS)
    m_pair.wait()
    dx_own[...] = dh + rms_back(x_own[...].astype(F32), g1[...], mp[0] + mr[...])
    l_pair.wait()
    loss[0, 0] = jnp.max((lbuf[0] + lbuf[1]) / num_tokens)
    t_out.wait()
    cube.finish(out_copies(PARTS - 2) + out_copies(PARTS - 1))


def table_kernel(cube, vb, real, ids, dx_own, dm_i, wd_i, deh, at_i, gt_i, u_i, de, dmf_o, act_o, dg_o, du_o, got_g, got_u, *scratch):
    dmf, wd, nat, mix, de_r, aoth, fin, fout, part, psend, precv, lsem, isem, osem, gsend, grecv, *rest = scratch
    gb, ag_sems = rest[:COLORS], rest[COLORS:]
    cube.bind(psend, precv)
    c = cube.c
    t = cube.rows
    fc = wd.shape[0] // PARTS
    half_d = aoth.shape[0]
    local = Local(lsem)
    mine_t = span(c, t)
    dm_copy, wd_copy, a_copy = local(dm_i, dmf.at[mine_t]), local(wd_i, wd), local(at_i.at[span(1 - c, half_d)], aoth)
    deh_copy, dm_out = local(deh, mix), local(dmf, dmf_o)
    dm_pair = cube.pair(dm_i, dmf.at[mine_t])

    def in_copies(p):
        return [pltpu.make_async_copy(src.at[p], fin.at[p % 2, i], isem.at[i, p]) for i, src in enumerate((gt_i, u_i))]

    def out_copies(p):
        return [pltpu.make_async_copy(fout.at[p % 2, i], dst.at[p], osem.at[i, p]) for i, dst in enumerate((act_o, dg_o, du_o))]

    def send_copies(p):
        dev = (cube.m, 1 - c)
        return [
            pltpu.make_async_remote_copy(
                src_ref=part.at[p % 2, i], dst_ref=dst.at[p], send_sem=gsend.at[i, p], recv_sem=grecv.at[i, p], device_id=dev, device_id_type=MESH
            )
            for i, dst in enumerate((got_g, got_u))
        ]

    def drain(p):
        cube.finish(out_copies(p))
        for copy in send_copies(p):
            copy.wait_send()

    cube.start([dm_copy, wd_copy] + in_copies(0) + [a_copy, deh_copy])
    cube.put_own(gb, dx_own[...])
    cube.barrier()
    step = cube.ag_start(gb, ag_sems)
    dm_pair.start()
    cube.finish([dm_copy, wd_copy, a_copy])
    tile = min(512, t)
    tiles = t // tile
    for p in range(PARTS):
        if p + 1 < PARTS:
            cube.start(in_copies(p + 1))
        cube.finish(in_copies(p))
        if p >= 2:
            drain(p - 2)
        src, dst, res = fin.at[p % 2], fout.at[p % 2], part.at[p % 2]

        def body(half, i):
            at = span(half * tiles + i, tile)
            d_act = nt(dmf[at, :], wd[pl.ds(p * fc, fc), :])
            gate = src[0, at, :].astype(F32)
            up = src[1, at, :].astype(F32)
            sig = jax.nn.sigmoid(gate)
            silu = gate * sig
            outs = (silu * up, d_act * up * (sig * (1.0 + gate * (1.0 - sig))), d_act * silu)
            for which, v in enumerate(outs):
                dst[which, at, :] = v.astype(BF16)

        if p == 0:
            loop(0, tiles, functools.partial(body, c))
            dm_pair.wait()
            dm_out.start()
            loop(0, tiles, functools.partial(body, 1 - c))
        else:
            loop(0, 2 * tiles, functools.partial(body, 0))
        for which in range(2):
            res[which] = nn(aoth[...], dst[which + 1])
        cube.start(out_copies(p) + send_copies(p))
        if step > 0 and p % 2 == 0:
            step = cube.ag_next(gb, ag_sems, step)
    while step >= 0:
        step = cube.ag_next(gb, ag_sems, step)
    cube.collect(gb, nat)
    cube.finish([deh_copy, dm_out])
    chunk = min(256, t)

    def scatter(i):
        at = span(i, chunk)
        hot = one_hot(2 * vb, table_rows(cube, real, vb, ids[:, at]))
        val = nat[at, :]
        hi = val.astype(BF16)
        rest = val - hi.astype(F32)
        mid = rest.astype(BF16)
        low = (rest - mid.astype(F32)).astype(BF16)
        mix[...] = mix[...] + ((nn(hot, low) + nn(hot, mid)) + nn(hot, hi))

    loop(0, t // chunk, scatter)
    e_pair = cube.pair(mix.at[pl.ds(vb, vb)], de_r)
    e_pair.start()
    drain(PARTS - 2)
    drain(PARTS - 1)
    for p in range(PARTS):
        for copy in send_copies(p):
            copy.wait_recv()
    e_pair.wait()
    de[...] = mix[pl.ds(0, vb), :] + de_r[...]


def weight_kernel(loss, de, at_i, dg, du, act, dmf_i, got_g, got_u, loss_o, de_o, og, ou, od, *scratch):
    aown, dmf, ring, gring, ostage, dstage, de_s, de_t, lsem, rsem, gsem, osem, xsem = scratch
    c = lax.axis_index("fsdp")
    depth, fc = ring.shape[0], ring.shape[-1]
    parts, half_f = dg.shape[0], dg.shape[0] * fc
    local = Local(lsem)
    a_copy, dm_copy = local(at_i.at[span(c, aown.shape[0])], aown), local(dmf_i, dmf)
    de_in, de_out = local(de, de_s), local(de_t, de_o)

    def reads(p):
        slot = lax.rem(p, depth)
        grads = [pltpu.make_async_copy(src.at[p], ring.at[slot, i], rsem.at[i, slot]) for i, src in enumerate((dg, du, act))]
        return grads, [pltpu.make_async_copy(src.at[p], gring.at[slot, i], gsem.at[i, slot]) for i, src in enumerate((got_g, got_u))]

    def columns(half, p):
        return pl.ds(pl.multiple_of(half * half_f + p * fc, fc), fc)

    def passes(p):
        slot = lax.rem(p, depth)
        return [pltpu.make_async_copy(gring.at[slot, i], dst.at[:, columns(1 - c, p)], xsem.at[i, slot]) for i, dst in enumerate((og, ou))]

    def writes(p):
        slot = lax.rem(p, 2)
        out = [pltpu.make_async_copy(ostage.at[slot, i], dst.at[:, columns(c, p)], osem.at[i, slot]) for i, dst in enumerate((og, ou))]
        return out + [pltpu.make_async_copy(dstage.at[slot], od.at[span(p, fc)], osem.at[2, slot])]

    def each(copies, verb):
        for copy in copies:
            getattr(copy, verb)()

    def fetch(p):
        grads, got = reads(p)
        each(grads + got, "start")

    a_copy.start()
    fetch(0)
    dm_copy.start()
    for p in range(1, depth):
        fetch(p)
    de_in.start()
    a_copy.wait()
    loss_o[0, 0] = loss[0, 0]

    def body(p):
        slot, oslot = lax.rem(p, depth), lax.rem(p, 2)
        grads, got = reads(p)
        each(got, "wait")
        each(passes(p), "start")
        each(grads, "wait")

        @pl.when(p >= 2)
        def _():
            each(writes(p - 2), "wait")

        for i in range(2):
            ostage[oslot, i] = nn(aown[...], ring[slot, i])

        @pl.when(p == 0)
        def _():
            dm_copy.wait()

        dstage[oslot] = tn(ring[slot, 2], dmf[...])
        each(writes(p), "start")
        each(passes(p), "wait")

        @pl.when(p + depth < parts)
        def _():
            fetch(p + depth)

    loop(0, parts, body)
    de_in.wait()
    de_t[...] = de_s[pl.ds(0, de_t.shape[0]), :]
    de_out.start()
    each(writes(parts - 2) + writes(parts - 1), "wait")
    de_out.wait()


def solution(mesh):
    model, fsdp_size = mesh.shape["model"], mesh.shape["fsdp"]
    tok_spec = P("fsdp", None)
    row_spec = P(("model", "fsdp"), None)
    weight_spec = P("fsdp", None)
    vmem = pl.BlockSpec(memory_space=pltpu.VMEM)
    hbm = pl.BlockSpec(memory_space=pl.ANY)
    sds = jax.ShapeDtypeStruct
    dma = pltpu.SemaphoreType.DMA

    def params(cid):
        return pltpu.CompilerParams(collective_id=cid, has_side_effects=True, vmem_limit_bytes=VMEM_LIMIT)

    def device_step(tok_ids, tok_labels, table_shard, gate_shard, up_shard, down_shard, gain_in, gain_out):
        t = tok_ids.size
        num_tokens = t * fsdp_size
        real, d = table_shard.shape
        vb = -(-real // 16) * 16
        f = gate_shard.shape[1]
        half_f, half_d = f // 2, d // 2
        fc = half_f // PARTS
        cube = Cube(model, t, d)
        last = cube.last
        ids, labels = tok_ids.reshape(1, t), tok_labels.reshape(1, t)
        smem = pl.BlockSpec(memory_space=pltpu.SMEM)
        g1, g2 = gain_in.reshape(1, d), gain_out.reshape(1, d)
        act_own = sds((2 * last, half_f), BF16)
        w_half = sds((d, half_f), BF16)
        hn, ep, wgh, wuh, h_own, gt_own, u_own, x_own = pl.pallas_call(
            functools.partial(embed_kernel, cube, vb),
            out_shape=(sds((t, d), BF16), sds((2 * vb, d), BF16), w_half, w_half, sds((last, d), F32), act_own, act_own, sds((last, d), BF16)),
            in_specs=[vmem, hbm, hbm, hbm, hbm, vmem, vmem],
            out_specs=(vmem, hbm, hbm, hbm, vmem, vmem, vmem, vmem),
            scratch_shapes=[
                pltpu.VMEM((real, d), BF16),
                pltpu.VMEM((half_f, d), BF16),
                pltpu.VMEM((2 * vb, d), BF16),
                pltpu.VMEM((d, half_f), BF16),
                pltpu.VMEM((d, half_f), BF16),
                pltpu.VMEM((t, d), BF16),
                pltpu.VMEM((2, last, d), BF16),
                pltpu.VMEM((2, last, d), F32),
                pltpu.VMEM((last, d), F32),
                dma((8,)),
                dma((8,)),
                dma((8,)),
            ]
            + cube.groups(BF16, BF16, BF16)
            + cube.sems(2),
            compiler_params=params(0),
            name="embed",
        )(ids, table_shard, gate_shard, up_shard, down_shard, g1, g2)
        chunked = sds((PARTS, 2 * t, fc), BF16)
        dm, loss, deh, dx_own, a_t, gt, u = pl.pallas_call(
            functools.partial(head_kernel, cube, vb, real, num_tokens),
            out_shape=(sds((t, d), BF16), sds((1, 1), F32), sds((2 * vb, d), F32), sds((last, d), F32), sds((d, 2 * t), BF16), chunked, chunked),
            in_specs=[vmem] * 9 + [hbm] * 3,
            out_specs=(vmem, smem, vmem, vmem) + (hbm,) * 3,
            scratch_shapes=[
                pltpu.VMEM((2 * vb, t), F32),
                pltpu.VMEM((2 * vb, t), BF16),
                pltpu.VMEM((t, d), F32),
                pltpu.VMEM((cube.axes + 1, RING, RING, t), F32),
                pltpu.VMEM((2, 8, 128), F32),
                pltpu.VMEM((2, last, d), BF16),
                pltpu.VMEM((2, last, d), F32),
                pltpu.VMEM((last, d), F32),
                pltpu.VMEM((d, half_f), BF16),
                pltpu.VMEM((d, half_f), BF16),
                pltpu.VMEM((half_f, d), BF16),
                pltpu.VMEM((2 * t, d), BF16),
                pltpu.VMEM((d, 2 * t), BF16),
                pltpu.VMEM((2, 2, 2 * t, fc), BF16),
                dma((8,)),
                dma((8,)),
                dma((8,)),
                dma((2, PARTS)),
                dma((cube.axes, RING)),
                dma((cube.axes, RING)),
            ]
            + cube.groups(F32, F32, BF16, BF16)
            + cube.sems(3),
            compiler_params=params(1),
            name="head",
        )(hn, ep, labels, h_own, g2, x_own, g1, gt_own, u_own, wgh, wuh, down_shard)
        got = sds((PARTS, half_d, fc), F32)
        de, dmf, act, d_gate, d_up, got_g, got_u = pl.pallas_call(
            functools.partial(table_kernel, cube, vb, real),
            out_shape=(sds((vb, d), F32), sds((2 * t, d), BF16), chunked, chunked, chunked, got, got),
            in_specs=[vmem] * 2 + [hbm] * 6,
            out_specs=(vmem,) + (hbm,) * 6,
            scratch_shapes=[
                pltpu.VMEM((2 * t, d), BF16),
                pltpu.VMEM((half_f, d), BF16),
                pltpu.VMEM((t, d), F32),
                pltpu.VMEM((2 * vb, d), F32),
                pltpu.VMEM((vb, d), F32),
                pltpu.VMEM((half_d, 2 * t), BF16),
                pltpu.VMEM((2, 2, 2 * t, fc), BF16),
                pltpu.VMEM((2, 3, 2 * t, fc), BF16),
                pltpu.VMEM((2, 2, half_d, fc), F32),
                dma((2,)),
                dma((2,)),
                dma((5,)),
                dma((2, PARTS)),
                dma((3, PARTS)),
                dma((2, PARTS)),
                dma((2, PARTS)),
            ]
            + cube.groups(F32)
            + cube.sems(1),
            compiler_params=params(2),
            name="table",
        )(ids, dx_own, dm, down_shard, deh, a_t, gt, u)
        depth = 3
        loss, de, grad_gate, grad_up, grad_down = pl.pallas_call(
            weight_kernel,
            out_shape=(sds((1, 1), F32), sds((real, d), F32), sds((half_d, f), F32), sds((half_d, f), F32), sds((half_f, d), F32)),
            in_specs=[smem] + [hbm] * 8,
            out_specs=(smem,) + (hbm,) * 4,
            scratch_shapes=[
                pltpu.VMEM((half_d, 2 * t), BF16),
                pltpu.VMEM((2 * t, d), BF16),
                pltpu.VMEM((depth, 3, 2 * t, fc), BF16),
                pltpu.VMEM((depth, 2, half_d, fc), F32),
                pltpu.VMEM((2, 2, half_d, fc), F32),
                pltpu.VMEM((2, fc, d), F32),
                pltpu.VMEM((vb, d), F32),
                pltpu.VMEM((real, d), F32),
                dma((4,)),
                dma((3, depth)),
                dma((2, depth)),
                dma((3, 2)),
                dma((2, depth)),
            ],
            compiler_params=pltpu.CompilerParams(vmem_limit_bytes=VMEM_LIMIT, has_side_effects=True),
            name="weights",
        )(loss, de, a_t, d_gate, d_up, act, dmf, got_g, got_u)
        return loss.reshape(()), de, grad_gate, grad_up, grad_down

    return jax.shard_map(device_step, mesh=mesh, in_specs=(tok_spec, tok_spec, row_spec, weight_spec, weight_spec, weight_spec, P(), P()), out_specs=(P(), row_spec, weight_spec, weight_spec, weight_spec), check_vma=False)
```

```python
import functools
import itertools

import jax
import jax.numpy as jnp
from jax import lax
from jax.experimental import pallas as pl
from jax.experimental.pallas import tpu as pltpu
from jax.sharding import PartitionSpec as P

EPS = 1e-6
MESH = pl.DeviceIdType.MESH
VMEM_LIMIT = 67043328
F32 = jnp.float32
BF16 = jnp.bfloat16
COLORS = 3
DIRECT = 3
PARTS = 8
RING = 4
TOP, SUM, LABEL = range(3)


def contract(a, b, dims):
    return lax.dot_general(a, b, (dims, ((), ())), preferred_element_type=F32)


def nn(a, b):
    return contract(a, b, ((1,), (0,)))


def nt(a, b):
    return contract(a, b, ((1,), (1,)))


def tn(a, b):
    return contract(a, b, ((0,), (0,)))


def span(i, n):
    return pl.ds(pl.multiple_of(i * n, n), n)


def loop(lo, hi, body):
    def step(i, carry):
        body(i)
        return carry

    lax.fori_loop(lo, hi, step, 0)


def mean(v):
    return jnp.mean(v, axis=-1, keepdims=True)


def rms_scale(values, gain):
    return values * lax.rsqrt(mean(values * values) + EPS) * gain


def rms_back(values, gain, grad):
    r = lax.rsqrt(mean(values * values) + EPS)
    gg = grad * gain
    return r * gg - values * (r * r * r) * mean(values * gg)


def one_hot(rows, ids):
    return (lax.broadcasted_iota(jnp.int32, (rows, ids.shape[-1]), 0) == ids).astype(F32).astype(BF16)


def table_rows(cube, real, vb, ids):
    here = ids - (2 * cube.m + cube.c) * real
    there = ids - (2 * cube.m + 1 - cube.c) * real
    return jnp.where((here >= 0) & (here < real), here, jnp.where((there >= 0) & (there < real), vb + there, -1))


class Local:
    def __init__(self, sems):
        self.sems, self.free = sems, itertools.count()

    def __call__(self, src, dst):
        return pltpu.make_async_copy(src, dst, self.sems.at[next(self.free)])


class Cube:
    def __init__(self, model, rows, width):
        axes = 1
        while RING**axes < model:
            axes += 1
        self.axes, self.nb, self.rows = axes, 2 * axes, rows
        self.direct = min(DIRECT, self.nb - 1)
        self.walk = self.nb - self.direct
        self.peers = 2**self.direct - 1
        self.last = rows >> self.nb
        tiles = width // 128
        big = -(-tiles // COLORS) * 128
        self.widths = [big, big, width - 2 * big]
        self.starts = [0, big, 2 * big]

    def dim(self, k, s):
        d = (k + s) % self.nb
        return d % self.axes, d // self.axes

    def bind(self, psend=None, precv=None):
        self.m = lax.axis_index("model")
        self.c = lax.axis_index("fsdp")
        self.psend, self.precv, self.free = psend, precv, itertools.count()
        self.digits = [(self.m // RING**a) % RING for a in range(self.axes)]
        self.bit, self.base = [], []
        for k in range(COLORS):
            bits, bases = [], [0]
            for s in range(self.nb):
                a, kind = self.dim(k, s)
                b = self.digits[a]
                v0, v1 = (b % 2 + b // 2) % 2, b // 2
                bits.append(v0 + ((kind + self.c) % 2) * (v1 - v0))
                bases.append(bases[-1] + bits[-1] * (self.rows >> len(bits)))
            self.bit.append(bits)
            self.base.append(bases)

    def toggled(self, k, steps):
        digits = list(self.digits)
        for s in steps:
            a, kind = self.dim(k, s)
            near = 1 - 2 * (digits[a] % 2)
            digits[a] = digits[a] + near + ((kind + self.c) % 2) * (RING - 1 - 2 * digits[a] - near)
        return sum(v * RING**a for a, v in enumerate(digits))

    def group(self, q):
        return [self.walk + i for i in range(self.direct) if (q >> i) % 2]

    def ring_peer(self, a, step):
        b = self.digits[a]
        return self.m + RING**a * ((b + step) % RING - b)

    def arrive(self, rings=False):
        peers = [(self.m, 1 - self.c)]
        for k in range(COLORS):
            steps = [[s] for s in range(self.walk)] + [self.group(q + 1) for q in range(self.peers)]
            peers += [(self.toggled(k, st), self.c) for st in steps]
        if rings:
            peers += [(self.ring_peer(a, step), self.c) for a in range(self.axes) for step in range(1, RING)]
        for peer in peers:
            pl.semaphore_signal(pltpu.get_barrier_semaphore(), inc=1, device_id=peer, device_id_type=MESH)
        self.expected = len(peers)

    def meet(self):
        pl.semaphore_wait(pltpu.get_barrier_semaphore(), self.expected)

    def place(self, k, j):
        pos = []
        for c in range(2):
            p = 0
            for s in range(self.nb):
                a, kind = self.dim(k, s)
                p = 2 * p + (j >> (a + self.axes * ((kind + c) % 2))) % 2
            pos.append(p * self.last)
        return self.rows_at(pos[0] + self.c * (pos[1] - pos[0]), self.last)

    def rows_at(self, start, size):
        return pl.ds(pl.multiple_of(start, self.last), size)

    def cols(self, k):
        return pl.ds(self.starts[k], self.widths[k])

    def pieces(self):
        return itertools.product(range(2**self.nb), range(COLORS))

    def spread(self, nat, bufs):
        for j, k in self.pieces():
            bufs[k][self.place(k, j), :] = nat[span(j, self.last), self.cols(k)]

    def collect(self, bufs, nat, half=None):
        start = 0 if half is None else half * self.rows
        for j, k in self.pieces():
            nat[self.rows_at(start + j * self.last, self.last), self.cols(k)] = bufs[k][self.place(k, j), :]

    def own(self, k):
        return self.rows_at(self.base[k][-1], self.last)

    def put_own(self, bufs, value):
        for k in range(COLORS):
            bufs[k][self.own(k), :] = value[:, self.starts[k] : self.starts[k] + self.widths[k]]

    def get_own(self, bufs):
        return jnp.concatenate([bufs[k][self.own(k), :] for k in range(COLORS)], axis=1)

    def send(self, src, dst, sems, index, peer):
        return pltpu.make_async_remote_copy(
            src_ref=src, dst_ref=dst, send_sem=sems[0].at[index], recv_sem=sems[1].at[index], device_id=(peer, self.c), device_id_type=MESH
        )

    def flip(self, k, steps):
        return sum((1 - 2 * self.bit[k][s]) * (self.rows >> (s + 1)) for s in steps)

    def start(self, copies):
        for copy in copies:
            copy.start()

    def finish(self, copies):
        for copy in copies:
            copy.wait()

    def rs_parts(self, k, s):
        base, off, ln = self.base[k], self.rows - (self.rows >> s), self.rows >> (s + 1)
        if s == self.walk:
            first = self.rows - (self.rows >> s)
            return [(base[-1] + self.flip(k, self.group(q + 1)), base[-1], first + q * self.last, self.last) for q in range(self.peers)]
        away = base[s + 1] + self.flip(k, [s])
        if s == self.walk - 1:
            return [(away, base[s + 1], off, ln)]
        half = ln // 2
        b = self.bit[k][s + 1]
        return [(away + x * half, base[s + 1] + x * half, off + i * half, half) for i, x in enumerate((1 - b, b))]

    def rs_copies(self, bufs, recvs, sems, k, s, which=slice(None)):
        out = []
        for i, (src, _, dst, ln) in list(enumerate(self.rs_parts(k, s)))[which]:
            peer = self.toggled(k, self.group(i + 1) if s == self.walk else [s])
            at = 2 * s + i
            out.append(self.send(bufs[k].at[self.rows_at(src, ln)], recvs[k].at[pl.ds(dst, ln)], sems, (k, at), peer))
        return out

    def rs_take(self, bufs, recvs, sems, k, s, which):
        parts = self.rs_parts(k, s)[which]
        self.finish(self.rs_copies(bufs, recvs, sems, k, s, which))
        at = self.rows_at(parts[0][1], parts[0][3])
        got = sum(recvs[k][pl.ds(dst, ln), :].astype(F32) for _, _, dst, ln in parts)
        bufs[k][at, :] = (bufs[k][at, :].astype(F32) + got).astype(bufs[k].dtype)

    def reduce_scatter(self, bufs, recvs, sems, fill=None):
        for k in range(COLORS):
            self.start(self.rs_copies(bufs, recvs, sems, k, 0))
        for s in range(self.walk + 1):
            if fill is not None:
                fill(s)
            for k in range(COLORS):
                if 0 < s < self.walk:
                    self.rs_take(bufs, recvs, sems, k, s - 1, slice(1, 2))
                if s < self.walk:
                    self.rs_take(bufs, recvs, sems, k, s, slice(0, 1))
                    self.start(self.rs_copies(bufs, recvs, sems, k, s + 1))
                else:
                    self.rs_take(bufs, recvs, sems, k, s, slice(None))

    def blocks(self, s):
        later = range(s + 1, self.walk)
        return [st for n in range(len(later) + 1) for st in itertools.combinations(later, n)]

    def ag_block(self, bufs, sems, k, s, block):
        at = self.base[k][self.walk] + self.flip(k, block)
        ref = bufs[k].at[self.rows_at(at, self.rows >> self.walk)]
        index = 2 ** (self.walk - 1 - s) - 1 + self.blocks(s).index(block)
        return self.send(ref, ref, sems, (k, self.peers + index), self.toggled(k, [s]))

    def ag_direct(self, bufs, sems, k):
        ref = bufs[k].at[self.own(k)]
        return [self.send(ref, ref, sems, (k, q), self.toggled(k, self.group(q + 1))) for q in range(self.peers)]

    def ag_start(self, bufs, sems):
        for k in range(COLORS):
            self.start(self.ag_direct(bufs, sems, k))
        return self.walk

    def ag_next(self, bufs, sems, s):
        if s == self.walk:
            for k in range(COLORS):
                self.finish(self.ag_direct(bufs, sems, k))
                for to in range(s - 1, -1, -1):
                    self.ag_block(bufs, sems, k, to, ()).start()
            return s - 1
        for block in self.blocks(s):
            for k in range(COLORS):
                self.ag_block(bufs, sems, k, s, block).wait()
                for to in range(s - 1, -1, -1):
                    self.ag_block(bufs, sems, k, to, tuple(sorted(block + (s,)))).start()
        return s - 1

    def all_gather(self, bufs, sems, fill=None):
        s = self.ag_start(bufs, sems)
        while s >= 0:
            if fill is not None:
                fill(s)
            s = self.ag_next(bufs, sems, s)

    def pair(self, src, dst):
        i = next(self.free)
        return pltpu.make_async_remote_copy(
            src_ref=src, dst_ref=dst, send_sem=self.psend.at[i], recv_sem=self.precv.at[i], device_id=(self.m, 1 - self.c), device_id_type=MESH
        )

    def groups(self, *dtypes):
        return [pltpu.VMEM((self.rows, w), dtype) for dtype in dtypes for w in self.widths]

    def sems(self, n):
        return [pltpu.SemaphoreType.DMA((COLORS, self.peers + max(2 * self.walk, 2**self.walk)))] * (2 * n)


def by(n, items):
    return [items[i : i + n] for i in range(0, len(items), n)]


def embed_kernel(cube, vb, ids, e_ref, wg, wu, wd, g1, g2, hn, ep_o, wgh_o, wuh_o, h_own, gt_own, u_own, x_own, *scratch):
    e_s, wd_s, ep, wgh, wuh, xnat, x32, mp, mr, psend, precv, lsem, *rest = scratch
    xb, xr, hb = by(COLORS, rest[: 3 * COLORS])
    rs_sems, hg_sems = by(2, rest[3 * COLORS :])
    cube.bind(psend, precv)
    cube.arrive()
    local = Local(lsem)
    c = cube.c
    d = hn.shape[1]
    half_d, half_f = d // 2, wgh.shape[1]
    last = cube.last
    mine_d = span(c, half_d)
    e_local = local(e_ref, e_s)
    e_local.start()
    w_local = [local(wd, wd_s), local(wg.at[:, span(c, half_f)], wgh.at[mine_d]), local(wu.at[:, span(c, half_f)], wuh.at[mine_d])]
    e_local.wait()
    real = e_s.shape[0]
    body = real - real % 16
    if body > 0:
        ep[pl.ds(0, body), :] = e_s[pl.ds(0, body), :]
    if vb > body:
        ep[pl.ds(body, vb - body), :] = jnp.zeros((vb - body, d), BF16)
        ep[pl.ds(body, real - body), :] = e_s[pl.ds(body, real - body), :]
    cube.meet()
    e_pair = cube.pair(ep.at[pl.ds(0, vb)], ep.at[pl.ds(vb, vb)])
    e_pair.start()
    w_pair = [cube.pair(src.at[:, span(1 - c, half_f)], dst.at[mine_d]) for src, dst in ((wg, wgh), (wu, wuh))]
    cube.start(w_pair + w_local)
    chunk = min(256, cube.rows)

    def lookup(i):
        at = span(i, chunk)
        xnat[at, :] = tn(one_hot(vb, table_rows(cube, real, vb, ids[:, at])), ep[pl.ds(0, vb), :]).astype(BF16)

    def lookup_other(i):
        at = span(i, chunk)
        found = tn(one_hot(vb, table_rows(cube, real, vb, ids[:, at]) - vb), ep[pl.ds(vb, vb), :])
        xnat[at, :] = (xnat[at, :].astype(F32) + found).astype(BF16)

    loop(0, cube.rows // chunk, lookup)
    e_pair.wait()
    outs = [local(ep, ep_o), local(wgh, wgh_o), local(wuh, wuh_o)]
    outs[0].start()
    loop(0, cube.rows // chunk, lookup_other)
    cube.spread(xnat, xb)
    cube.reduce_scatter(xb, xr, rs_sems)
    x_own[...] = cube.get_own(xb)
    x32[0] = x_own[...]
    x_pair = cube.pair(x32.at[0], x32.at[1])
    x_pair.start()
    cube.finish(w_local + w_pair)
    cube.start(outs[1:])
    x_pair.wait()
    a_rows = rms_scale(x32[...].reshape(2 * last, d).astype(F32), g1[...]).astype(BF16)
    parts = 4
    fc = half_f // parts
    total = jnp.zeros((2 * last, d), F32)
    for p in range(parts):
        at = pl.ds(p * fc, fc)
        gate = nn(a_rows, wgh[:, at]).astype(BF16)
        up = nn(a_rows, wuh[:, at]).astype(BF16)
        gt_own[:, at] = gate
        u_own[:, at] = up
        gate_f = gate.astype(F32)
        act = (gate_f * jax.nn.sigmoid(gate_f) * up.astype(F32)).astype(BF16)
        total = total + nn(act, wd_s[at, :])
    mp[...] = total.reshape(2, last, d)
    m_pair = cube.pair(mp.at[1], mr)
    m_pair.start()
    m_pair.wait()
    h_rows = x_own[...].astype(F32) + (mp[0] + mr[...]).astype(BF16).astype(F32)
    h_own[...] = h_rows
    cube.put_own(hb, rms_scale(h_rows, g2[...]).astype(BF16))
    cube.all_gather(hb, hg_sems)
    cube.collect(hb, hn)
    cube.finish(outs)


def head_kernel(
    cube, vb, real, num_tokens, hn_i, ep_i, labels, h_own, g2, x_own, g1, gt_own, u_own, wgh_i, wuh_i, wd_i,
    dm_nat, loss, deh_o, dx_own, at_o, gt_o, u_o, *scratch
):
    hn, ep, z, dz, nat, stats, lbuf, dm32, mp, mr, wgh, wuh, wd, xf, tstage, stage, psend, precv, lsem, osem, st_s, st_r, *rest = scratch
    rb, rr, gb, xg = by(COLORS, rest[: 4 * COLORS])
    rs_sems, ag_sems, xg_sems = by(2, rest[4 * COLORS :])
    cube.bind(psend, precv)
    cube.arrive(rings=True)
    local = Local(lsem)
    c = cube.c
    t, d = hn.shape
    walk, last = cube.walk, cube.last
    first = [local(ep_i, ep), local(hn_i, hn)]
    cube.start(first)
    w_copies = [local(wgh_i, wgh), local(wuh_i, wuh), local(wd_i, wd)]
    cube.start(w_copies)
    cube.put_own(xg, x_own[...])
    chunk = min(256, t)
    chunks = t // chunk
    mine = cube.digits[0]

    def logits(i):
        at = span(i, chunk)
        row = lax.broadcasted_iota(jnp.int32, (2 * vb, chunk), 0)
        valid = (row < real) | ((row >= vb) & (row < vb + real))
        zz = jnp.where(valid, nt(ep[...], hn[at, :]), -1e38)
        z[:, at] = zz
        top = jnp.max(zz, axis=0, keepdims=True)
        parts = {TOP: top, SUM: jnp.exp(zz - top), LABEL: jnp.where(row == table_rows(cube, real, vb, labels[:, at]), zz, 0.0)}
        for r, v in parts.items():
            stats[0, mine, pl.ds(r, 1), at] = v if r == TOP else jnp.sum(v, axis=0, keepdims=True)

    cube.finish(first)
    loop(0, chunks // 2, logits)
    cube.meet()
    xstep = cube.ag_start(xg, xg_sems)
    loop(chunks // 2, chunks, logits)
    xstep = cube.ag_next(xg, xg_sems, xstep)
    for a in range(cube.axes):
        here = stats.at[a, cube.digits[a]]
        copies = [cube.send(here, here, (st_s, st_r), (a, step - 1), cube.ring_peer(a, step)) for step in range(1, RING)]
        cube.start(copies)
        cube.finish(copies)
        if xstep > 1:
            xstep = cube.ag_next(xg, xg_sems, xstep)
        tops, sums, marks = [[stats[a, i, pl.ds(r, 1), :] for i in range(RING)] for r in range(LABEL + 1)]
        top = functools.reduce(jnp.maximum, tops)
        total = sum(v * jnp.exp(m - top) for m, v in zip(tops, sums))
        label = sum(marks)
        slot = cube.digits[a + 1] if a + 1 < cube.axes else 0
        for r, v in enumerate((top, total, label)):
            stats[a + 1, slot, pl.ds(r, 1), :] = v
    while xstep > 0:
        xstep = cube.ag_next(xg, xg_sems, xstep)
    tok_loss = jnp.sum(top + jnp.log(total) - label, axis=1, keepdims=True)
    lbuf[c] = jnp.broadcast_to(tok_loss, lbuf.shape[1:])
    l_pair = cube.pair(lbuf.at[c], lbuf.at[c])
    l_pair.start()
    final = stats.at[cube.axes, 0]
    deh = z.at[:, pl.ds(0, d)]
    deh_out = local(deh, deh_o)

    def backward(i):
        at = span(i, chunk)
        row = lax.broadcasted_iota(jnp.int32, (2 * vb, chunk), 0)
        soft = jnp.exp(z[:, at] - final[pl.ds(TOP, 1), at]) / final[pl.ds(SUM, 1), at]
        dzz = (jnp.where(row == table_rows(cube, real, vb, labels[:, at]), soft - 1.0, soft) / num_tokens).astype(BF16)
        dz[:, at] = dzz
        nat[at, :] = tn(dzz, ep[...])

    loop(0, chunks, backward)
    cube.spread(nat, rb)
    mine_t = span(c, t)
    xf_pair = cube.pair(xf.at[mine_t], xf.at[mine_t])
    d_pair = cube.pair(dm32.at[0], dm32.at[1])
    m_pair = cube.pair(mp.at[1], mr)
    t_out = local(tstage, at_o)
    fc = wgh.shape[1] // PARTS
    tile = min(512, 2 * t)

    def out_copies(p):
        return [pltpu.make_async_copy(stage.at[p % 2, i], dst.at[p], osem.at[i, p]) for i, dst in enumerate((gt_o, u_o))]

    def gate_up(p):
        if p >= 2:
            cube.finish(out_copies(p - 2))
        cols = pl.ds(p * fc, fc)
        slot = stage.at[p % 2]

        def body(i):
            at = span(i, tile)
            for which, w in enumerate((wgh, wuh)):
                slot[which, at, :] = nn(xf[at, :], w[:, cols]).astype(BF16)

        loop(0, 2 * t // tile, body)
        cube.start(out_copies(p))

    def normalise(i):
        at = span(c * chunks + i, chunk)
        xf[at, :] = rms_scale(xf[at, :].astype(F32), g1[...]).astype(BF16)

    def transpose(half, i):
        at = span(half * chunks + i, chunk)
        tstage[:, at] = xf[at, :].astype(F32).T.astype(BF16)

    def head_grad(i):
        deh[span(i, vb), :] = nn(dz[span(i, vb), :], hn[...])

    todo = list(range(PARTS))

    def run(n):
        while n > 0 and todo:
            gate_up(todo.pop(0))
            n -= 1

    def rs_fill(s):
        if s == 0:
            cube.ag_next(xg, xg_sems, xstep)
            cube.collect(xg, xf, c)
            loop(0, chunks, normalise)
            xf_pair.start()
            loop(0, 2, head_grad)
            deh_out.start()
            loop(0, chunks, functools.partial(transpose, c))
        elif s == 1:
            cube.finish(w_copies + [xf_pair])
            loop(0, chunks, functools.partial(transpose, 1 - c))
            t_out.start()
            run(2)
        else:
            run(2)

    cube.reduce_scatter(rb, rr, rs_sems, rs_fill)
    dh = rms_back(h_own[...], g2[...], cube.get_own(rb))
    dm = dh.astype(BF16)
    cube.put_own(gb, dm)
    dm32[0] = dm

    def token_back():
        d_pair.wait()
        w = wgh.shape[1] // RING
        part = jnp.zeros((2 * last, d), F32)
        for p in range(RING):
            at = pl.ds(p * w, w)
            d_act = nt(dm32[...].reshape(2 * last, d), wd[at, :])
            gate = gt_own[:, at].astype(F32)
            sig = jax.nn.sigmoid(gate)
            d_gate = (d_act * u_own[:, at].astype(F32) * (sig * (1.0 + gate * (1.0 - sig)))).astype(BF16)
            d_up = (d_act * (gate * sig)).astype(BF16)
            part = part + (nt(d_gate, wgh[:, at]) + nt(d_up, wuh[:, at]))
        mp[...] = part.reshape(mp.shape)
        m_pair.start()

    def ag_fill(s):
        if s == walk:
            token_back()
        else:
            run(1)

    d_pair.start()
    cube.all_gather(gb, ag_sems, ag_fill)
    cube.collect(gb, dm_nat)
    run(PARTS)
    m_pair.wait()
    dx_own[...] = dh + rms_back(x_own[...].astype(F32), g1[...], mp[0] + mr[...])
    l_pair.wait()
    loss[0, 0] = jnp.max((lbuf[0] + lbuf[1]) / num_tokens)
    cube.finish([t_out, deh_out])
    cube.finish(out_copies(PARTS - 2) + out_copies(PARTS - 1))


def table_kernel(cube, vb, real, ids, dx_own, dm_i, wd_i, deh, at_i, gt_i, u_i, de, dmf_o, act_o, dg_o, du_o, got_g, got_u, *scratch):
    dmf, wd, nat, mix, de_r, aoth, fin, fout, part, psend, precv, lsem, isem, osem, gsend, grecv, *rest = scratch
    gb, ag_sems = rest[:COLORS], rest[COLORS:]
    cube.bind(psend, precv)
    cube.arrive()
    c = cube.c
    t = cube.rows
    fc = wd.shape[0] // PARTS
    half_d = aoth.shape[0]
    local = Local(lsem)
    mine_t = span(c, t)
    dm_copy, wd_copy, a_copy = local(dm_i, dmf.at[mine_t]), local(wd_i, wd), local(at_i.at[span(1 - c, half_d)], aoth)
    deh_copy, dm_out = local(deh, mix), local(dmf, dmf_o)
    dm_pair = cube.pair(dm_i, dmf.at[mine_t])

    def in_copies(p):
        return [pltpu.make_async_copy(src.at[p], fin.at[p % 2, i], isem.at[i, p]) for i, src in enumerate((gt_i, u_i))]

    def out_copies(p):
        return [pltpu.make_async_copy(fout.at[p % 2, i], dst.at[p], osem.at[i, p]) for i, dst in enumerate((act_o, dg_o, du_o))]

    def send_copies(p):
        dev = (cube.m, 1 - c)
        return [
            pltpu.make_async_remote_copy(
                src_ref=part.at[p % 2, i], dst_ref=dst.at[p], send_sem=gsend.at[i, p], recv_sem=grecv.at[i, p], device_id=dev, device_id_type=MESH
            )
            for i, dst in enumerate((got_g, got_u))
        ]

    def drain(p):
        cube.finish(out_copies(p))
        for copy in send_copies(p):
            copy.wait_send()

    cube.start([dm_copy, wd_copy] + in_copies(0) + [a_copy, deh_copy])
    cube.put_own(gb, dx_own[...])
    cube.meet()
    step = cube.ag_start(gb, ag_sems)
    dm_pair.start()
    cube.finish([dm_copy, wd_copy, a_copy])
    tile = min(512, t)
    tiles = t // tile
    for p in range(PARTS):
        if p + 1 < PARTS:
            cube.start(in_copies(p + 1))
        cube.finish(in_copies(p))
        if p >= 2:
            drain(p - 2)
        src, dst, res = fin.at[p % 2], fout.at[p % 2], part.at[p % 2]

        def body(half, i):
            at = span(half * tiles + i, tile)
            d_act = nt(dmf[at, :], wd[pl.ds(p * fc, fc), :])
            gate = src[0, at, :].astype(F32)
            up = src[1, at, :].astype(F32)
            sig = jax.nn.sigmoid(gate)
            silu = gate * sig
            outs = (silu * up, d_act * up * (sig * (1.0 + gate * (1.0 - sig))), d_act * silu)
            for which, v in enumerate(outs):
                dst[which, at, :] = v.astype(BF16)

        if p == 0:
            loop(0, tiles, functools.partial(body, c))
            dm_pair.wait()
            dm_out.start()
            loop(0, tiles, functools.partial(body, 1 - c))
        else:
            loop(0, 2 * tiles, functools.partial(body, 0))
        for which in range(2):
            res[which] = nn(aoth[...], dst[which + 1])
        cube.start(out_copies(p) + send_copies(p))
        if step > 0 and p % 2 == 0:
            step = cube.ag_next(gb, ag_sems, step)
    while step >= 0:
        step = cube.ag_next(gb, ag_sems, step)
    cube.collect(gb, nat)
    cube.finish([deh_copy, dm_out])
    chunk = min(256, t)

    def scatter(half, i):
        at = span(i, chunk)
        rows = pl.ds(half * vb, vb)
        hot = one_hot(vb, table_rows(cube, real, vb, ids[:, at]) - half * vb)
        val = nat[at, :]
        hi = val.astype(BF16)
        rest = val - hi.astype(F32)
        mid = rest.astype(BF16)
        low = (rest - mid.astype(F32)).astype(BF16)
        mix[rows, :] = mix[rows, :] + ((nn(hot, low) + nn(hot, mid)) + nn(hot, hi))

    loop(0, t // chunk, functools.partial(scatter, 1))
    e_pair = cube.pair(mix.at[pl.ds(vb, vb)], de_r)
    e_pair.start()
    loop(0, t // chunk, functools.partial(scatter, 0))
    drain(PARTS - 2)
    drain(PARTS - 1)
    for p in range(PARTS):
        for copy in send_copies(p):
            copy.wait_recv()
    e_pair.wait()
    de[...] = mix[pl.ds(0, vb), :] + de_r[...]


def weight_kernel(loss, de, at_i, dg, du, act, dmf_i, got_g, got_u, loss_o, de_o, og, ou, od, *scratch):
    aown, dmf, ring, gring, ostage, dstage, de_s, de_t, lsem, rsem, gsem, osem, xsem = scratch
    c = lax.axis_index("fsdp")
    depth, fc = ring.shape[0], ring.shape[-1]
    parts, half_f = dg.shape[0], dg.shape[0] * fc
    local = Local(lsem)
    a_copy, dm_copy = local(at_i.at[span(c, aown.shape[0])], aown), local(dmf_i, dmf)
    de_in, de_out = local(de, de_s), local(de_t, de_o)

    def reads(p):
        slot = lax.rem(p, depth)
        grads = [pltpu.make_async_copy(src.at[p], ring.at[slot, i], rsem.at[i, slot]) for i, src in enumerate((dg, du, act))]
        return grads, [pltpu.make_async_copy(src.at[p], gring.at[slot, i], gsem.at[i, slot]) for i, src in enumerate((got_g, got_u))]

    def columns(half, p):
        return pl.ds(pl.multiple_of(half * half_f + p * fc, fc), fc)

    def passes(p):
        slot = lax.rem(p, depth)
        return [pltpu.make_async_copy(gring.at[slot, i], dst.at[:, columns(1 - c, p)], xsem.at[i, slot]) for i, dst in enumerate((og, ou))]

    def writes(p):
        slot = lax.rem(p, 2)
        out = [pltpu.make_async_copy(ostage.at[slot, i], dst.at[:, columns(c, p)], osem.at[i, slot]) for i, dst in enumerate((og, ou))]
        return out + [pltpu.make_async_copy(dstage.at[slot], od.at[span(p, fc)], osem.at[2, slot])]

    def each(copies, verb):
        for copy in copies:
            getattr(copy, verb)()

    def fetch(p):
        grads, got = reads(p)
        each(grads + got, "start")

    a_copy.start()
    fetch(0)
    dm_copy.start()
    for p in range(1, depth):
        fetch(p)
    de_in.start()
    a_copy.wait()
    loss_o[0, 0] = loss[0, 0]

    def body(p):
        slot, oslot = lax.rem(p, depth), lax.rem(p, 2)
        grads, got = reads(p)
        each(got, "wait")
        each(passes(p), "start")
        each(grads, "wait")

        @pl.when(p >= 2)
        def _():
            each(writes(p - 2), "wait")

        for i in range(2):
            ostage[oslot, i] = nn(aown[...], ring[slot, i])

        @pl.when(p == 0)
        def _():
            dm_copy.wait()

        dstage[oslot] = tn(ring[slot, 2], dmf[...])
        each(writes(p), "start")

        @pl.when(p >= 1)
        def _():
            each(passes(p - 1), "wait")

        @pl.when((p >= 1) & (p - 1 + depth < parts))
        def _():
            fetch(p - 1 + depth)

    loop(0, parts, body)
    de_in.wait()
    de_t[...] = de_s[pl.ds(0, de_t.shape[0]), :]
    de_out.start()
    each(passes(parts - 1) + writes(parts - 2) + writes(parts - 1), "wait")
    de_out.wait()


def solution(mesh):
    model, fsdp_size = mesh.shape["model"], mesh.shape["fsdp"]
    tok_spec = P("fsdp", None)
    row_spec = P(("model", "fsdp"), None)
    weight_spec = P("fsdp", None)
    vmem = pl.BlockSpec(memory_space=pltpu.VMEM)
    hbm = pl.BlockSpec(memory_space=pl.ANY)
    sds = jax.ShapeDtypeStruct
    dma = pltpu.SemaphoreType.DMA

    def params(cid):
        return pltpu.CompilerParams(collective_id=cid, has_side_effects=True, vmem_limit_bytes=VMEM_LIMIT)

    def device_step(tok_ids, tok_labels, table_shard, gate_shard, up_shard, down_shard, gain_in, gain_out):
        t = tok_ids.size
        num_tokens = t * fsdp_size
        real, d = table_shard.shape
        vb = -(-real // 16) * 16
        f = gate_shard.shape[1]
        half_f, half_d = f // 2, d // 2
        fc = half_f // PARTS
        cube = Cube(model, t, d)
        last = cube.last
        ids, labels = tok_ids.reshape(1, t), tok_labels.reshape(1, t)
        smem = pl.BlockSpec(memory_space=pltpu.SMEM)
        g1, g2 = gain_in.reshape(1, d), gain_out.reshape(1, d)
        act_own = sds((2 * last, half_f), BF16)
        w_half = sds((d, half_f), BF16)
        hn, ep, wgh, wuh, h_own, gt_own, u_own, x_own = pl.pallas_call(
            functools.partial(embed_kernel, cube, vb),
            out_shape=(sds((t, d), BF16), sds((2 * vb, d), BF16), w_half, w_half, sds((last, d), F32), act_own, act_own, sds((last, d), BF16)),
            in_specs=[vmem, hbm, hbm, hbm, hbm, vmem, vmem],
            out_specs=(vmem, hbm, hbm, hbm, vmem, vmem, vmem, vmem),
            scratch_shapes=[
                pltpu.VMEM((real, d), BF16),
                pltpu.VMEM((half_f, d), BF16),
                pltpu.VMEM((2 * vb, d), BF16),
                pltpu.VMEM((d, half_f), BF16),
                pltpu.VMEM((d, half_f), BF16),
                pltpu.VMEM((t, d), BF16),
                pltpu.VMEM((2, last, d), BF16),
                pltpu.VMEM((2, last, d), F32),
                pltpu.VMEM((last, d), F32),
                dma((8,)),
                dma((8,)),
                dma((8,)),
            ]
            + cube.groups(BF16, BF16, BF16)
            + cube.sems(2),
            compiler_params=params(0),
            name="embed",
        )(ids, table_shard, gate_shard, up_shard, down_shard, g1, g2)
        chunked = sds((PARTS, 2 * t, fc), BF16)
        dm, loss, deh, dx_own, a_t, gt, u = pl.pallas_call(
            functools.partial(head_kernel, cube, vb, real, num_tokens),
            out_shape=(sds((t, d), BF16), sds((1, 1), F32), sds((2 * vb, d), F32), sds((last, d), F32), sds((d, 2 * t), BF16), chunked, chunked),
            in_specs=[hbm] * 2 + [vmem] * 7 + [hbm] * 3,
            out_specs=(vmem, smem, hbm, vmem) + (hbm,) * 3,
            scratch_shapes=[
                pltpu.VMEM((t, d), BF16),
                pltpu.VMEM((2 * vb, d), BF16),
                pltpu.VMEM((2 * vb, max(t, d)), F32),
                pltpu.VMEM((2 * vb, t), BF16),
                pltpu.VMEM((t, d), F32),
                pltpu.VMEM((cube.axes + 1, RING, RING, t), F32),
                pltpu.VMEM((2, 8, 128), F32),
                pltpu.VMEM((2, last, d), BF16),
                pltpu.VMEM((2, last, d), F32),
                pltpu.VMEM((last, d), F32),
                pltpu.VMEM((d, half_f), BF16),
                pltpu.VMEM((d, half_f), BF16),
                pltpu.VMEM((half_f, d), BF16),
                pltpu.VMEM((2 * t, d), BF16),
                pltpu.VMEM((d, 2 * t), BF16),
                pltpu.VMEM((2, 2, 2 * t, fc), BF16),
                dma((8,)),
                dma((8,)),
                dma((8,)),
                dma((2, PARTS)),
                dma((cube.axes, RING)),
                dma((cube.axes, RING)),
            ]
            + cube.groups(F32, F32, BF16, BF16)
            + cube.sems(3),
            compiler_params=params(1),
            name="head",
        )(hn, ep, labels, h_own, g2, x_own, g1, gt_own, u_own, wgh, wuh, down_shard)
        got = sds((PARTS, half_d, fc), F32)
        de, dmf, act, d_gate, d_up, got_g, got_u = pl.pallas_call(
            functools.partial(table_kernel, cube, vb, real),
            out_shape=(sds((vb, d), F32), sds((2 * t, d), BF16), chunked, chunked, chunked, got, got),
            in_specs=[vmem] * 2 + [hbm] * 6,
            out_specs=(vmem,) + (hbm,) * 6,
            scratch_shapes=[
                pltpu.VMEM((2 * t, d), BF16),
                pltpu.VMEM((half_f, d), BF16),
                pltpu.VMEM((t, d), F32),
                pltpu.VMEM((2 * vb, d), F32),
                pltpu.VMEM((vb, d), F32),
                pltpu.VMEM((half_d, 2 * t), BF16),
                pltpu.VMEM((2, 2, 2 * t, fc), BF16),
                pltpu.VMEM((2, 3, 2 * t, fc), BF16),
                pltpu.VMEM((2, 2, half_d, fc), F32),
                dma((2,)),
                dma((2,)),
                dma((5,)),
                dma((2, PARTS)),
                dma((3, PARTS)),
                dma((2, PARTS)),
                dma((2, PARTS)),
            ]
            + cube.groups(F32)
            + cube.sems(1),
            compiler_params=params(2),
            name="table",
        )(ids, dx_own, dm, down_shard, deh, a_t, gt, u)
        depth = 4
        loss, de, grad_gate, grad_up, grad_down = pl.pallas_call(
            weight_kernel,
            out_shape=(sds((1, 1), F32), sds((real, d), F32), sds((half_d, f), F32), sds((half_d, f), F32), sds((half_f, d), F32)),
            in_specs=[smem] + [hbm] * 8,
            out_specs=(smem,) + (hbm,) * 4,
            scratch_shapes=[
                pltpu.VMEM((half_d, 2 * t), BF16),
                pltpu.VMEM((2 * t, d), BF16),
                pltpu.VMEM((depth, 3, 2 * t, fc), BF16),
                pltpu.VMEM((depth, 2, half_d, fc), F32),
                pltpu.VMEM((2, 2, half_d, fc), F32),
                pltpu.VMEM((2, fc, d), F32),
                pltpu.VMEM((vb, d), F32),
                pltpu.VMEM((real, d), F32),
                dma((4,)),
                dma((3, depth)),
                dma((2, depth)),
                dma((3, 2)),
                dma((2, depth)),
            ],
            compiler_params=pltpu.CompilerParams(vmem_limit_bytes=VMEM_LIMIT, has_side_effects=True),
            name="weights",
        )(loss, de, a_t, d_gate, d_up, act, dmf, got_g, got_u)
        return loss.reshape(()), de, grad_gate, grad_up, grad_down

    return jax.shard_map(device_step, mesh=mesh, in_specs=(tok_spec, tok_spec, row_spec, weight_spec, weight_spec, weight_spec, P(), P()), out_specs=(P(), row_spec, weight_spec, weight_spec, weight_spec), check_vma=False)
```

```python
import functools
import itertools

import jax
import jax.numpy as jnp
from jax import lax
from jax.experimental import pallas as pl
from jax.experimental.pallas import tpu as pltpu
from jax.sharding import PartitionSpec as P

EPS = 1e-6
MESH = pl.DeviceIdType.MESH
VMEM_LIMIT = 67043328
F32 = jnp.float32
BF16 = jnp.bfloat16
COLORS = 3
DIRECT = 3
PARTS = 8
RING = 4
TOP, SUM, LABEL = range(3)


def contract(a, b, dims):
    return lax.dot_general(a, b, (dims, ((), ())), preferred_element_type=F32)


def nn(a, b):
    return contract(a, b, ((1,), (0,)))


def nt(a, b):
    return contract(a, b, ((1,), (1,)))


def tn(a, b):
    return contract(a, b, ((0,), (0,)))


def span(i, n):
    return pl.ds(pl.multiple_of(i * n, n), n)


def loop(lo, hi, body):
    def step(i, carry):
        body(i)
        return carry

    lax.fori_loop(lo, hi, step, 0)


def mean(v):
    return jnp.mean(v, axis=-1, keepdims=True)


def rms_scale(values, gain):
    return values * lax.rsqrt(mean(values * values) + EPS) * gain


def rms_back(values, gain, grad):
    r = lax.rsqrt(mean(values * values) + EPS)
    gg = grad * gain
    return r * gg - values * (r * r * r) * mean(values * gg)


def one_hot(rows, ids):
    return (lax.broadcasted_iota(jnp.int32, (rows, ids.shape[-1]), 0) == ids).astype(F32).astype(BF16)


def table_rows(cube, real, vb, ids):
    here = ids - (2 * cube.m + cube.c) * real
    there = ids - (2 * cube.m + 1 - cube.c) * real
    return jnp.where((here >= 0) & (here < real), here, jnp.where((there >= 0) & (there < real), vb + there, -1))


class Local:
    def __init__(self, sems):
        self.sems, self.free = sems, itertools.count()

    def __call__(self, src, dst):
        return pltpu.make_async_copy(src, dst, self.sems.at[next(self.free)])


class Cube:
    def __init__(self, model, rows, width):
        axes = 1
        while RING**axes < model:
            axes += 1
        self.axes, self.nb, self.rows = axes, 2 * axes, rows
        self.direct = min(DIRECT, self.nb - 1)
        self.walk = self.nb - self.direct
        self.peers = 2**self.direct - 1
        self.last = rows >> self.nb
        tiles = width // 128
        big = -(-tiles // COLORS) * 128
        self.widths = [big, big, width - 2 * big]
        self.starts = [0, big, 2 * big]

    def dim(self, k, s):
        d = (k + s) % self.nb
        return d % self.axes, d // self.axes

    def bind(self, psend=None, precv=None):
        self.m = lax.axis_index("model")
        self.c = lax.axis_index("fsdp")
        self.psend, self.precv, self.free = psend, precv, itertools.count()
        self.digits = [(self.m // RING**a) % RING for a in range(self.axes)]
        self.bit, self.base = [], []
        for k in range(COLORS):
            bits, bases = [], [0]
            for s in range(self.nb):
                a, kind = self.dim(k, s)
                b = self.digits[a]
                v0, v1 = (b % 2 + b // 2) % 2, b // 2
                bits.append(v0 + ((kind + self.c) % 2) * (v1 - v0))
                bases.append(bases[-1] + bits[-1] * (self.rows >> len(bits)))
            self.bit.append(bits)
            self.base.append(bases)

    def toggled(self, k, steps):
        digits = list(self.digits)
        for s in steps:
            a, kind = self.dim(k, s)
            near = 1 - 2 * (digits[a] % 2)
            digits[a] = digits[a] + near + ((kind + self.c) % 2) * (RING - 1 - 2 * digits[a] - near)
        return sum(v * RING**a for a, v in enumerate(digits))

    def group(self, q):
        return [self.walk + i for i in range(self.direct) if (q >> i) % 2]

    def ring_peer(self, a, step):
        b = self.digits[a]
        return self.m + RING**a * ((b + step) % RING - b)

    def arrive(self, rings=False):
        peers = [(self.m, 1 - self.c)]
        for k in range(COLORS):
            steps = [[s] for s in range(self.walk)] + [self.group(q + 1) for q in range(self.peers)]
            peers += [(self.toggled(k, st), self.c) for st in steps]
        if rings:
            peers += [(self.ring_peer(a, step), self.c) for a in range(self.axes) for step in range(1, RING)]
        for peer in peers:
            pl.semaphore_signal(pltpu.get_barrier_semaphore(), inc=1, device_id=peer, device_id_type=MESH)
        self.expected = len(peers)

    def meet(self):
        pl.semaphore_wait(pltpu.get_barrier_semaphore(), self.expected)

    def place(self, k, j):
        pos = []
        for c in range(2):
            p = 0
            for s in range(self.nb):
                a, kind = self.dim(k, s)
                p = 2 * p + (j >> (a + self.axes * ((kind + c) % 2))) % 2
            pos.append(p * self.last)
        return self.rows_at(pos[0] + self.c * (pos[1] - pos[0]), self.last)

    def rows_at(self, start, size):
        return pl.ds(pl.multiple_of(start, self.last), size)

    def cols(self, k):
        return pl.ds(self.starts[k], self.widths[k])

    def pieces(self):
        return itertools.product(range(2**self.nb), range(COLORS))

    def spread(self, nat, bufs):
        for j, k in self.pieces():
            bufs[k][self.place(k, j), :] = nat[span(j, self.last), self.cols(k)]

    def collect(self, bufs, nat, half=None):
        start = 0 if half is None else half * self.rows
        for j, k in self.pieces():
            nat[self.rows_at(start + j * self.last, self.last), self.cols(k)] = bufs[k][self.place(k, j), :]

    def own(self, k):
        return self.rows_at(self.base[k][-1], self.last)

    def put_own(self, bufs, value):
        for k in range(COLORS):
            bufs[k][self.own(k), :] = value[:, self.starts[k] : self.starts[k] + self.widths[k]]

    def get_own(self, bufs):
        return jnp.concatenate([bufs[k][self.own(k), :] for k in range(COLORS)], axis=1)

    def send(self, src, dst, sems, index, peer):
        return pltpu.make_async_remote_copy(
            src_ref=src, dst_ref=dst, send_sem=sems[0].at[index], recv_sem=sems[1].at[index], device_id=(peer, self.c), device_id_type=MESH
        )

    def flip(self, k, steps):
        return sum((1 - 2 * self.bit[k][s]) * (self.rows >> (s + 1)) for s in steps)

    def start(self, copies):
        for copy in copies:
            copy.start()

    def finish(self, copies):
        for copy in copies:
            copy.wait()

    def rs_parts(self, k, s):
        base, off, ln = self.base[k], self.rows - (self.rows >> s), self.rows >> (s + 1)
        if s == self.walk:
            first = self.rows - (self.rows >> s)
            return [(base[-1] + self.flip(k, self.group(q + 1)), base[-1], first + q * self.last, self.last) for q in range(self.peers)]
        away = base[s + 1] + self.flip(k, [s])
        if s == self.walk - 1:
            return [(away, base[s + 1], off, ln)]
        half = ln // 2
        b = self.bit[k][s + 1]
        return [(away + x * half, base[s + 1] + x * half, off + i * half, half) for i, x in enumerate((1 - b, b))]

    def rs_copies(self, bufs, recvs, sems, k, s, which=slice(None)):
        out = []
        for i, (src, _, dst, ln) in list(enumerate(self.rs_parts(k, s)))[which]:
            peer = self.toggled(k, self.group(i + 1) if s == self.walk else [s])
            at = 2 * s + i
            out.append(self.send(bufs[k].at[self.rows_at(src, ln)], recvs[k].at[pl.ds(dst, ln)], sems, (k, at), peer))
        return out

    def rs_take(self, bufs, recvs, sems, k, s, which):
        parts = self.rs_parts(k, s)[which]
        self.finish(self.rs_copies(bufs, recvs, sems, k, s, which))
        at = self.rows_at(parts[0][1], parts[0][3])
        got = sum(recvs[k][pl.ds(dst, ln), :].astype(F32) for _, _, dst, ln in parts)
        bufs[k][at, :] = (bufs[k][at, :].astype(F32) + got).astype(bufs[k].dtype)

    def reduce_scatter(self, bufs, recvs, sems, fill=None):
        for k in range(COLORS):
            self.start(self.rs_copies(bufs, recvs, sems, k, 0))
        for s in range(self.walk + 1):
            if fill is not None:
                fill(s)
            for k in range(COLORS):
                if 0 < s < self.walk:
                    self.rs_take(bufs, recvs, sems, k, s - 1, slice(1, 2))
                if s < self.walk:
                    self.rs_take(bufs, recvs, sems, k, s, slice(0, 1))
                    self.start(self.rs_copies(bufs, recvs, sems, k, s + 1))
                else:
                    self.rs_take(bufs, recvs, sems, k, s, slice(None))

    def blocks(self, s):
        later = range(s + 1, self.walk)
        return [st for n in range(len(later) + 1) for st in itertools.combinations(later, n)]

    def ag_block(self, bufs, sems, k, s, block):
        at = self.base[k][self.walk] + self.flip(k, block)
        ref = bufs[k].at[self.rows_at(at, self.rows >> self.walk)]
        index = 2 ** (self.walk - 1 - s) - 1 + self.blocks(s).index(block)
        return self.send(ref, ref, sems, (k, self.peers + index), self.toggled(k, [s]))

    def ag_direct(self, bufs, sems, k):
        ref = bufs[k].at[self.own(k)]
        return [self.send(ref, ref, sems, (k, q), self.toggled(k, self.group(q + 1))) for q in range(self.peers)]

    def ag_start(self, bufs, sems):
        for k in range(COLORS):
            self.start(self.ag_direct(bufs, sems, k))
        return self.walk

    def ag_next(self, bufs, sems, s):
        if s == self.walk:
            for k in range(COLORS):
                self.finish(self.ag_direct(bufs, sems, k))
                for to in range(s - 1, -1, -1):
                    self.ag_block(bufs, sems, k, to, ()).start()
            return s - 1
        for block in self.blocks(s):
            for k in range(COLORS):
                self.ag_block(bufs, sems, k, s, block).wait()
                for to in range(s - 1, -1, -1):
                    self.ag_block(bufs, sems, k, to, tuple(sorted(block + (s,)))).start()
        return s - 1

    def all_gather(self, bufs, sems, fill=None):
        s = self.ag_start(bufs, sems)
        while s >= 0:
            if fill is not None:
                fill(s)
            s = self.ag_next(bufs, sems, s)

    def pair(self, src, dst):
        i = next(self.free)
        return pltpu.make_async_remote_copy(
            src_ref=src, dst_ref=dst, send_sem=self.psend.at[i], recv_sem=self.precv.at[i], device_id=(self.m, 1 - self.c), device_id_type=MESH
        )

    def groups(self, *dtypes):
        return [pltpu.VMEM((self.rows, w), dtype) for dtype in dtypes for w in self.widths]

    def sems(self, n):
        return [pltpu.SemaphoreType.DMA((COLORS, self.peers + max(2 * self.walk, 2**self.walk)))] * (2 * n)


def by(n, items):
    return [items[i : i + n] for i in range(0, len(items), n)]


def embed_kernel(cube, vb, ids, e_ref, wg, wu, wd, g1, g2, hn, ep_o, wgh_o, wuh_o, h_own, gt_own, u_own, x_own, *scratch):
    e_s, wd_s, ep, wgh, wuh, xnat, x32, mp, mr, psend, precv, lsem, *rest = scratch
    xb, xr, hb = by(COLORS, rest[: 3 * COLORS])
    rs_sems, hg_sems = by(2, rest[3 * COLORS :])
    cube.bind(psend, precv)
    cube.arrive()
    local = Local(lsem)
    c = cube.c
    d = hn.shape[1]
    half_d, half_f = d // 2, wgh.shape[1]
    last = cube.last
    mine_d = span(c, half_d)
    e_local = local(e_ref, e_s)
    e_local.start()
    w_local = [local(wd, wd_s), local(wg.at[:, span(c, half_f)], wgh.at[mine_d]), local(wu.at[:, span(c, half_f)], wuh.at[mine_d])]
    e_local.wait()
    real = e_s.shape[0]
    body = real - real % 16
    if body > 0:
        ep[pl.ds(0, body), :] = e_s[pl.ds(0, body), :]
    if vb > body:
        ep[pl.ds(body, vb - body), :] = jnp.zeros((vb - body, d), BF16)
        ep[pl.ds(body, real - body), :] = e_s[pl.ds(body, real - body), :]
    cube.meet()
    e_pair = cube.pair(ep.at[pl.ds(0, vb)], ep.at[pl.ds(vb, vb)])
    e_pair.start()
    w_pair = [cube.pair(src.at[:, span(1 - c, half_f)], dst.at[mine_d]) for src, dst in ((wg, wgh), (wu, wuh))]
    cube.start(w_pair + w_local)
    chunk = min(512, cube.rows)

    def lookup(i):
        at = span(i, chunk)
        xnat[at, :] = tn(one_hot(vb, table_rows(cube, real, vb, ids[:, at])), ep[pl.ds(0, vb), :]).astype(BF16)

    def lookup_other(i):
        at = span(i, chunk)
        found = tn(one_hot(vb, table_rows(cube, real, vb, ids[:, at]) - vb), ep[pl.ds(vb, vb), :])
        xnat[at, :] = (xnat[at, :].astype(F32) + found).astype(BF16)

    loop(0, cube.rows // chunk, lookup)
    e_pair.wait()
    outs = [local(ep, ep_o), local(wgh, wgh_o), local(wuh, wuh_o)]
    outs[0].start()
    loop(0, cube.rows // chunk, lookup_other)
    cube.spread(xnat, xb)
    cube.reduce_scatter(xb, xr, rs_sems)
    x_own[...] = cube.get_own(xb)
    x32[0] = x_own[...]
    x_pair = cube.pair(x32.at[0], x32.at[1])
    x_pair.start()
    cube.finish(w_local + w_pair)
    cube.start(outs[1:])
    x_pair.wait()
    a_rows = rms_scale(x32[...].reshape(2 * last, d).astype(F32), g1[...]).astype(BF16)
    parts = 4
    fc = half_f // parts
    total = jnp.zeros((2 * last, d), F32)
    for p in range(parts):
        at = pl.ds(p * fc, fc)
        gate = nn(a_rows, wgh[:, at]).astype(BF16)
        up = nn(a_rows, wuh[:, at]).astype(BF16)
        gt_own[:, at] = gate
        u_own[:, at] = up
        gate_f = gate.astype(F32)
        act = (gate_f * jax.nn.sigmoid(gate_f) * up.astype(F32)).astype(BF16)
        total = total + nn(act, wd_s[at, :])
    mp[...] = total.reshape(2, last, d)
    m_pair = cube.pair(mp.at[1], mr)
    m_pair.start()
    m_pair.wait()
    h_rows = x_own[...].astype(F32) + (mp[0] + mr[...]).astype(BF16).astype(F32)
    h_own[...] = h_rows
    cube.put_own(hb, rms_scale(h_rows, g2[...]).astype(BF16))
    cube.all_gather(hb, hg_sems)
    cube.collect(hb, hn)
    cube.finish(outs)


def head_kernel(
    cube, vb, real, num_tokens, hn_i, ep_i, labels, h_own, g2, x_own, g1, gt_own, u_own, wgh_i, wuh_i, wd_i,
    dm_nat, loss, deh_o, dx_own, at_o, gt_o, u_o, *scratch
):
    hn, ep, z, dz, nat, stats, lbuf, dm32, mp, mr, wgh, wuh, wd, xf, tstage, stage, psend, precv, lsem, osem, st_s, st_r, *rest = scratch
    rb, rr, gb, xg = by(COLORS, rest[: 4 * COLORS])
    rs_sems, ag_sems, xg_sems = by(2, rest[4 * COLORS :])
    cube.bind(psend, precv)
    cube.arrive(rings=True)
    local = Local(lsem)
    c = cube.c
    t, d = hn.shape
    walk, last = cube.walk, cube.last
    first = [local(ep_i, ep), local(hn_i, hn)]
    cube.start(first)
    w_copies = [local(wgh_i, wgh), local(wuh_i, wuh), local(wd_i, wd)]
    cube.start(w_copies)
    cube.put_own(xg, x_own[...])
    chunk = min(256, t)
    chunks = t // chunk
    mine = cube.digits[0]

    def logits(i):
        at = span(i, chunk)
        row = lax.broadcasted_iota(jnp.int32, (2 * vb, chunk), 0)
        valid = (row < real) | ((row >= vb) & (row < vb + real))
        zz = jnp.where(valid, nt(ep[...], hn[at, :]), -1e38)
        z[:, at] = zz
        top = jnp.max(zz, axis=0, keepdims=True)
        parts = {TOP: top, SUM: jnp.exp(zz - top), LABEL: jnp.where(row == table_rows(cube, real, vb, labels[:, at]), zz, 0.0)}
        for r, v in parts.items():
            stats[0, mine, pl.ds(r, 1), at] = v if r == TOP else jnp.sum(v, axis=0, keepdims=True)

    cube.finish(first)
    loop(0, chunks // 2, logits)
    cube.meet()
    xstep = cube.ag_start(xg, xg_sems)
    loop(chunks // 2, chunks, logits)
    xstep = cube.ag_next(xg, xg_sems, xstep)
    for a in range(cube.axes):
        here = stats.at[a, cube.digits[a]]
        copies = [cube.send(here, here, (st_s, st_r), (a, step - 1), cube.ring_peer(a, step)) for step in range(1, RING)]
        cube.start(copies)
        cube.finish(copies)
        if xstep > 1:
            xstep = cube.ag_next(xg, xg_sems, xstep)
        tops, sums, marks = [[stats[a, i, pl.ds(r, 1), :] for i in range(RING)] for r in range(LABEL + 1)]
        top = functools.reduce(jnp.maximum, tops)
        total = sum(v * jnp.exp(m - top) for m, v in zip(tops, sums))
        label = sum(marks)
        slot = cube.digits[a + 1] if a + 1 < cube.axes else 0
        for r, v in enumerate((top, total, label)):
            stats[a + 1, slot, pl.ds(r, 1), :] = v
    while xstep > 0:
        xstep = cube.ag_next(xg, xg_sems, xstep)
    tok_loss = jnp.sum(top + jnp.log(total) - label, axis=1, keepdims=True)
    lbuf[c] = jnp.broadcast_to(tok_loss, lbuf.shape[1:])
    l_pair = cube.pair(lbuf.at[c], lbuf.at[c])
    l_pair.start()
    final = stats.at[cube.axes, 0]
    deh = z.at[:, pl.ds(0, d)]
    deh_out = local(deh, deh_o)

    wide = min(512, t)

    def backward(i):
        at = span(i, wide)
        row = lax.broadcasted_iota(jnp.int32, (2 * vb, wide), 0)
        soft = jnp.exp(z[:, at] - final[pl.ds(TOP, 1), at]) / final[pl.ds(SUM, 1), at]
        dzz = (jnp.where(row == table_rows(cube, real, vb, labels[:, at]), soft - 1.0, soft) / num_tokens).astype(BF16)
        dz[:, at] = dzz
        nat[at, :] = tn(dzz, ep[...])

    loop(0, t // wide, backward)
    cube.spread(nat, rb)
    mine_t = span(c, t)
    xf_pair = cube.pair(xf.at[mine_t], xf.at[mine_t])
    d_pair = cube.pair(dm32.at[0], dm32.at[1])
    m_pair = cube.pair(mp.at[1], mr)
    t_out = local(tstage, at_o)
    fc = wgh.shape[1] // PARTS

    def out_copies(p):
        slot = lax.rem(p, 2)
        return [pltpu.make_async_copy(stage.at[slot, i], dst.at[p], osem.at[i, slot]) for i, dst in enumerate((gt_o, u_o))]

    def gate_up(p):
        @pl.when(p >= 2)
        def _():
            cube.finish(out_copies(p - 2))

        cols = span(p, fc)
        slot = stage.at[lax.rem(p, 2)]

        def body(i):
            at = span(i, t)
            for which, w in enumerate((wgh, wuh)):
                slot[which, at, :] = nn(xf[at, :], w[:, cols]).astype(BF16)

        loop(0, 2, body)
        cube.start(out_copies(p))

    def normalise(i):
        at = span(c * chunks + i, chunk)
        xf[at, :] = rms_scale(xf[at, :].astype(F32), g1[...]).astype(BF16)

    def transpose(half, i):
        at = span(half * chunks + i, chunk)
        tstage[:, at] = xf[at, :].astype(F32).T.astype(BF16)

    def head_grad(i):
        deh[span(i, vb), :] = nn(dz[span(i, vb), :], hn[...])

    todo = [0]

    def run(n):
        lo, hi = todo[0], min(todo[0] + n, PARTS)
        todo[0] = hi
        if lo < hi:
            loop(lo, hi, gate_up)

    def rs_fill(s):
        if s == 0:
            cube.ag_next(xg, xg_sems, xstep)
            cube.collect(xg, xf, c)
            loop(0, chunks, normalise)
            xf_pair.start()
            loop(0, 2, head_grad)
            deh_out.start()
            loop(0, chunks, functools.partial(transpose, c))
        elif s == 1:
            cube.finish(w_copies + [xf_pair])
            loop(0, chunks, functools.partial(transpose, 1 - c))
            t_out.start()
            run(2)
        else:
            run(2)

    cube.reduce_scatter(rb, rr, rs_sems, rs_fill)
    dh = rms_back(h_own[...], g2[...], cube.get_own(rb))
    dm = dh.astype(BF16)
    cube.put_own(gb, dm)
    dm32[0] = dm

    def token_back(lo, hi):
        w = wgh.shape[1] // RING
        part = jnp.zeros((2 * last, d), F32)
        for p in range(lo, hi):
            at = pl.ds(p * w, w)
            d_act = nt(dm32[...].reshape(2 * last, d), wd[at, :])
            gate = gt_own[:, at].astype(F32)
            sig = jax.nn.sigmoid(gate)
            d_gate = (d_act * u_own[:, at].astype(F32) * (sig * (1.0 + gate * (1.0 - sig)))).astype(BF16)
            d_up = (d_act * (gate * sig)).astype(BF16)
            part = part + (nt(d_gate, wgh[:, at]) + nt(d_up, wuh[:, at]))
        part = part.reshape(mp.shape)
        mp[...] = part if lo == 0 else mp[...] + part

    def ag_fill(s):
        if s == walk:
            d_pair.wait()
            token_back(0, 2)
        elif s == walk - 1:
            token_back(2, RING)
            m_pair.start()
        else:
            run(1)

    d_pair.start()
    cube.all_gather(gb, ag_sems, ag_fill)
    cube.collect(gb, dm_nat)
    run(PARTS)
    m_pair.wait()
    dx_own[...] = dh + rms_back(x_own[...].astype(F32), g1[...], mp[0] + mr[...])
    l_pair.wait()
    loss[0, 0] = jnp.max((lbuf[0] + lbuf[1]) / num_tokens)
    cube.finish([t_out, deh_out])
    for p in (PARTS - 2, PARTS - 1):
        cube.finish(out_copies(p))


def table_kernel(cube, vb, real, ids, dx_own, dm_i, wd_i, deh, at_i, gt_i, u_i, de, dmf_o, act_o, dg_o, du_o, got_g, got_u, *scratch):
    dmf, wd, nat, mix, de_r, aoth, fin, fout, part, psend, precv, lsem, isem, osem, gsend, grecv, *rest = scratch
    gb, ag_sems = rest[:COLORS], rest[COLORS:]
    cube.bind(psend, precv)
    cube.arrive()
    c = cube.c
    t = cube.rows
    fc = wd.shape[0] // PARTS
    half_d = aoth.shape[0]
    local = Local(lsem)
    mine_t = span(c, t)
    dm_copy, wd_copy, a_copy = local(dm_i, dmf.at[mine_t]), local(wd_i, wd), local(at_i.at[span(1 - c, half_d)], aoth)
    deh_copy, dm_out = local(deh, mix), local(dmf, dmf_o)
    dm_pair = cube.pair(dm_i, dmf.at[mine_t])

    def in_copies(p):
        slot = lax.rem(p, 2)
        return [pltpu.make_async_copy(src.at[p], fin.at[slot, i], isem.at[i, slot]) for i, src in enumerate((gt_i, u_i))]

    def out_copies(p):
        slot = lax.rem(p, 2)
        return [pltpu.make_async_copy(fout.at[slot, i], dst.at[p], osem.at[i, slot]) for i, dst in enumerate((act_o, dg_o, du_o))]

    def send_copies(p):
        slot = lax.rem(p, 2)
        return [
            pltpu.make_async_remote_copy(
                src_ref=part.at[slot, i], dst_ref=dst.at[p], send_sem=gsend.at[i, p], recv_sem=grecv.at[i, p], device_id=(cube.m, 1 - c), device_id_type=MESH
            )
            for i, dst in enumerate((got_g, got_u))
        ]

    def drain(p):
        cube.finish(out_copies(p))
        for copy in send_copies(p):
            copy.wait_send()

    cube.start([dm_copy, wd_copy] + in_copies(0) + [a_copy, deh_copy])
    cube.put_own(gb, dx_own[...])
    cube.meet()
    step = cube.ag_start(gb, ag_sems)
    dm_pair.start()
    cube.finish([dm_copy, wd_copy, a_copy])

    def chunk_work(p, first=False):
        @pl.when(p + 1 < PARTS)
        def _():
            cube.start(in_copies(p + 1))

        cube.finish(in_copies(p))

        @pl.when(p >= 2)
        def _():
            drain(p - 2)

        slot = lax.rem(p, 2)
        src, dst, res = fin.at[slot], fout.at[slot], part.at[slot]

        def body(half):
            at = span(half, t)
            d_act = nt(dmf[at, :], wd[span(p, fc), :])
            gate = src[0, at, :].astype(F32)
            up = src[1, at, :].astype(F32)
            sig = jax.nn.sigmoid(gate)
            silu = gate * sig
            outs = (silu * up, d_act * up * (sig * (1.0 + gate * (1.0 - sig))), d_act * silu)
            for which, v in enumerate(outs):
                dst[which, at, :] = v.astype(BF16)

        if first:
            body(c)
            dm_pair.wait()
            dm_out.start()
            body(1 - c)
        else:
            loop(0, 2, body)
        for which in range(2):
            res[which] = nn(aoth[...], dst[which + 1])
        cube.start(out_copies(p) + send_copies(p))

    chunk_work(0, True)
    step = cube.ag_next(gb, ag_sems, step)
    p = 1
    while p < PARTS:
        q = min(p + 2, PARTS)
        loop(p, q, chunk_work)
        if step >= 0:
            step = cube.ag_next(gb, ag_sems, step)
        p = q
    while step >= 0:
        step = cube.ag_next(gb, ag_sems, step)
    cube.collect(gb, nat)
    cube.finish([deh_copy, dm_out])
    chunk = min(256, t)

    def scatter(half, i):
        at = span(i, chunk)
        rows = pl.ds(half * vb, vb)
        hot = one_hot(vb, table_rows(cube, real, vb, ids[:, at]) - half * vb)
        val = nat[at, :]
        hi = val.astype(BF16)
        rest = val - hi.astype(F32)
        mid = rest.astype(BF16)
        low = (rest - mid.astype(F32)).astype(BF16)
        mix[rows, :] = mix[rows, :] + ((nn(hot, low) + nn(hot, mid)) + nn(hot, hi))

    loop(0, t // chunk, functools.partial(scatter, 1))
    e_pair = cube.pair(mix.at[pl.ds(vb, vb)], de_r)
    e_pair.start()
    loop(0, t // chunk, functools.partial(scatter, 0))
    drain(PARTS - 2)
    drain(PARTS - 1)
    for p in range(PARTS):
        for copy in send_copies(p):
            copy.wait_recv()
    e_pair.wait()
    de[...] = mix[pl.ds(0, vb), :] + de_r[...]


def weight_kernel(loss, de, at_i, dg, du, act, dmf_i, got_g, got_u, loss_o, de_o, og, ou, od, *scratch):
    aown, dmf, ring, abuf, gring, ostage, dstage, de_s, de_t, lsem, rsem, asem, gsem, osem, dsem, xsem = scratch
    c = lax.axis_index("fsdp")
    depth, fc = ring.shape[0], ring.shape[-1]
    parts, half_f = dg.shape[0], dg.shape[0] * fc
    quad = abuf.shape[-1] // fc
    local = Local(lsem)
    a_copy, dm_copy = local(at_i.at[span(c, aown.shape[0])], aown), local(dmf_i, dmf)
    de_in, de_out = local(de, de_s), local(de_t, de_o)

    def reads(p):
        slot = lax.rem(p, depth)
        return [pltpu.make_async_copy(src.at[p], ring.at[slot, i], rsem.at[i, slot]) for i, src in enumerate((dg, du))]

    def got(p):
        slot = lax.rem(p, depth)
        return [pltpu.make_async_copy(src.at[p], gring.at[slot, i], gsem.at[i, slot]) for i, src in enumerate((got_g, got_u))]

    def acts(q):
        return [pltpu.make_async_copy(act.at[q * quad + i], abuf.at[q, :, pl.ds(i * fc, fc)], asem.at[q, i]) for i in range(quad)]

    def columns(half, p):
        return pl.ds(pl.multiple_of(half * half_f + p * fc, fc), fc)

    def passes(p):
        slot = lax.rem(p, depth)
        return [pltpu.make_async_copy(gring.at[slot, i], dst.at[:, columns(1 - c, p)], xsem.at[i, slot]) for i, dst in enumerate((og, ou))]

    def writes(p):
        slot = lax.rem(p, 2)
        return [pltpu.make_async_copy(ostage.at[slot, i], dst.at[:, columns(c, p)], osem.at[i, slot]) for i, dst in enumerate((og, ou))]

    def down(q):
        return pltpu.make_async_copy(dstage.at[q], od.at[span(q, quad * fc)], dsem.at[q])

    def each(copies, verb):
        for copy in copies:
            getattr(copy, verb)()

    def fetch(p):
        each(reads(p) + got(p), "start")

    a_copy.start()
    fetch(0)
    fetch(1)
    each(acts(0), "start")
    dm_copy.start()
    for p in range(2, depth):
        fetch(p)
    de_in.start()
    a_copy.wait()
    loss_o[0, 0] = loss[0, 0]

    def body(p):
        slot, oslot = lax.rem(p, depth), lax.rem(p, 2)
        each(got(p), "wait")
        each(passes(p), "start")
        each(reads(p), "wait")

        @pl.when(p >= 2)
        def _():
            each(writes(p - 2), "wait")

        for i in range(2):
            ostage[oslot, i] = nn(aown[...], ring[slot, i])
        each(writes(p), "start")

        @pl.when(p >= 1)
        def _():
            each(passes(p - 1), "wait")

        @pl.when((p >= 1) & (p - 1 + depth < parts))
        def _():
            fetch(p - 1 + depth)

    def group(q):
        loop(q * quad, (q + 1) * quad, body)

        @pl.when(q == 0)
        def _():
            each(acts(1), "start")
            dm_copy.wait()

        each(acts(q), "wait")
        dstage[q] = tn(abuf[q], dmf[...])
        down(q).start()

    loop(0, parts // quad, group)
    de_in.wait()
    de_t[...] = de_s[pl.ds(0, de_t.shape[0]), :]
    de_out.start()
    each(passes(parts - 1) + writes(parts - 2) + writes(parts - 1), "wait")
    each([down(q) for q in range(parts // quad)], "wait")
    de_out.wait()


def solution(mesh):
    model, fsdp_size = mesh.shape["model"], mesh.shape["fsdp"]
    tok_spec = P("fsdp", None)
    row_spec = P(("model", "fsdp"), None)
    weight_spec = P("fsdp", None)
    vmem = pl.BlockSpec(memory_space=pltpu.VMEM)
    hbm = pl.BlockSpec(memory_space=pl.ANY)
    sds = jax.ShapeDtypeStruct
    dma = pltpu.SemaphoreType.DMA

    def params(cid):
        return pltpu.CompilerParams(collective_id=cid, has_side_effects=True, vmem_limit_bytes=VMEM_LIMIT)

    def device_step(tok_ids, tok_labels, table_shard, gate_shard, up_shard, down_shard, gain_in, gain_out):
        t = tok_ids.size
        num_tokens = t * fsdp_size
        real, d = table_shard.shape
        vb = -(-real // 16) * 16
        f = gate_shard.shape[1]
        half_f, half_d = f // 2, d // 2
        fc = half_f // PARTS
        cube = Cube(model, t, d)
        last = cube.last
        ids, labels = tok_ids.reshape(1, t), tok_labels.reshape(1, t)
        smem = pl.BlockSpec(memory_space=pltpu.SMEM)
        g1, g2 = gain_in.reshape(1, d), gain_out.reshape(1, d)
        act_own = sds((2 * last, half_f), BF16)
        w_half = sds((d, half_f), BF16)
        hn, ep, wgh, wuh, h_own, gt_own, u_own, x_own = pl.pallas_call(
            functools.partial(embed_kernel, cube, vb),
            out_shape=(sds((t, d), BF16), sds((2 * vb, d), BF16), w_half, w_half, sds((last, d), F32), act_own, act_own, sds((last, d), BF16)),
            in_specs=[vmem, hbm, hbm, hbm, hbm, vmem, vmem],
            out_specs=(vmem, hbm, hbm, hbm, vmem, vmem, vmem, vmem),
            scratch_shapes=[
                pltpu.VMEM((real, d), BF16),
                pltpu.VMEM((half_f, d), BF16),
                pltpu.VMEM((2 * vb, d), BF16),
                pltpu.VMEM((d, half_f), BF16),
                pltpu.VMEM((d, half_f), BF16),
                pltpu.VMEM((t, d), BF16),
                pltpu.VMEM((2, last, d), BF16),
                pltpu.VMEM((2, last, d), F32),
                pltpu.VMEM((last, d), F32),
                dma((8,)),
                dma((8,)),
                dma((8,)),
            ]
            + cube.groups(BF16, BF16, BF16)
            + cube.sems(2),
            compiler_params=params(0),
            name="embed",
        )(ids, table_shard, gate_shard, up_shard, down_shard, g1, g2)
        chunked = sds((PARTS, 2 * t, fc), BF16)
        dm, loss, deh, dx_own, a_t, gt, u = pl.pallas_call(
            functools.partial(head_kernel, cube, vb, real, num_tokens),
            out_shape=(sds((t, d), BF16), sds((1, 1), F32), sds((2 * vb, d), F32), sds((last, d), F32), sds((d, 2 * t), BF16), chunked, chunked),
            in_specs=[hbm] * 2 + [vmem] * 7 + [hbm] * 3,
            out_specs=(vmem, smem, hbm, vmem) + (hbm,) * 3,
            scratch_shapes=[
                pltpu.VMEM((t, d), BF16),
                pltpu.VMEM((2 * vb, d), BF16),
                pltpu.VMEM((2 * vb, max(t, d)), F32),
                pltpu.VMEM((2 * vb, t), BF16),
                pltpu.VMEM((t, d), F32),
                pltpu.VMEM((cube.axes + 1, RING, RING, t), F32),
                pltpu.VMEM((2, 8, 128), F32),
                pltpu.VMEM((2, last, d), BF16),
                pltpu.VMEM((2, last, d), F32),
                pltpu.VMEM((last, d), F32),
                pltpu.VMEM((d, half_f), BF16),
                pltpu.VMEM((d, half_f), BF16),
                pltpu.VMEM((half_f, d), BF16),
                pltpu.VMEM((2 * t, d), BF16),
                pltpu.VMEM((d, 2 * t), BF16),
                pltpu.VMEM((2, 2, 2 * t, fc), BF16),
                dma((8,)),
                dma((8,)),
                dma((8,)),
                dma((2, PARTS)),
                dma((cube.axes, RING)),
                dma((cube.axes, RING)),
            ]
            + cube.groups(F32, F32, BF16, BF16)
            + cube.sems(3),
            compiler_params=params(1),
            name="head",
        )(hn, ep, labels, h_own, g2, x_own, g1, gt_own, u_own, wgh, wuh, down_shard)
        got = sds((PARTS, half_d, fc), F32)
        de, dmf, act, d_gate, d_up, got_g, got_u = pl.pallas_call(
            functools.partial(table_kernel, cube, vb, real),
            out_shape=(sds((vb, d), F32), sds((2 * t, d), BF16), chunked, chunked, chunked, got, got),
            in_specs=[vmem] * 2 + [hbm] * 6,
            out_specs=(vmem,) + (hbm,) * 6,
            scratch_shapes=[
                pltpu.VMEM((2 * t, d), BF16),
                pltpu.VMEM((half_f, d), BF16),
                pltpu.VMEM((t, d), F32),
                pltpu.VMEM((2 * vb, d), F32),
                pltpu.VMEM((vb, d), F32),
                pltpu.VMEM((half_d, 2 * t), BF16),
                pltpu.VMEM((2, 2, 2 * t, fc), BF16),
                pltpu.VMEM((2, 3, 2 * t, fc), BF16),
                pltpu.VMEM((2, 2, half_d, fc), F32),
                dma((2,)),
                dma((2,)),
                dma((5,)),
                dma((2, PARTS)),
                dma((3, PARTS)),
                dma((2, PARTS)),
                dma((2, PARTS)),
            ]
            + cube.groups(F32)
            + cube.sems(1),
            compiler_params=params(2),
            name="table",
        )(ids, dx_own, dm, down_shard, deh, a_t, gt, u)
        depth = 4
        loss, de, grad_gate, grad_up, grad_down = pl.pallas_call(
            weight_kernel,
            out_shape=(sds((1, 1), F32), sds((real, d), F32), sds((half_d, f), F32), sds((half_d, f), F32), sds((half_f, d), F32)),
            in_specs=[smem] + [hbm] * 8,
            out_specs=(smem,) + (hbm,) * 4,
            scratch_shapes=[
                pltpu.VMEM((half_d, 2 * t), BF16),
                pltpu.VMEM((2 * t, d), BF16),
                pltpu.VMEM((depth, 2, 2 * t, fc), BF16),
                pltpu.VMEM((2, 2 * t, half_f // 2), BF16),
                pltpu.VMEM((depth, 2, half_d, fc), F32),
                pltpu.VMEM((2, 2, half_d, fc), F32),
                pltpu.VMEM((2, half_f // 2, d), F32),
                pltpu.VMEM((vb, d), F32),
                pltpu.VMEM((real, d), F32),
                dma((4,)),
                dma((2, depth)),
                dma((2, PARTS // 2)),
                dma((2, depth)),
                dma((2, 2)),
                dma((2,)),
                dma((2, depth)),
            ],
            compiler_params=pltpu.CompilerParams(vmem_limit_bytes=VMEM_LIMIT, has_side_effects=True),
            name="weights",
        )(loss, de, a_t, d_gate, d_up, act, dmf, got_g, got_u)
        return loss.reshape(()), de, grad_gate, grad_up, grad_down

    return jax.shard_map(device_step, mesh=mesh, in_specs=(tok_spec, tok_spec, row_spec, weight_spec, weight_spec, weight_spec, P(), P()), out_specs=(P(), row_spec, weight_spec, weight_spec, weight_spec), check_vma=False)
```

```python
import functools
import itertools

import jax
import jax.numpy as jnp
from jax import lax
from jax.experimental import pallas as pl
from jax.experimental.pallas import tpu as pltpu
from jax.sharding import PartitionSpec as P

EPS = 1e-6
MESH = pl.DeviceIdType.MESH
VMEM_LIMIT = 67043328
F32 = jnp.float32
BF16 = jnp.bfloat16
COLORS = 3
DIRECT = 3
PARTS = 8
RING = 4
TOP, SUM, LABEL = range(3)


def contract(a, b, dims):
    return lax.dot_general(a, b, (dims, ((), ())), preferred_element_type=F32)


def nn(a, b):
    return contract(a, b, ((1,), (0,)))


def nt(a, b):
    return contract(a, b, ((1,), (1,)))


def tn(a, b):
    return contract(a, b, ((0,), (0,)))


def span(i, n):
    return pl.ds(pl.multiple_of(i * n, n), n)


def loop(lo, hi, body):
    def step(i, carry):
        body(i)
        return carry

    lax.fori_loop(lo, hi, step, 0)


def mean(v):
    return jnp.mean(v, axis=-1, keepdims=True)


def rms_scale(values, gain):
    return values * lax.rsqrt(mean(values * values) + EPS) * gain


def rms_back(values, gain, grad):
    r = lax.rsqrt(mean(values * values) + EPS)
    gg = grad * gain
    return r * gg - values * (r * r * r) * mean(values * gg)


def one_hot(rows, ids):
    return (lax.broadcasted_iota(jnp.int32, (rows, ids.shape[-1]), 0) == ids).astype(F32).astype(BF16)


def table_rows(cube, real, vb, ids):
    here = ids - (2 * cube.m + cube.c) * real
    there = ids - (2 * cube.m + 1 - cube.c) * real
    return jnp.where((here >= 0) & (here < real), here, jnp.where((there >= 0) & (there < real), vb + there, -1))


class Local:
    def __init__(self, sems):
        self.sems, self.free = sems, itertools.count()

    def __call__(self, src, dst):
        return pltpu.make_async_copy(src, dst, self.sems.at[next(self.free)])


class Cube:
    def __init__(self, model, rows, width):
        axes = 1
        while RING**axes < model:
            axes += 1
        self.axes, self.nb, self.rows = axes, 2 * axes, rows
        self.direct = min(DIRECT, self.nb - 1)
        self.walk = self.nb - self.direct
        self.peers = 2**self.direct - 1
        self.last = rows >> self.nb
        tiles = width // 128
        big = -(-tiles // COLORS) * 128
        self.widths = [big, big, width - 2 * big]
        self.starts = [0, big, 2 * big]

    def dim(self, k, s):
        d = (k + s) % self.nb
        return d % self.axes, d // self.axes

    def bind(self, psend=None, precv=None):
        self.m = lax.axis_index("model")
        self.c = lax.axis_index("fsdp")
        self.psend, self.precv, self.free = psend, precv, itertools.count()
        self.digits = [(self.m // RING**a) % RING for a in range(self.axes)]
        self.bit, self.base = [], []
        for k in range(COLORS):
            bits, bases = [], [0]
            for s in range(self.nb):
                a, kind = self.dim(k, s)
                b = self.digits[a]
                v0, v1 = (b % 2 + b // 2) % 2, b // 2
                bits.append(v0 + ((kind + self.c) % 2) * (v1 - v0))
                bases.append(bases[-1] + bits[-1] * (self.rows >> len(bits)))
            self.bit.append(bits)
            self.base.append(bases)

    def toggled(self, k, steps):
        digits = list(self.digits)
        for s in steps:
            a, kind = self.dim(k, s)
            near = 1 - 2 * (digits[a] % 2)
            digits[a] = digits[a] + near + ((kind + self.c) % 2) * (RING - 1 - 2 * digits[a] - near)
        return sum(v * RING**a for a, v in enumerate(digits))

    def group(self, q):
        return [self.walk + i for i in range(self.direct) if (q >> i) % 2]

    def ring_peer(self, a, step):
        b = self.digits[a]
        return self.m + RING**a * ((b + step) % RING - b)

    def arrive(self, rings=False):
        peers = [(self.m, 1 - self.c)]
        for k in range(COLORS):
            steps = [[s] for s in range(self.walk)] + [self.group(q + 1) for q in range(self.peers)]
            peers += [(self.toggled(k, st), self.c) for st in steps]
        if rings:
            peers += [(self.ring_peer(a, step), self.c) for a in range(self.axes) for step in range(1, RING)]
        for peer in peers:
            pl.semaphore_signal(pltpu.get_barrier_semaphore(), inc=1, device_id=peer, device_id_type=MESH)
        self.expected = len(peers)

    def meet(self):
        pl.semaphore_wait(pltpu.get_barrier_semaphore(), self.expected)

    def place(self, k, j):
        pos = []
        for c in range(2):
            p = 0
            for s in range(self.nb):
                a, kind = self.dim(k, s)
                p = 2 * p + (j >> (a + self.axes * ((kind + c) % 2))) % 2
            pos.append(p * self.last)
        return self.rows_at(pos[0] + self.c * (pos[1] - pos[0]), self.last)

    def rows_at(self, start, size):
        return pl.ds(pl.multiple_of(start, self.last), size)

    def cols(self, k):
        return pl.ds(self.starts[k], self.widths[k])

    def pieces(self):
        return itertools.product(range(2**self.nb), range(COLORS))

    def spread(self, nat, bufs):
        for j, k in self.pieces():
            bufs[k][self.place(k, j), :] = nat[span(j, self.last), self.cols(k)]

    def collect(self, bufs, nat, half=None):
        start = 0 if half is None else half * self.rows
        for j, k in self.pieces():
            nat[self.rows_at(start + j * self.last, self.last), self.cols(k)] = bufs[k][self.place(k, j), :]

    def own(self, k):
        return self.rows_at(self.base[k][-1], self.last)

    def put_own(self, bufs, value):
        for k in range(COLORS):
            bufs[k][self.own(k), :] = value[:, self.starts[k] : self.starts[k] + self.widths[k]]

    def get_own(self, bufs):
        return jnp.concatenate([bufs[k][self.own(k), :] for k in range(COLORS)], axis=1)

    def send(self, src, dst, sems, index, peer):
        return pltpu.make_async_remote_copy(
            src_ref=src, dst_ref=dst, send_sem=sems[0].at[index], recv_sem=sems[1].at[index], device_id=(peer, self.c), device_id_type=MESH
        )

    def flip(self, k, steps):
        return sum((1 - 2 * self.bit[k][s]) * (self.rows >> (s + 1)) for s in steps)

    def start(self, copies):
        for copy in copies:
            copy.start()

    def finish(self, copies):
        for copy in copies:
            copy.wait()

    def rs_parts(self, k, s):
        base, off, ln = self.base[k], self.rows - (self.rows >> s), self.rows >> (s + 1)
        if s == self.walk:
            first = self.rows - (self.rows >> s)
            return [(base[-1] + self.flip(k, self.group(q + 1)), base[-1], first + q * self.last, self.last) for q in range(self.peers)]
        away = base[s + 1] + self.flip(k, [s])
        if s == self.walk - 1:
            return [(away, base[s + 1], off, ln)]
        half = ln // 2
        b = self.bit[k][s + 1]
        return [(away + x * half, base[s + 1] + x * half, off + i * half, half) for i, x in enumerate((1 - b, b))]

    def rs_copies(self, bufs, recvs, sems, k, s, which=slice(None)):
        out = []
        for i, (src, _, dst, ln) in list(enumerate(self.rs_parts(k, s)))[which]:
            peer = self.toggled(k, self.group(i + 1) if s == self.walk else [s])
            at = 2 * s + i
            out.append(self.send(bufs[k].at[self.rows_at(src, ln)], recvs[k].at[pl.ds(dst, ln)], sems, (k, at), peer))
        return out

    def rs_take(self, bufs, recvs, sems, k, s, which):
        parts = self.rs_parts(k, s)[which]
        self.finish(self.rs_copies(bufs, recvs, sems, k, s, which))
        at = self.rows_at(parts[0][1], parts[0][3])
        got = sum(recvs[k][pl.ds(dst, ln), :].astype(F32) for _, _, dst, ln in parts)
        bufs[k][at, :] = (bufs[k][at, :].astype(F32) + got).astype(bufs[k].dtype)

    def reduce_scatter(self, bufs, recvs, sems, fill=None):
        for k in range(COLORS):
            self.start(self.rs_copies(bufs, recvs, sems, k, 0))
        for s in range(self.walk + 1):
            if fill is not None:
                fill(s)
            for k in range(COLORS):
                if 0 < s < self.walk:
                    self.rs_take(bufs, recvs, sems, k, s - 1, slice(1, 2))
                if s < self.walk:
                    self.rs_take(bufs, recvs, sems, k, s, slice(0, 1))
                    self.start(self.rs_copies(bufs, recvs, sems, k, s + 1))
                else:
                    self.rs_take(bufs, recvs, sems, k, s, slice(None))

    def blocks(self, s):
        later = range(s + 1, self.walk)
        return [st for n in range(len(later) + 1) for st in itertools.combinations(later, n)]

    def ag_block(self, bufs, sems, k, s, block):
        at = self.base[k][self.walk] + self.flip(k, block)
        ref = bufs[k].at[self.rows_at(at, self.rows >> self.walk)]
        index = 2 ** (self.walk - 1 - s) - 1 + self.blocks(s).index(block)
        return self.send(ref, ref, sems, (k, self.peers + index), self.toggled(k, [s]))

    def ag_direct(self, bufs, sems, k):
        ref = bufs[k].at[self.own(k)]
        return [self.send(ref, ref, sems, (k, q), self.toggled(k, self.group(q + 1))) for q in range(self.peers)]

    def ag_start(self, bufs, sems):
        for k in range(COLORS):
            self.start(self.ag_direct(bufs, sems, k))
        return self.walk

    def ag_next(self, bufs, sems, s):
        if s == self.walk:
            for k in range(COLORS):
                self.finish(self.ag_direct(bufs, sems, k))
                for to in range(s - 1, -1, -1):
                    self.ag_block(bufs, sems, k, to, ()).start()
            return s - 1
        for block in self.blocks(s):
            for k in range(COLORS):
                self.ag_block(bufs, sems, k, s, block).wait()
                for to in range(s - 1, -1, -1):
                    self.ag_block(bufs, sems, k, to, tuple(sorted(block + (s,)))).start()
        return s - 1

    def all_gather(self, bufs, sems, fill=None):
        s = self.ag_start(bufs, sems)
        while s >= 0:
            if fill is not None:
                fill(s)
            s = self.ag_next(bufs, sems, s)

    def pair(self, src, dst):
        i = next(self.free)
        return pltpu.make_async_remote_copy(
            src_ref=src, dst_ref=dst, send_sem=self.psend.at[i], recv_sem=self.precv.at[i], device_id=(self.m, 1 - self.c), device_id_type=MESH
        )

    def groups(self, *dtypes):
        return [pltpu.VMEM((self.rows, w), dtype) for dtype in dtypes for w in self.widths]

    def sems(self, n):
        return [pltpu.SemaphoreType.DMA((COLORS, self.peers + max(2 * self.walk, 2**self.walk)))] * (2 * n)


def by(n, items):
    return [items[i : i + n] for i in range(0, len(items), n)]


def embed_kernel(cube, vb, ids, e_ref, wg, wu, wd, g1, g2, hn, ep_o, wgh_o, wuh_o, h_own, gt_own, u_own, x_own, *scratch):
    e_s, wd_s, ep, wgh, wuh, xnat, x32, mp, mr, psend, precv, lsem, *rest = scratch
    xb, xr, hb = by(COLORS, rest[: 3 * COLORS])
    rs_sems, hg_sems = by(2, rest[3 * COLORS :])
    cube.bind(psend, precv)
    cube.arrive()
    local = Local(lsem)
    c = cube.c
    d = hn.shape[1]
    half_d, half_f = d // 2, wgh.shape[1]
    last = cube.last
    mine_d = span(c, half_d)
    e_local = local(e_ref, e_s)
    e_local.start()
    w_local = [local(wd, wd_s), local(wg.at[:, span(c, half_f)], wgh.at[mine_d]), local(wu.at[:, span(c, half_f)], wuh.at[mine_d])]
    e_local.wait()
    real = e_s.shape[0]
    body = real - real % 16
    if body > 0:
        ep[pl.ds(0, body), :] = e_s[pl.ds(0, body), :]
    if vb > body:
        ep[pl.ds(body, vb - body), :] = jnp.zeros((vb - body, d), BF16)
        ep[pl.ds(body, real - body), :] = e_s[pl.ds(body, real - body), :]
    cube.meet()
    e_pair = cube.pair(ep.at[pl.ds(0, vb)], ep.at[pl.ds(vb, vb)])
    e_pair.start()
    w_pair = [cube.pair(src.at[:, span(1 - c, half_f)], dst.at[mine_d]) for src, dst in ((wg, wgh), (wu, wuh))]
    cube.start(w_pair + w_local)
    chunk = min(512, cube.rows)

    def lookup(i):
        at = span(i, chunk)
        xnat[at, :] = tn(one_hot(vb, table_rows(cube, real, vb, ids[:, at])), ep[pl.ds(0, vb), :]).astype(BF16)

    def lookup_other(i):
        at = span(i, chunk)
        found = tn(one_hot(vb, table_rows(cube, real, vb, ids[:, at]) - vb), ep[pl.ds(vb, vb), :])
        xnat[at, :] = (xnat[at, :].astype(F32) + found).astype(BF16)

    loop(0, cube.rows // chunk, lookup)
    e_pair.wait()
    outs = [local(ep, ep_o), local(wgh, wgh_o), local(wuh, wuh_o)]
    outs[0].start()
    loop(0, cube.rows // chunk, lookup_other)
    cube.spread(xnat, xb)
    cube.reduce_scatter(xb, xr, rs_sems)
    x_own[...] = cube.get_own(xb)
    x32[0] = x_own[...]
    x_pair = cube.pair(x32.at[0], x32.at[1])
    x_pair.start()
    cube.finish(w_local + w_pair)
    cube.start(outs[1:])
    x_pair.wait()
    a_rows = rms_scale(x32[...].reshape(2 * last, d).astype(F32), g1[...]).astype(BF16)
    parts = 4
    fc = half_f // parts
    total = jnp.zeros((2 * last, d), F32)
    for p in range(parts):
        at = pl.ds(p * fc, fc)
        gate = nn(a_rows, wgh[:, at]).astype(BF16)
        up = nn(a_rows, wuh[:, at]).astype(BF16)
        gt_own[:, at] = gate
        u_own[:, at] = up
        gate_f = gate.astype(F32)
        act = (gate_f * jax.nn.sigmoid(gate_f) * up.astype(F32)).astype(BF16)
        total = total + nn(act, wd_s[at, :])
    mp[...] = total.reshape(2, last, d)
    m_pair = cube.pair(mp.at[1], mr)
    m_pair.start()
    m_pair.wait()
    h_rows = x_own[...].astype(F32) + (mp[0] + mr[...]).astype(BF16).astype(F32)
    h_own[...] = h_rows
    cube.put_own(hb, rms_scale(h_rows, g2[...]).astype(BF16))
    cube.all_gather(hb, hg_sems)
    cube.collect(hb, hn)
    cube.finish(outs)


def head_kernel(
    cube, vb, real, num_tokens, hn_i, ep_i, labels, h_own, g2, x_own, g1, gt_own, u_own, wgh_i, wuh_i, wd_i,
    dm_nat, loss, deh_o, dx_own, at_o, gt_o, u_o, *scratch
):
    hn, ep, z, dz, nat, stats, lbuf, dm32, mp, mr, wgh, wuh, wd, xf, tstage, stage, psend, precv, lsem, osem, st_s, st_r, *rest = scratch
    rb, rr, gb, xg = by(COLORS, rest[: 4 * COLORS])
    rs_sems, ag_sems, xg_sems = by(2, rest[4 * COLORS :])
    cube.bind(psend, precv)
    cube.arrive(rings=True)
    local = Local(lsem)
    c = cube.c
    t, d = hn.shape
    walk, last = cube.walk, cube.last
    first = [local(ep_i, ep), local(hn_i, hn)]
    cube.start(first)
    w_copies = [local(wgh_i, wgh), local(wuh_i, wuh), local(wd_i, wd)]
    cube.start(w_copies)
    cube.put_own(xg, x_own[...])
    chunk = min(256, t)
    chunks = t // chunk
    mine = cube.digits[0]

    def logits(i):
        at = span(i, chunk)
        row = lax.broadcasted_iota(jnp.int32, (2 * vb, chunk), 0)
        valid = (row < real) | ((row >= vb) & (row < vb + real))
        zz = jnp.where(valid, nt(ep[...], hn[at, :]), -1e38)
        z[:, at] = zz
        top = jnp.max(zz, axis=0, keepdims=True)
        parts = {TOP: top, SUM: jnp.exp(zz - top), LABEL: jnp.where(row == table_rows(cube, real, vb, labels[:, at]), zz, 0.0)}
        for r, v in parts.items():
            stats[0, mine, pl.ds(r, 1), at] = v if r == TOP else jnp.sum(v, axis=0, keepdims=True)

    cube.finish(first)
    loop(0, chunks // 2, logits)
    cube.meet()
    xstep = cube.ag_start(xg, xg_sems)
    loop(chunks // 2, chunks, logits)
    xstep = cube.ag_next(xg, xg_sems, xstep)
    for a in range(cube.axes):
        here = stats.at[a, cube.digits[a]]
        copies = [cube.send(here, here, (st_s, st_r), (a, step - 1), cube.ring_peer(a, step)) for step in range(1, RING)]
        cube.start(copies)
        cube.finish(copies)
        if xstep > 1:
            xstep = cube.ag_next(xg, xg_sems, xstep)
        tops, sums, marks = [[stats[a, i, pl.ds(r, 1), :] for i in range(RING)] for r in range(LABEL + 1)]
        top = functools.reduce(jnp.maximum, tops)
        total = sum(v * jnp.exp(m - top) for m, v in zip(tops, sums))
        label = sum(marks)
        slot = cube.digits[a + 1] if a + 1 < cube.axes else 0
        for r, v in enumerate((top, total, label)):
            stats[a + 1, slot, pl.ds(r, 1), :] = v
    while xstep > 0:
        xstep = cube.ag_next(xg, xg_sems, xstep)
    tok_loss = jnp.sum(top + jnp.log(total) - label, axis=1, keepdims=True)
    lbuf[c] = jnp.broadcast_to(tok_loss, lbuf.shape[1:])
    l_pair = cube.pair(lbuf.at[c], lbuf.at[c])
    l_pair.start()
    final = stats.at[cube.axes, 0]
    deh = z.at[:, pl.ds(0, d)]
    deh_out = local(deh, deh_o)

    wide = min(512, t)

    def backward(i):
        at = span(i, wide)
        row = lax.broadcasted_iota(jnp.int32, (2 * vb, wide), 0)
        soft = jnp.exp(z[:, at] - final[pl.ds(TOP, 1), at]) / final[pl.ds(SUM, 1), at]
        dzz = (jnp.where(row == table_rows(cube, real, vb, labels[:, at]), soft - 1.0, soft) / num_tokens).astype(BF16)
        dz[:, at] = dzz
        nat[at, :] = tn(dzz, ep[...])

    loop(0, t // wide, backward)
    cube.spread(nat, rb)
    mine_t = span(c, t)
    xf_pair = cube.pair(xf.at[mine_t], xf.at[mine_t])
    d_pair = cube.pair(dm32.at[0], dm32.at[1])
    m_pair = cube.pair(mp.at[1], mr)
    t_out = local(tstage, at_o)
    fc = wgh.shape[1] // PARTS

    def out_copies(p):
        slot = lax.rem(p, 2)
        return [pltpu.make_async_copy(stage.at[slot, i], dst.at[p], osem.at[i, slot]) for i, dst in enumerate((gt_o, u_o))]

    def gate_up(p):
        @pl.when(p >= 2)
        def _():
            cube.finish(out_copies(p - 2))

        cols = span(p, fc)
        slot = stage.at[lax.rem(p, 2)]

        def body(i):
            at = span(i, t)
            for which, w in enumerate((wgh, wuh)):
                slot[which, at, :] = nn(xf[at, :], w[:, cols]).astype(BF16)

        loop(0, 2, body)
        cube.start(out_copies(p))

    def normalise(i):
        at = span(c * chunks + i, chunk)
        xf[at, :] = rms_scale(xf[at, :].astype(F32), g1[...]).astype(BF16)

    def transpose(half, i):
        at = span(half * chunks + i, chunk)
        tstage[:, at] = xf[at, :].astype(F32).T.astype(BF16)

    def head_grad(i):
        deh[span(i, vb), :] = nn(dz[span(i, vb), :], hn[...])

    todo = [0]

    def run(n):
        lo, hi = todo[0], min(todo[0] + n, PARTS)
        todo[0] = hi
        if lo < hi:
            loop(lo, hi, gate_up)

    def rs_fill(s):
        if s == 0:
            cube.ag_next(xg, xg_sems, xstep)
            cube.collect(xg, xf, c)
            loop(0, chunks, normalise)
            xf_pair.start()
            loop(0, 2, head_grad)
            deh_out.start()
            loop(0, chunks, functools.partial(transpose, c))
        elif s == 1:
            cube.finish(w_copies + [xf_pair])
            loop(0, chunks, functools.partial(transpose, 1 - c))
            t_out.start()
            run(2)
        else:
            run(2)

    cube.reduce_scatter(rb, rr, rs_sems, rs_fill)
    dh = rms_back(h_own[...], g2[...], cube.get_own(rb))
    dm = dh.astype(BF16)
    cube.put_own(gb, dm)
    dm32[0] = dm

    def token_back(lo, hi):
        w = wgh.shape[1] // RING
        part = jnp.zeros((2 * last, d), F32)
        for p in range(lo, hi):
            at = pl.ds(p * w, w)
            d_act = nt(dm32[...].reshape(2 * last, d), wd[at, :])
            gate = gt_own[:, at].astype(F32)
            sig = jax.nn.sigmoid(gate)
            d_gate = (d_act * u_own[:, at].astype(F32) * (sig * (1.0 + gate * (1.0 - sig)))).astype(BF16)
            d_up = (d_act * (gate * sig)).astype(BF16)
            part = part + (nt(d_gate, wgh[:, at]) + nt(d_up, wuh[:, at]))
        part = part.reshape(mp.shape)
        mp[...] = part if lo == 0 else mp[...] + part

    def ag_fill(s):
        if s == walk:
            d_pair.wait()
            token_back(0, 2)
        elif s == walk - 1:
            token_back(2, RING)
            m_pair.start()
        else:
            run(1)

    d_pair.start()
    cube.all_gather(gb, ag_sems, ag_fill)
    cube.collect(gb, dm_nat)
    run(PARTS)
    m_pair.wait()
    dx_own[...] = dh + rms_back(x_own[...].astype(F32), g1[...], mp[0] + mr[...])
    l_pair.wait()
    loss[0, 0] = jnp.max((lbuf[0] + lbuf[1]) / num_tokens)
    cube.finish([t_out, deh_out])
    for p in (PARTS - 2, PARTS - 1):
        cube.finish(out_copies(p))


def table_kernel(cube, vb, real, ids, dx_own, dm_i, wd_i, deh, at_i, gt_i, u_i, de, dmf_o, act_o, dg_o, du_o, got_g, got_u, *scratch):
    dmf, wd, nat, mix, de_r, aoth, fin, fout, part, psend, precv, lsem, isem, osem, gsend, grecv, *rest = scratch
    gb, ag_sems = rest[:COLORS], rest[COLORS:]
    cube.bind(psend, precv)
    cube.arrive()
    c = cube.c
    t = cube.rows
    fc = wd.shape[0] // PARTS
    half_d = aoth.shape[0]
    local = Local(lsem)
    mine_t = span(c, t)
    dm_copy, wd_copy, a_copy = local(dm_i, dmf.at[mine_t]), local(wd_i, wd), local(at_i.at[span(1 - c, half_d)], aoth)
    deh_copy, dm_out = local(deh, mix), local(dmf, dmf_o)
    dm_pair = cube.pair(dm_i, dmf.at[mine_t])

    def in_copies(p):
        slot = lax.rem(p, 2)
        return [pltpu.make_async_copy(src.at[p], fin.at[slot, i], isem.at[i, slot]) for i, src in enumerate((gt_i, u_i))]

    def out_copies(p):
        slot = lax.rem(p, 2)
        return [pltpu.make_async_copy(fout.at[slot, i], dst.at[p], osem.at[i, slot]) for i, dst in enumerate((act_o, dg_o, du_o))]

    def send_copies(p):
        slot = lax.rem(p, 2)
        return [
            pltpu.make_async_remote_copy(
                src_ref=part.at[slot, i], dst_ref=dst.at[p], send_sem=gsend.at[i, p], recv_sem=grecv.at[i, p], device_id=(cube.m, 1 - c), device_id_type=MESH
            )
            for i, dst in enumerate((got_g, got_u))
        ]

    def drain(p):
        cube.finish(out_copies(p))
        for copy in send_copies(p):
            copy.wait_send()

    cube.start([dm_copy, wd_copy] + in_copies(0) + [a_copy, deh_copy])
    cube.put_own(gb, dx_own[...])
    cube.meet()
    step = cube.ag_start(gb, ag_sems)
    dm_pair.start()
    cube.finish([dm_copy, wd_copy, a_copy])

    def chunk_work(p, first=False):
        @pl.when(p + 1 < PARTS)
        def _():
            cube.start(in_copies(p + 1))

        cube.finish(in_copies(p))

        @pl.when(p >= 2)
        def _():
            drain(p - 2)

        slot = lax.rem(p, 2)
        src, dst, res = fin.at[slot], fout.at[slot], part.at[slot]

        def body(half):
            at = span(half, t)
            d_act = nt(dmf[at, :], wd[span(p, fc), :])
            gate = src[0, at, :].astype(F32)
            up = src[1, at, :].astype(F32)
            sig = jax.nn.sigmoid(gate)
            silu = gate * sig
            outs = (silu * up, d_act * up * (sig * (1.0 + gate * (1.0 - sig))), d_act * silu)
            for which, v in enumerate(outs):
                dst[which, at, :] = v.astype(BF16)

        if first:
            body(c)
            dm_pair.wait()
            dm_out.start()
            body(1 - c)
        else:
            loop(0, 2, body)
        for which in range(2):
            res[which] = nn(aoth[...], dst[which + 1])
        cube.start(out_copies(p) + send_copies(p))

    chunk_work(0, True)
    step = cube.ag_next(gb, ag_sems, step)
    p = 1
    while p + 1 < PARTS:
        loop(p, p + 2, chunk_work)
        if step >= 0:
            step = cube.ag_next(gb, ag_sems, step)
        p += 2
    while step >= 0:
        step = cube.ag_next(gb, ag_sems, step)
    cube.collect(gb, nat)
    cube.finish([deh_copy, dm_out])
    chunk = min(256, t)

    def scatter(i):
        at = span(i, chunk)
        hot = one_hot(2 * vb, table_rows(cube, real, vb, ids[:, at]))
        val = nat[at, :]
        hi = val.astype(BF16)
        rest = val - hi.astype(F32)
        mid = rest.astype(BF16)
        low = (rest - mid.astype(F32)).astype(BF16)
        mix[...] = mix[...] + ((nn(hot, low) + nn(hot, mid)) + nn(hot, hi))

    loop(0, t // chunk, scatter)
    e_pair = cube.pair(mix.at[pl.ds(vb, vb)], de_r)
    e_pair.start()
    loop(PARTS - 1, PARTS, chunk_work)
    drain(PARTS - 2)
    drain(PARTS - 1)
    for p in range(PARTS):
        for copy in send_copies(p):
            copy.wait_recv()
    e_pair.wait()
    de[...] = mix[pl.ds(0, vb), :] + de_r[...]


def weight_kernel(loss, de, at_i, dg, du, act, dmf_i, got_g, got_u, loss_o, de_o, og, ou, od, *scratch):
    aown, dmf, ring, gring, ostage, dstage, de_s, de_t, lsem, rsem, gsem, osem, xsem = scratch
    c = lax.axis_index("fsdp")
    depth, fc = ring.shape[0], ring.shape[-1]
    parts, half_f = dg.shape[0], dg.shape[0] * fc
    local = Local(lsem)
    a_copy, dm_copy = local(at_i.at[span(c, aown.shape[0])], aown), local(dmf_i, dmf)
    de_in, de_out = local(de, de_s), local(de_t, de_o)

    def reads(p):
        slot = lax.rem(p, depth)
        grads = [pltpu.make_async_copy(src.at[p], ring.at[slot, i], rsem.at[i, slot]) for i, src in enumerate((dg, du, act))]
        return grads, [pltpu.make_async_copy(src.at[p], gring.at[slot, i], gsem.at[i, slot]) for i, src in enumerate((got_g, got_u))]

    def columns(half, p):
        return pl.ds(pl.multiple_of(half * half_f + p * fc, fc), fc)

    def passes(p):
        slot = lax.rem(p, depth)
        return [pltpu.make_async_copy(gring.at[slot, i], dst.at[:, columns(1 - c, p)], xsem.at[i, slot]) for i, dst in enumerate((og, ou))]

    def writes(p):
        slot = lax.rem(p, 2)
        out = [pltpu.make_async_copy(ostage.at[slot, i], dst.at[:, columns(c, p)], osem.at[i, slot]) for i, dst in enumerate((og, ou))]
        return out + [pltpu.make_async_copy(dstage.at[slot], od.at[span(p, fc)], osem.at[2, slot])]

    def each(copies, verb):
        for copy in copies:
            getattr(copy, verb)()

    def fetch(p):
        grads, got = reads(p)
        each(grads + got, "start")

    a_copy.start()
    fetch(0)
    a_copy.wait()
    dm_copy.start()
    fetch(1)
    loss_o[0, 0] = loss[0, 0]

    def body(p):
        slot, oslot = lax.rem(p, depth), lax.rem(p, 2)
        grads, got = reads(p)
        each(grads, "wait")
        each(got, "wait")
        each(passes(p), "start")

        @pl.when(p == 0)
        def _():
            for later in range(2, depth):
                fetch(later)
            de_in.start()

        @pl.when(p >= 2)
        def _():
            each(writes(p - 2), "wait")

        for i in range(2):
            ostage[oslot, i] = nn(aown[...], ring[slot, i])

        @pl.when(p == 0)
        def _():
            dm_copy.wait()

        dstage[oslot] = tn(ring[slot, 2], dmf[...])
        each(writes(p), "start")

        @pl.when(p >= 1)
        def _():
            each(passes(p - 1), "wait")

        @pl.when((p >= 1) & (p - 1 + depth < parts))
        def _():
            fetch(p - 1 + depth)

    loop(0, parts, body)
    de_in.wait()
    de_t[...] = de_s[pl.ds(0, de_t.shape[0]), :]
    de_out.start()
    each(passes(parts - 1) + writes(parts - 2) + writes(parts - 1), "wait")
    de_out.wait()


def solution(mesh):
    model, fsdp_size = mesh.shape["model"], mesh.shape["fsdp"]
    tok_spec = P("fsdp", None)
    row_spec = P(("model", "fsdp"), None)
    weight_spec = P("fsdp", None)
    vmem = pl.BlockSpec(memory_space=pltpu.VMEM)
    hbm = pl.BlockSpec(memory_space=pl.ANY)
    sds = jax.ShapeDtypeStruct
    dma = pltpu.SemaphoreType.DMA

    def params(cid):
        return pltpu.CompilerParams(collective_id=cid, has_side_effects=True, vmem_limit_bytes=VMEM_LIMIT)

    def device_step(tok_ids, tok_labels, table_shard, gate_shard, up_shard, down_shard, gain_in, gain_out):
        t = tok_ids.size
        num_tokens = t * fsdp_size
        real, d = table_shard.shape
        vb = -(-real // 16) * 16
        f = gate_shard.shape[1]
        half_f, half_d = f // 2, d // 2
        fc = half_f // PARTS
        cube = Cube(model, t, d)
        last = cube.last
        ids, labels = tok_ids.reshape(1, t), tok_labels.reshape(1, t)
        smem = pl.BlockSpec(memory_space=pltpu.SMEM)
        g1, g2 = gain_in.reshape(1, d), gain_out.reshape(1, d)
        act_own = sds((2 * last, half_f), BF16)
        w_half = sds((d, half_f), BF16)
        hn, ep, wgh, wuh, h_own, gt_own, u_own, x_own = pl.pallas_call(
            functools.partial(embed_kernel, cube, vb),
            out_shape=(sds((t, d), BF16), sds((2 * vb, d), BF16), w_half, w_half, sds((last, d), F32), act_own, act_own, sds((last, d), BF16)),
            in_specs=[vmem, hbm, hbm, hbm, hbm, vmem, vmem],
            out_specs=(vmem, hbm, hbm, hbm, vmem, vmem, vmem, vmem),
            scratch_shapes=[
                pltpu.VMEM((real, d), BF16),
                pltpu.VMEM((half_f, d), BF16),
                pltpu.VMEM((2 * vb, d), BF16),
                pltpu.VMEM((d, half_f), BF16),
                pltpu.VMEM((d, half_f), BF16),
                pltpu.VMEM((t, d), BF16),
                pltpu.VMEM((2, last, d), BF16),
                pltpu.VMEM((2, last, d), F32),
                pltpu.VMEM((last, d), F32),
                dma((8,)),
                dma((8,)),
                dma((8,)),
            ]
            + cube.groups(BF16, BF16, BF16)
            + cube.sems(2),
            compiler_params=params(0),
            name="embed",
        )(ids, table_shard, gate_shard, up_shard, down_shard, g1, g2)
        chunked = sds((PARTS, 2 * t, fc), BF16)
        dm, loss, deh, dx_own, a_t, gt, u = pl.pallas_call(
            functools.partial(head_kernel, cube, vb, real, num_tokens),
            out_shape=(sds((t, d), BF16), sds((1, 1), F32), sds((2 * vb, d), F32), sds((last, d), F32), sds((d, 2 * t), BF16), chunked, chunked),
            in_specs=[hbm] * 2 + [vmem] * 7 + [hbm] * 3,
            out_specs=(vmem, smem, hbm, vmem) + (hbm,) * 3,
            scratch_shapes=[
                pltpu.VMEM((t, d), BF16),
                pltpu.VMEM((2 * vb, d), BF16),
                pltpu.VMEM((2 * vb, max(t, d)), F32),
                pltpu.VMEM((2 * vb, t), BF16),
                pltpu.VMEM((t, d), F32),
                pltpu.VMEM((cube.axes + 1, RING, RING, t), F32),
                pltpu.VMEM((2, 8, 128), F32),
                pltpu.VMEM((2, last, d), BF16),
                pltpu.VMEM((2, last, d), F32),
                pltpu.VMEM((last, d), F32),
                pltpu.VMEM((d, half_f), BF16),
                pltpu.VMEM((d, half_f), BF16),
                pltpu.VMEM((half_f, d), BF16),
                pltpu.VMEM((2 * t, d), BF16),
                pltpu.VMEM((d, 2 * t), BF16),
                pltpu.VMEM((2, 2, 2 * t, fc), BF16),
                dma((8,)),
                dma((8,)),
                dma((8,)),
                dma((2, PARTS)),
                dma((cube.axes, RING)),
                dma((cube.axes, RING)),
            ]
            + cube.groups(F32, F32, BF16, BF16)
            + cube.sems(3),
            compiler_params=params(1),
            name="head",
        )(hn, ep, labels, h_own, g2, x_own, g1, gt_own, u_own, wgh, wuh, down_shard)
        got = sds((PARTS, half_d, fc), F32)
        de, dmf, act, d_gate, d_up, got_g, got_u = pl.pallas_call(
            functools.partial(table_kernel, cube, vb, real),
            out_shape=(sds((vb, d), F32), sds((2 * t, d), BF16), chunked, chunked, chunked, got, got),
            in_specs=[vmem] * 2 + [hbm] * 6,
            out_specs=(vmem,) + (hbm,) * 6,
            scratch_shapes=[
                pltpu.VMEM((2 * t, d), BF16),
                pltpu.VMEM((half_f, d), BF16),
                pltpu.VMEM((t, d), F32),
                pltpu.VMEM((2 * vb, d), F32),
                pltpu.VMEM((vb, d), F32),
                pltpu.VMEM((half_d, 2 * t), BF16),
                pltpu.VMEM((2, 2, 2 * t, fc), BF16),
                pltpu.VMEM((2, 3, 2 * t, fc), BF16),
                pltpu.VMEM((2, 2, half_d, fc), F32),
                dma((2,)),
                dma((2,)),
                dma((5,)),
                dma((2, PARTS)),
                dma((3, PARTS)),
                dma((2, PARTS)),
                dma((2, PARTS)),
            ]
            + cube.groups(F32)
            + cube.sems(1),
            compiler_params=params(2),
            name="table",
        )(ids, dx_own, dm, down_shard, deh, a_t, gt, u)
        depth = 4
        loss, de, grad_gate, grad_up, grad_down = pl.pallas_call(
            weight_kernel,
            out_shape=(sds((1, 1), F32), sds((real, d), F32), sds((half_d, f), F32), sds((half_d, f), F32), sds((half_f, d), F32)),
            in_specs=[smem] + [hbm] * 8,
            out_specs=(smem,) + (hbm,) * 4,
            scratch_shapes=[
                pltpu.VMEM((half_d, 2 * t), BF16),
                pltpu.VMEM((2 * t, d), BF16),
                pltpu.VMEM((depth, 3, 2 * t, fc), BF16),
                pltpu.VMEM((depth, 2, half_d, fc), F32),
                pltpu.VMEM((2, 2, half_d, fc), F32),
                pltpu.VMEM((2, fc, d), F32),
                pltpu.VMEM((vb, d), F32),
                pltpu.VMEM((real, d), F32),
                dma((4,)),
                dma((3, depth)),
                dma((2, depth)),
                dma((3, 2)),
                dma((2, depth)),
            ],
            compiler_params=pltpu.CompilerParams(vmem_limit_bytes=VMEM_LIMIT, has_side_effects=True),
            name="weights",
        )(loss, de, a_t, d_gate, d_up, act, dmf, got_g, got_u)
        return loss.reshape(()), de, grad_gate, grad_up, grad_down

    return jax.shard_map(device_step, mesh=mesh, in_specs=(tok_spec, tok_spec, row_spec, weight_spec, weight_spec, weight_spec, P(), P()), out_specs=(P(), row_spec, weight_spec, weight_spec, weight_spec), check_vma=False)
```

```python
import functools
import itertools

import jax
import jax.numpy as jnp
from jax import lax
from jax.experimental import pallas as pl
from jax.experimental.pallas import tpu as pltpu
from jax.sharding import PartitionSpec as P

EPS = 1e-6
MESH = pl.DeviceIdType.MESH
VMEM_LIMIT = 67043328
F32 = jnp.float32
BF16 = jnp.bfloat16
COLORS = 3
DIRECT = 3
PARTS = 8
RING = 4
TOP, SUM, LABEL = range(3)


def contract(a, b, dims):
    return lax.dot_general(a, b, (dims, ((), ())), preferred_element_type=F32)


def nn(a, b):
    return contract(a, b, ((1,), (0,)))


def nt(a, b):
    return contract(a, b, ((1,), (1,)))


def tn(a, b):
    return contract(a, b, ((0,), (0,)))


def span(i, n):
    return pl.ds(pl.multiple_of(i * n, n), n)


def loop(lo, hi, body):
    def step(i, carry):
        body(i)
        return carry

    lax.fori_loop(lo, hi, step, 0)


def mean(v):
    return jnp.mean(v, axis=-1, keepdims=True)


def rms_scale(values, gain):
    return values * lax.rsqrt(mean(values * values) + EPS) * gain


def rms_back(values, gain, grad):
    r = lax.rsqrt(mean(values * values) + EPS)
    gg = grad * gain
    return r * gg - values * (r * r * r) * mean(values * gg)


def one_hot(rows, ids):
    return (lax.broadcasted_iota(jnp.int32, (rows, ids.shape[-1]), 0) == ids).astype(F32).astype(BF16)


def table_rows(cube, real, vb, ids):
    here = ids - (2 * cube.m + cube.c) * real
    there = ids - (2 * cube.m + 1 - cube.c) * real
    return jnp.where((here >= 0) & (here < real), here, jnp.where((there >= 0) & (there < real), vb + there, -1))


class Local:
    def __init__(self, sems):
        self.sems, self.free = sems, itertools.count()

    def __call__(self, src, dst):
        return pltpu.make_async_copy(src, dst, self.sems.at[next(self.free)])


class Cube:
    def __init__(self, model, rows, width):
        axes = 1
        while RING**axes < model:
            axes += 1
        self.axes, self.nb, self.rows = axes, 2 * axes, rows
        self.direct = min(DIRECT, self.nb - 1)
        self.walk = self.nb - self.direct
        self.peers = 2**self.direct - 1
        self.last = rows >> self.nb
        tiles = width // 128
        big = -(-tiles // COLORS) * 128
        self.widths = [big, big, width - 2 * big]
        self.starts = [0, big, 2 * big]

    def dim(self, k, s):
        d = (k + s) % self.nb
        return d % self.axes, d // self.axes

    def bind(self, psend=None, precv=None):
        self.m = lax.axis_index("model")
        self.c = lax.axis_index("fsdp")
        self.psend, self.precv, self.free = psend, precv, itertools.count()
        self.digits = [(self.m // RING**a) % RING for a in range(self.axes)]
        self.bit, self.base = [], []
        for k in range(COLORS):
            bits, bases = [], [0]
            for s in range(self.nb):
                a, kind = self.dim(k, s)
                b = self.digits[a]
                v0, v1 = (b % 2 + b // 2) % 2, b // 2
                bits.append(v0 + ((kind + self.c) % 2) * (v1 - v0))
                bases.append(bases[-1] + bits[-1] * (self.rows >> len(bits)))
            self.bit.append(bits)
            self.base.append(bases)

    def toggled(self, k, steps):
        digits = list(self.digits)
        for s in steps:
            a, kind = self.dim(k, s)
            near = 1 - 2 * (digits[a] % 2)
            digits[a] = digits[a] + near + ((kind + self.c) % 2) * (RING - 1 - 2 * digits[a] - near)
        return sum(v * RING**a for a, v in enumerate(digits))

    def group(self, q):
        return [self.walk + i for i in range(self.direct) if (q >> i) % 2]

    def ring_peer(self, a, step):
        b = self.digits[a]
        return self.m + RING**a * ((b + step) % RING - b)

    def arrive(self, rings=False):
        peers = [(self.m, 1 - self.c)]
        for k in range(COLORS):
            steps = [[s] for s in range(self.walk)] + [self.group(q + 1) for q in range(self.peers)]
            peers += [(self.toggled(k, st), self.c) for st in steps]
        if rings:
            peers += [(self.ring_peer(a, step), self.c) for a in range(self.axes) for step in range(1, RING)]
        for peer in peers:
            pl.semaphore_signal(pltpu.get_barrier_semaphore(), inc=1, device_id=peer, device_id_type=MESH)
        self.expected = len(peers)

    def meet(self):
        pl.semaphore_wait(pltpu.get_barrier_semaphore(), self.expected)

    def place(self, k, j):
        pos = []
        for c in range(2):
            p = 0
            for s in range(self.nb):
                a, kind = self.dim(k, s)
                p = 2 * p + (j >> (a + self.axes * ((kind + c) % 2))) % 2
            pos.append(p * self.last)
        return self.rows_at(pos[0] + self.c * (pos[1] - pos[0]), self.last)

    def rows_at(self, start, size):
        return pl.ds(pl.multiple_of(start, self.last), size)

    def cols(self, k):
        return pl.ds(self.starts[k], self.widths[k])

    def pieces(self):
        return itertools.product(range(2**self.nb), range(COLORS))

    def spread(self, nat, bufs):
        for j, k in self.pieces():
            bufs[k][self.place(k, j), :] = nat[span(j, self.last), self.cols(k)]

    def collect(self, bufs, nat, half=None):
        start = 0 if half is None else half * self.rows
        for j, k in self.pieces():
            nat[self.rows_at(start + j * self.last, self.last), self.cols(k)] = bufs[k][self.place(k, j), :]

    def own(self, k):
        return self.rows_at(self.base[k][-1], self.last)

    def put_own(self, bufs, value):
        for k in range(COLORS):
            bufs[k][self.own(k), :] = value[:, self.starts[k] : self.starts[k] + self.widths[k]]

    def get_own(self, bufs):
        return jnp.concatenate([bufs[k][self.own(k), :] for k in range(COLORS)], axis=1)

    def send(self, src, dst, sems, index, peer):
        return pltpu.make_async_remote_copy(
            src_ref=src, dst_ref=dst, send_sem=sems[0].at[index], recv_sem=sems[1].at[index], device_id=(peer, self.c), device_id_type=MESH
        )

    def flip(self, k, steps):
        return sum((1 - 2 * self.bit[k][s]) * (self.rows >> (s + 1)) for s in steps)

    def start(self, copies):
        for copy in copies:
            copy.start()

    def finish(self, copies):
        for copy in copies:
            copy.wait()

    def rs_parts(self, k, s):
        base, off, ln = self.base[k], self.rows - (self.rows >> s), self.rows >> (s + 1)
        if s == self.walk:
            first = self.rows - (self.rows >> s)
            return [(base[-1] + self.flip(k, self.group(q + 1)), base[-1], first + q * self.last, self.last) for q in range(self.peers)]
        away = base[s + 1] + self.flip(k, [s])
        if s == self.walk - 1:
            return [(away, base[s + 1], off, ln)]
        half = ln // 2
        b = self.bit[k][s + 1]
        return [(away + x * half, base[s + 1] + x * half, off + i * half, half) for i, x in enumerate((1 - b, b))]

    def rs_copies(self, bufs, recvs, sems, k, s, which=slice(None)):
        out = []
        for i, (src, _, dst, ln) in list(enumerate(self.rs_parts(k, s)))[which]:
            peer = self.toggled(k, self.group(i + 1) if s == self.walk else [s])
            at = 2 * s + i
            out.append(self.send(bufs[k].at[self.rows_at(src, ln)], recvs[k].at[pl.ds(dst, ln)], sems, (k, at), peer))
        return out

    def rs_take(self, bufs, recvs, sems, k, s, which):
        parts = self.rs_parts(k, s)[which]
        self.finish(self.rs_copies(bufs, recvs, sems, k, s, which))
        at = self.rows_at(parts[0][1], parts[0][3])
        got = sum(recvs[k][pl.ds(dst, ln), :].astype(F32) for _, _, dst, ln in parts)
        bufs[k][at, :] = (bufs[k][at, :].astype(F32) + got).astype(bufs[k].dtype)

    def reduce_scatter(self, bufs, recvs, sems, fill=None):
        for k in range(COLORS):
            self.start(self.rs_copies(bufs, recvs, sems, k, 0))
        for s in range(self.walk + 1):
            if fill is not None:
                fill(s)
            for k in range(COLORS):
                if 0 < s < self.walk:
                    self.rs_take(bufs, recvs, sems, k, s - 1, slice(1, 2))
                if s < self.walk:
                    self.rs_take(bufs, recvs, sems, k, s, slice(0, 1))
                    self.start(self.rs_copies(bufs, recvs, sems, k, s + 1))
                else:
                    self.rs_take(bufs, recvs, sems, k, s, slice(None))

    def blocks(self, s):
        later = range(s + 1, self.walk)
        return [st for n in range(len(later) + 1) for st in itertools.combinations(later, n)]

    def ag_block(self, bufs, sems, k, s, block):
        at = self.base[k][self.walk] + self.flip(k, block)
        ref = bufs[k].at[self.rows_at(at, self.rows >> self.walk)]
        index = 2 ** (self.walk - 1 - s) - 1 + self.blocks(s).index(block)
        return self.send(ref, ref, sems, (k, self.peers + index), self.toggled(k, [s]))

    def ag_direct(self, bufs, sems, k):
        ref = bufs[k].at[self.own(k)]
        return [self.send(ref, ref, sems, (k, q), self.toggled(k, self.group(q + 1))) for q in range(self.peers)]

    def ag_start(self, bufs, sems):
        for k in range(COLORS):
            self.start(self.ag_direct(bufs, sems, k))
        return self.walk

    def ag_next(self, bufs, sems, s):
        if s == self.walk:
            for k in range(COLORS):
                self.finish(self.ag_direct(bufs, sems, k))
                for to in range(s - 1, -1, -1):
                    self.ag_block(bufs, sems, k, to, ()).start()
            return s - 1
        for block in self.blocks(s):
            for k in range(COLORS):
                self.ag_block(bufs, sems, k, s, block).wait()
                for to in range(s - 1, -1, -1):
                    self.ag_block(bufs, sems, k, to, tuple(sorted(block + (s,)))).start()
        return s - 1

    def all_gather(self, bufs, sems, fill=None):
        s = self.ag_start(bufs, sems)
        while s >= 0:
            if fill is not None:
                fill(s)
            s = self.ag_next(bufs, sems, s)

    def pair(self, src, dst):
        i = next(self.free)
        return pltpu.make_async_remote_copy(
            src_ref=src, dst_ref=dst, send_sem=self.psend.at[i], recv_sem=self.precv.at[i], device_id=(self.m, 1 - self.c), device_id_type=MESH
        )

    def groups(self, *dtypes):
        return [pltpu.VMEM((self.rows, w), dtype) for dtype in dtypes for w in self.widths]

    def sems(self, n):
        return [pltpu.SemaphoreType.DMA((COLORS, self.peers + max(2 * self.walk, 2**self.walk)))] * (2 * n)


def by(n, items):
    return [items[i : i + n] for i in range(0, len(items), n)]


def embed_kernel(cube, vb, ids, e_ref, wg, wu, wd, g1, g2, hn, ep_o, wgh_o, wuh_o, h_own, gt_own, u_own, x_own, *scratch):
    e_s, wd_s, ep, wgh, wuh, xnat, x32, mp, mr, psend, precv, lsem, *rest = scratch
    xb, xr, hb = by(COLORS, rest[: 3 * COLORS])
    rs_sems, hg_sems = by(2, rest[3 * COLORS :])
    cube.bind(psend, precv)
    cube.arrive()
    local = Local(lsem)
    c = cube.c
    d = hn.shape[1]
    half_d, half_f = d // 2, wgh.shape[1]
    last = cube.last
    mine_d = span(c, half_d)
    e_local = local(e_ref, e_s)
    e_local.start()
    w_local = [local(wd, wd_s), local(wg.at[:, span(c, half_f)], wgh.at[mine_d]), local(wu.at[:, span(c, half_f)], wuh.at[mine_d])]
    e_local.wait()
    real = e_s.shape[0]
    body = real - real % 16
    if body > 0:
        ep[pl.ds(0, body), :] = e_s[pl.ds(0, body), :]
    if vb > body:
        ep[pl.ds(body, vb - body), :] = jnp.zeros((vb - body, d), BF16)
        ep[pl.ds(body, real - body), :] = e_s[pl.ds(body, real - body), :]
    cube.meet()
    e_pair = cube.pair(ep.at[pl.ds(0, vb)], ep.at[pl.ds(vb, vb)])
    e_pair.start()
    w_pair = [cube.pair(src.at[:, span(1 - c, half_f)], dst.at[mine_d]) for src, dst in ((wg, wgh), (wu, wuh))]
    cube.start(w_pair + w_local)
    chunk = min(512, cube.rows)

    def lookup(i):
        at = span(i, chunk)
        xnat[at, :] = tn(one_hot(vb, table_rows(cube, real, vb, ids[:, at])), ep[pl.ds(0, vb), :]).astype(BF16)

    def lookup_other(i):
        at = span(i, chunk)
        found = tn(one_hot(vb, table_rows(cube, real, vb, ids[:, at]) - vb), ep[pl.ds(vb, vb), :])
        xnat[at, :] = (xnat[at, :].astype(F32) + found).astype(BF16)

    loop(0, cube.rows // chunk, lookup)
    e_pair.wait()
    outs = [local(ep, ep_o), local(wgh, wgh_o), local(wuh, wuh_o)]
    outs[0].start()
    loop(0, cube.rows // chunk, lookup_other)
    cube.spread(xnat, xb)
    cube.reduce_scatter(xb, xr, rs_sems)
    x_own[...] = cube.get_own(xb)
    x32[0] = x_own[...]
    x_pair = cube.pair(x32.at[0], x32.at[1])
    x_pair.start()
    cube.finish(w_local + w_pair)
    cube.start(outs[1:])
    x_pair.wait()
    a_rows = rms_scale(x32[...].reshape(2 * last, d).astype(F32), g1[...]).astype(BF16)
    parts = 4
    fc = half_f // parts
    total = jnp.zeros((2 * last, d), F32)
    for p in range(parts):
        at = pl.ds(p * fc, fc)
        gate = nn(a_rows, wgh[:, at]).astype(BF16)
        up = nn(a_rows, wuh[:, at]).astype(BF16)
        gt_own[:, at] = gate
        u_own[:, at] = up
        gate_f = gate.astype(F32)
        act = (gate_f * jax.nn.sigmoid(gate_f) * up.astype(F32)).astype(BF16)
        total = total + nn(act, wd_s[at, :])
    mp[...] = total.reshape(2, last, d)
    m_pair = cube.pair(mp.at[1], mr)
    m_pair.start()
    m_pair.wait()
    h_rows = x_own[...].astype(F32) + (mp[0] + mr[...]).astype(BF16).astype(F32)
    h_own[...] = h_rows
    cube.put_own(hb, rms_scale(h_rows, g2[...]).astype(BF16))
    cube.all_gather(hb, hg_sems)
    cube.collect(hb, hn)
    cube.finish(outs)


def head_kernel(
    cube, vb, real, num_tokens, hn_i, ep_i, labels, h_own, g2, x_own, g1, gt_own, u_own, wgh_i, wuh_i, wd_i,
    dm_nat, loss, deh_o, dx_own, at_o, gt_o, u_o, *scratch
):
    hn, ep, z, dz, nat, stats, lbuf, dm32, mp, mr, wgh, wuh, wd, xf, tstage, stage, psend, precv, lsem, osem, st_s, st_r, *rest = scratch
    rb, rr, gb, xg = by(COLORS, rest[: 4 * COLORS])
    rs_sems, ag_sems, xg_sems = by(2, rest[4 * COLORS :])
    cube.bind(psend, precv)
    cube.arrive(rings=True)
    local = Local(lsem)
    c = cube.c
    t, d = hn.shape
    walk, last = cube.walk, cube.last
    first = [local(ep_i, ep), local(hn_i, hn)]
    cube.start(first)
    w_copies = [local(wgh_i, wgh), local(wuh_i, wuh), local(wd_i, wd)]
    cube.start(w_copies)
    cube.put_own(xg, x_own[...])
    chunk = min(256, t)
    chunks = t // chunk
    mine = cube.digits[0]

    def logits(i):
        at = span(i, chunk)
        row = lax.broadcasted_iota(jnp.int32, (2 * vb, chunk), 0)
        valid = (row < real) | ((row >= vb) & (row < vb + real))
        zz = jnp.where(valid, nt(ep[...], hn[at, :]), -1e38)
        z[:, at] = zz
        top = jnp.max(zz, axis=0, keepdims=True)
        parts = {TOP: top, SUM: jnp.exp(zz - top), LABEL: jnp.where(row == table_rows(cube, real, vb, labels[:, at]), zz, 0.0)}
        for r, v in parts.items():
            stats[0, mine, pl.ds(r, 1), at] = v if r == TOP else jnp.sum(v, axis=0, keepdims=True)

    cube.finish(first)
    loop(0, chunks // 2, logits)
    cube.meet()
    xstep = cube.ag_start(xg, xg_sems)
    loop(chunks // 2, chunks, logits)
    xstep = cube.ag_next(xg, xg_sems, xstep)
    for a in range(cube.axes):
        here = stats.at[a, cube.digits[a]]
        copies = [cube.send(here, here, (st_s, st_r), (a, step - 1), cube.ring_peer(a, step)) for step in range(1, RING)]
        cube.start(copies)
        cube.finish(copies)
        if xstep > 1:
            xstep = cube.ag_next(xg, xg_sems, xstep)
        tops, sums, marks = [[stats[a, i, pl.ds(r, 1), :] for i in range(RING)] for r in range(LABEL + 1)]
        top = functools.reduce(jnp.maximum, tops)
        total = sum(v * jnp.exp(m - top) for m, v in zip(tops, sums))
        label = sum(marks)
        slot = cube.digits[a + 1] if a + 1 < cube.axes else 0
        for r, v in enumerate((top, total, label)):
            stats[a + 1, slot, pl.ds(r, 1), :] = v
    while xstep > 0:
        xstep = cube.ag_next(xg, xg_sems, xstep)
    tok_loss = jnp.sum(top + jnp.log(total) - label, axis=1, keepdims=True)
    lbuf[c] = jnp.broadcast_to(tok_loss, lbuf.shape[1:])
    l_pair = cube.pair(lbuf.at[c], lbuf.at[c])
    l_pair.start()
    final = stats.at[cube.axes, 0]
    deh = z.at[:, pl.ds(0, d)]
    deh_out = local(deh, deh_o)

    wide = min(512, t)

    def backward(i):
        at = span(i, wide)
        row = lax.broadcasted_iota(jnp.int32, (2 * vb, wide), 0)
        soft = jnp.exp(z[:, at] - final[pl.ds(TOP, 1), at]) / final[pl.ds(SUM, 1), at]
        dzz = (jnp.where(row == table_rows(cube, real, vb, labels[:, at]), soft - 1.0, soft) / num_tokens).astype(BF16)
        dz[:, at] = dzz
        nat[at, :] = tn(dzz, ep[...])

    loop(0, t // wide, backward)
    cube.spread(nat, rb)
    mine_t = span(c, t)
    xf_pair = cube.pair(xf.at[mine_t], xf.at[mine_t])
    d_pair = cube.pair(dm32.at[0], dm32.at[1])
    m_pair = cube.pair(mp.at[1], mr)
    t_out = local(tstage, at_o)
    fc = wgh.shape[1] // PARTS

    def out_copies(p):
        slot = lax.rem(p, 2)
        return [pltpu.make_async_copy(stage.at[slot, i], dst.at[p], osem.at[i, slot]) for i, dst in enumerate((gt_o, u_o))]

    def gate_up(p):
        @pl.when(p >= 2)
        def _():
            cube.finish(out_copies(p - 2))

        cols = span(p, fc)
        slot = stage.at[lax.rem(p, 2)]

        def body(i):
            at = span(i, t)
            for which, w in enumerate((wgh, wuh)):
                slot[which, at, :] = nn(xf[at, :], w[:, cols]).astype(BF16)

        loop(0, 2, body)
        cube.start(out_copies(p))

    def normalise(i):
        at = span(c * chunks + i, chunk)
        xf[at, :] = rms_scale(xf[at, :].astype(F32), g1[...]).astype(BF16)

    def transpose(half, i):
        at = span(half * chunks + i, chunk)
        tstage[:, at] = xf[at, :].astype(F32).T.astype(BF16)

    def head_grad(i):
        deh[span(i, vb), :] = nn(dz[span(i, vb), :], hn[...])

    todo = [0]

    def run(n):
        lo, hi = todo[0], min(todo[0] + n, PARTS)
        todo[0] = hi
        if lo < hi:
            loop(lo, hi, gate_up)

    def rs_fill(s):
        if s == 0:
            cube.ag_next(xg, xg_sems, xstep)
            cube.collect(xg, xf, c)
            loop(0, chunks, normalise)
            xf_pair.start()
            loop(0, 2, head_grad)
            deh_out.start()
            loop(0, chunks, functools.partial(transpose, c))
        elif s == 1:
            cube.finish(w_copies + [xf_pair])
            loop(0, chunks, functools.partial(transpose, 1 - c))
            t_out.start()
            run(2)
        else:
            run(2)

    cube.reduce_scatter(rb, rr, rs_sems, rs_fill)
    dh = rms_back(h_own[...], g2[...], cube.get_own(rb))
    dm = dh.astype(BF16)
    cube.put_own(gb, dm)
    dm32[0] = dm

    def token_back(lo, hi):
        w = wgh.shape[1] // RING
        part = jnp.zeros((2 * last, d), F32)
        for p in range(lo, hi):
            at = pl.ds(p * w, w)
            d_act = nt(dm32[...].reshape(2 * last, d), wd[at, :])
            gate = gt_own[:, at].astype(F32)
            sig = jax.nn.sigmoid(gate)
            d_gate = (d_act * u_own[:, at].astype(F32) * (sig * (1.0 + gate * (1.0 - sig)))).astype(BF16)
            d_up = (d_act * (gate * sig)).astype(BF16)
            part = part + (nt(d_gate, wgh[:, at]) + nt(d_up, wuh[:, at]))
        part = part.reshape(mp.shape)
        mp[...] = part if lo == 0 else mp[...] + part

    def ag_fill(s):
        if s == walk:
            d_pair.wait()
            token_back(0, 2)
        elif s == walk - 1:
            token_back(2, RING)
            m_pair.start()
        else:
            run(1)

    d_pair.start()
    cube.all_gather(gb, ag_sems, ag_fill)
    cube.collect(gb, dm_nat)
    run(PARTS)
    m_pair.wait()
    dx_own[...] = dh + rms_back(x_own[...].astype(F32), g1[...], mp[0] + mr[...])
    l_pair.wait()
    loss[0, 0] = jnp.max((lbuf[0] + lbuf[1]) / num_tokens)
    cube.finish([t_out, deh_out])
    for p in (PARTS - 2, PARTS - 1):
        cube.finish(out_copies(p))


def table_kernel(cube, vb, real, ids, dx_own, dm_i, wd_i, deh, at_i, gt_i, u_i, de, dmf_o, act_o, dg_o, du_o, got_g, got_u, *scratch):
    dmf, wd, nat, mix, de_r, aoth, fin, fout, part, psend, precv, lsem, isem, osem, gsend, grecv, *rest = scratch
    gb, ag_sems = rest[:COLORS], rest[COLORS:]
    cube.bind(psend, precv)
    cube.arrive()
    c = cube.c
    t = cube.rows
    fc = wd.shape[0] // PARTS
    half_d = aoth.shape[0]
    local = Local(lsem)
    mine_t = span(c, t)
    dm_copy, wd_copy, a_copy = local(dm_i, dmf.at[mine_t]), local(wd_i, wd), local(at_i.at[span(1 - c, half_d)], aoth)
    deh_copy, dm_out = local(deh, mix), local(dmf, dmf_o)
    dm_pair = cube.pair(dm_i, dmf.at[mine_t])

    def in_copies(p):
        slot = lax.rem(p, 2)
        return [pltpu.make_async_copy(src.at[p], fin.at[slot, i], isem.at[i, slot]) for i, src in enumerate((gt_i, u_i))]

    def out_copies(p):
        slot = lax.rem(p, 2)
        return [pltpu.make_async_copy(fout.at[slot, i], dst.at[p], osem.at[i, slot]) for i, dst in enumerate((act_o, dg_o, du_o))]

    def send_copies(p):
        slot = lax.rem(p, 2)
        return [
            pltpu.make_async_remote_copy(
                src_ref=part.at[slot, i], dst_ref=dst.at[p], send_sem=gsend.at[i, p], recv_sem=grecv.at[i, p], device_id=(cube.m, 1 - c), device_id_type=MESH
            )
            for i, dst in enumerate((got_g, got_u))
        ]

    def drain(p):
        cube.finish(out_copies(p))
        for copy in send_copies(p):
            copy.wait_send()

    cube.start([dm_copy, wd_copy] + in_copies(0) + [a_copy, deh_copy])
    cube.put_own(gb, dx_own[...])
    cube.meet()
    step = cube.ag_start(gb, ag_sems)
    dm_pair.start()
    cube.finish([dm_copy, wd_copy, a_copy])

    def chunk_work(p, first=False):
        @pl.when(p + 1 < PARTS)
        def _():
            cube.start(in_copies(p + 1))

        cube.finish(in_copies(p))

        @pl.when(p >= 2)
        def _():
            drain(p - 2)

        slot = lax.rem(p, 2)
        src, dst, res = fin.at[slot], fout.at[slot], part.at[slot]

        def body(half):
            at = span(half, t)
            d_act = nt(dmf[at, :], wd[span(p, fc), :])
            gate = src[0, at, :].astype(F32)
            up = src[1, at, :].astype(F32)
            sig = jax.nn.sigmoid(gate)
            silu = gate * sig
            outs = (silu * up, d_act * up * (sig * (1.0 + gate * (1.0 - sig))), d_act * silu)
            for which, v in enumerate(outs):
                dst[which, at, :] = v.astype(BF16)

        if first:
            body(c)
            dm_pair.wait()
            dm_out.start()
            body(1 - c)
        else:
            loop(0, 2, body)
        for which in range(2):
            res[which] = nn(aoth[...], dst[which + 1])
        cube.start(out_copies(p) + send_copies(p))

    chunk_work(0, True)
    step = cube.ag_next(gb, ag_sems, step)
    p = 1
    while p < PARTS:
        q = min(p + 2, PARTS)
        loop(p, q, chunk_work)
        if step >= 0:
            step = cube.ag_next(gb, ag_sems, step)
        p = q
    while step >= 0:
        step = cube.ag_next(gb, ag_sems, step)
    cube.collect(gb, nat)
    cube.finish([deh_copy, dm_out])
    chunk = min(256, t)

    def scatter(half, i):
        at = span(i, chunk)
        rows = pl.ds(half * vb, vb)
        hot = one_hot(vb, table_rows(cube, real, vb, ids[:, at]) - half * vb)
        val = nat[at, :]
        hi = val.astype(BF16)
        rest = val - hi.astype(F32)
        mid = rest.astype(BF16)
        low = (rest - mid.astype(F32)).astype(BF16)
        mix[rows, :] = mix[rows, :] + ((nn(hot, low) + nn(hot, mid)) + nn(hot, hi))

    loop(0, t // chunk, functools.partial(scatter, 1))
    e_pair = cube.pair(mix.at[pl.ds(vb, vb)], de_r)
    e_pair.start()
    loop(0, t // chunk, functools.partial(scatter, 0))
    drain(PARTS - 2)
    drain(PARTS - 1)
    for p in range(PARTS):
        for copy in send_copies(p):
            copy.wait_recv()
    e_pair.wait()
    de[...] = mix[pl.ds(0, vb), :] + de_r[...]


def weight_kernel(loss, de, at_i, dg, du, act, dmf_i, got_g, got_u, loss_o, de_o, og, ou, od, *scratch):
    aown, dmf, ring, gring, ostage, dstage, de_s, de_t, lsem, rsem, gsem, osem, xsem = scratch
    c = lax.axis_index("fsdp")
    depth, fc = ring.shape[0], ring.shape[-1]
    parts, half_f = dg.shape[0], dg.shape[0] * fc
    local = Local(lsem)
    a_copy, dm_copy = local(at_i.at[span(c, aown.shape[0])], aown), local(dmf_i, dmf)
    de_in, de_out = local(de, de_s), local(de_t, de_o)

    def reads(p):
        slot = lax.rem(p, depth)
        grads = [pltpu.make_async_copy(src.at[p], ring.at[slot, i], rsem.at[i, slot]) for i, src in enumerate((dg, du, act))]
        return grads, [pltpu.make_async_copy(src.at[p], gring.at[slot, i], gsem.at[i, slot]) for i, src in enumerate((got_g, got_u))]

    def columns(half, p):
        return pl.ds(pl.multiple_of(half * half_f + p * fc, fc), fc)

    def passes(p):
        slot = lax.rem(p, depth)
        return [pltpu.make_async_copy(gring.at[slot, i], dst.at[:, columns(1 - c, p)], xsem.at[i, slot]) for i, dst in enumerate((og, ou))]

    def writes(p):
        slot = lax.rem(p, 2)
        out = [pltpu.make_async_copy(ostage.at[slot, i], dst.at[:, columns(c, p)], osem.at[i, slot]) for i, dst in enumerate((og, ou))]
        return out + [pltpu.make_async_copy(dstage.at[slot], od.at[span(p, fc)], osem.at[2, slot])]

    def each(copies, verb):
        for copy in copies:
            getattr(copy, verb)()

    def fetch(p):
        grads, got = reads(p)
        each(grads + got, "start")

    a_copy.start()
    fetch(0)
    a_copy.wait()
    dm_copy.start()
    fetch(1)
    loss_o[0, 0] = loss[0, 0]

    def body(p):
        slot, oslot = lax.rem(p, depth), lax.rem(p, 2)
        grads, got = reads(p)
        each(grads, "wait")
        each(got, "wait")
        each(passes(p), "start")

        @pl.when(p == 0)
        def _():
            for later in range(2, depth):
                fetch(later)
            de_in.start()

        @pl.when(p >= 2)
        def _():
            each(writes(p - 2), "wait")

        for i in range(2):
            ostage[oslot, i] = nn(aown[...], ring[slot, i])

        @pl.when(p == 0)
        def _():
            dm_copy.wait()

        dstage[oslot] = tn(ring[slot, 2], dmf[...])
        each(writes(p), "start")

        @pl.when(p >= 1)
        def _():
            each(passes(p - 1), "wait")

        @pl.when((p >= 1) & (p - 1 + depth < parts))
        def _():
            fetch(p - 1 + depth)

    loop(0, parts, body)
    de_in.wait()
    de_t[...] = de_s[pl.ds(0, de_t.shape[0]), :]
    de_out.start()
    each(passes(parts - 1) + writes(parts - 2) + writes(parts - 1), "wait")
    de_out.wait()


def solution(mesh):
    model, fsdp_size = mesh.shape["model"], mesh.shape["fsdp"]
    tok_spec = P("fsdp", None)
    row_spec = P(("model", "fsdp"), None)
    weight_spec = P("fsdp", None)
    vmem = pl.BlockSpec(memory_space=pltpu.VMEM)
    hbm = pl.BlockSpec(memory_space=pl.ANY)
    sds = jax.ShapeDtypeStruct
    dma = pltpu.SemaphoreType.DMA

    def params(cid):
        return pltpu.CompilerParams(collective_id=cid, has_side_effects=True, vmem_limit_bytes=VMEM_LIMIT)

    def device_step(tok_ids, tok_labels, table_shard, gate_shard, up_shard, down_shard, gain_in, gain_out):
        t = tok_ids.size
        num_tokens = t * fsdp_size
        real, d = table_shard.shape
        vb = -(-real // 16) * 16
        f = gate_shard.shape[1]
        half_f, half_d = f // 2, d // 2
        fc = half_f // PARTS
        cube = Cube(model, t, d)
        last = cube.last
        ids, labels = tok_ids.reshape(1, t), tok_labels.reshape(1, t)
        smem = pl.BlockSpec(memory_space=pltpu.SMEM)
        g1, g2 = gain_in.reshape(1, d), gain_out.reshape(1, d)
        act_own = sds((2 * last, half_f), BF16)
        w_half = sds((d, half_f), BF16)
        hn, ep, wgh, wuh, h_own, gt_own, u_own, x_own = pl.pallas_call(
            functools.partial(embed_kernel, cube, vb),
            out_shape=(sds((t, d), BF16), sds((2 * vb, d), BF16), w_half, w_half, sds((last, d), F32), act_own, act_own, sds((last, d), BF16)),
            in_specs=[vmem, hbm, hbm, hbm, hbm, vmem, vmem],
            out_specs=(vmem, hbm, hbm, hbm, vmem, vmem, vmem, vmem),
            scratch_shapes=[
                pltpu.VMEM((real, d), BF16),
                pltpu.VMEM((half_f, d), BF16),
                pltpu.VMEM((2 * vb, d), BF16),
                pltpu.VMEM((d, half_f), BF16),
                pltpu.VMEM((d, half_f), BF16),
                pltpu.VMEM((t, d), BF16),
                pltpu.VMEM((2, last, d), BF16),
                pltpu.VMEM((2, last, d), F32),
                pltpu.VMEM((last, d), F32),
                dma((8,)),
                dma((8,)),
                dma((8,)),
            ]
            + cube.groups(BF16, BF16, BF16)
            + cube.sems(2),
            compiler_params=params(0),
            name="embed",
        )(ids, table_shard, gate_shard, up_shard, down_shard, g1, g2)
        chunked = sds((PARTS, 2 * t, fc), BF16)
        dm, loss, deh, dx_own, a_t, gt, u = pl.pallas_call(
            functools.partial(head_kernel, cube, vb, real, num_tokens),
            out_shape=(sds((t, d), BF16), sds((1, 1), F32), sds((2 * vb, d), F32), sds((last, d), F32), sds((d, 2 * t), BF16), chunked, chunked),
            in_specs=[hbm] * 2 + [vmem] * 7 + [hbm] * 3,
            out_specs=(vmem, smem, hbm, vmem) + (hbm,) * 3,
            scratch_shapes=[
                pltpu.VMEM((t, d), BF16),
                pltpu.VMEM((2 * vb, d), BF16),
                pltpu.VMEM((2 * vb, max(t, d)), F32),
                pltpu.VMEM((2 * vb, t), BF16),
                pltpu.VMEM((t, d), F32),
                pltpu.VMEM((cube.axes + 1, RING, RING, t), F32),
                pltpu.VMEM((2, 8, 128), F32),
                pltpu.VMEM((2, last, d), BF16),
                pltpu.VMEM((2, last, d), F32),
                pltpu.VMEM((last, d), F32),
                pltpu.VMEM((d, half_f), BF16),
                pltpu.VMEM((d, half_f), BF16),
                pltpu.VMEM((half_f, d), BF16),
                pltpu.VMEM((2 * t, d), BF16),
                pltpu.VMEM((d, 2 * t), BF16),
                pltpu.VMEM((2, 2, 2 * t, fc), BF16),
                dma((8,)),
                dma((8,)),
                dma((8,)),
                dma((2, PARTS)),
                dma((cube.axes, RING)),
                dma((cube.axes, RING)),
            ]
            + cube.groups(F32, F32, BF16, BF16)
            + cube.sems(3),
            compiler_params=params(1),
            name="head",
        )(hn, ep, labels, h_own, g2, x_own, g1, gt_own, u_own, wgh, wuh, down_shard)
        got = sds((PARTS, half_d, fc), F32)
        de, dmf, act, d_gate, d_up, got_g, got_u = pl.pallas_call(
            functools.partial(table_kernel, cube, vb, real),
            out_shape=(sds((vb, d), F32), sds((2 * t, d), BF16), chunked, chunked, chunked, got, got),
            in_specs=[vmem] * 2 + [hbm] * 6,
            out_specs=(vmem,) + (hbm,) * 6,
            scratch_shapes=[
                pltpu.VMEM((2 * t, d), BF16),
                pltpu.VMEM((half_f, d), BF16),
                pltpu.VMEM((t, d), F32),
                pltpu.VMEM((2 * vb, d), F32),
                pltpu.VMEM((vb, d), F32),
                pltpu.VMEM((half_d, 2 * t), BF16),
                pltpu.VMEM((2, 2, 2 * t, fc), BF16),
                pltpu.VMEM((2, 3, 2 * t, fc), BF16),
                pltpu.VMEM((2, 2, half_d, fc), F32),
                dma((2,)),
                dma((2,)),
                dma((5,)),
                dma((2, PARTS)),
                dma((3, PARTS)),
                dma((2, PARTS)),
                dma((2, PARTS)),
            ]
            + cube.groups(F32)
            + cube.sems(1),
            compiler_params=params(2),
            name="table",
        )(ids, dx_own, dm, down_shard, deh, a_t, gt, u)
        depth = 4
        loss, de, grad_gate, grad_up, grad_down = pl.pallas_call(
            weight_kernel,
            out_shape=(sds((1, 1), F32), sds((real, d), F32), sds((half_d, f), F32), sds((half_d, f), F32), sds((half_f, d), F32)),
            in_specs=[smem] + [hbm] * 8,
            out_specs=(smem,) + (hbm,) * 4,
            scratch_shapes=[
                pltpu.VMEM((half_d, 2 * t), BF16),
                pltpu.VMEM((2 * t, d), BF16),
                pltpu.VMEM((depth, 3, 2 * t, fc), BF16),
                pltpu.VMEM((depth, 2, half_d, fc), F32),
                pltpu.VMEM((2, 2, half_d, fc), F32),
                pltpu.VMEM((2, fc, d), F32),
                pltpu.VMEM((vb, d), F32),
                pltpu.VMEM((real, d), F32),
                dma((4,)),
                dma((3, depth)),
                dma((2, depth)),
                dma((3, 2)),
                dma((2, depth)),
            ],
            compiler_params=pltpu.CompilerParams(vmem_limit_bytes=VMEM_LIMIT, has_side_effects=True),
            name="weights",
        )(loss, de, a_t, d_gate, d_up, act, dmf, got_g, got_u)
        return loss.reshape(()), de, grad_gate, grad_up, grad_down

    return jax.shard_map(device_step, mesh=mesh, in_specs=(tok_spec, tok_spec, row_spec, weight_spec, weight_spec, weight_spec, P(), P()), out_specs=(P(), row_spec, weight_spec, weight_spec, weight_spec), check_vma=False)
```
